32 devices in a mesh: fsdp: 2 (over x), context: 4 (over z), tensor: 4 (over y, core).
Axes of the slice: x: 2, y: 2, z: 4, core: 2. Of those that a mesh axis runs over, the one named last changes fastest.
Arguments:
- activations: bfloat16 [2, 2048, 1152], P('fsdp', 'context'), may hold values from -6 to 6
- positions: int32 [2, 2048], P('fsdp', 'context'), may hold values from 0 to 2047, as said below
- seg_ids: int32 [2, 2048], P('fsdp', 'context'), may hold values from 0 to 3, as said below
- norm_gains: bfloat16 [4, 1152], P(None, ('fsdp', 'context')), may hold values from 0.5 to 1.5
- head_gains: bfloat16 [2, 256], P(None, ('fsdp', 'context')), may hold values from 0.25 to 1.75
- w_query: bfloat16 [1152, 1024], P(('fsdp', 'context'), 'tensor'), may hold values from -0.1875 to 0.1875
- w_keyval: bfloat16 [1152, 512], P(('fsdp', 'context')), may hold values from -0.1875 to 0.1875
- w_out: bfloat16 [1152, 1024], P(('fsdp', 'context'), 'tensor'), may hold values from -0.1875 to 0.1875
- w_gateup: bfloat16 [1152, 2, 6912], P(('fsdp', 'context'), None, 'tensor'), may hold values from -0.1875 to 0.1875
- w_down: bfloat16 [1152, 6912], P(('fsdp', 'context'), 'tensor'), may hold values from -0.078125 to 0.078125
- cotangent: bfloat16 [2, 2048, 1152], P('fsdp', 'context'), may hold values from -6 to 6
Outputs:
- block_output: bfloat16 [2, 2048, 1152], P('fsdp', 'context')
- input_grad: bfloat16 [2, 2048, 1152], P('fsdp', 'context')
- norm_gains_grad: float32 [4, 1152], P(None, ('fsdp', 'context'))
- head_gains_grad: float32 [2, 256], P(None, ('fsdp', 'context'))
- w_query_grad: float32 [1152, 1024], P(('fsdp', 'context'), 'tensor')
- w_keyval_grad: float32 [1152, 512], P(('fsdp', 'context'))
- w_out_grad: float32 [1152, 1024], P(('fsdp', 'context'), 'tensor')
- w_gateup_grad: float32 [1152, 2, 6912], P(('fsdp', 'context'), None, 'tensor')
- w_down_grad: float32 [1152, 6912], P(('fsdp', 'context'), 'tensor')
The draws below stay inside these ranges and needn't reach their ends.
Inputs may be any that keep to these rules, and one draw needn't show every extreme that they name: `positions`: within a sequence, a document is a run of consecutive tokens with one document number; numbers never fall along a sequence. Positions are 0 at a document's first token and rise by one from token to token inside it. The first sequence is one document. `seg_ids`: document numbers of a sequence start at 0 and never fall along it.
All inputs are finite; a program needn't handle non-finite values.
Results may differ from the reference program's by a relative error of at most 0.024.
Values may be sent and summed in bfloat16 or wider, within the bound.
A program may use at most 192 MiB of HBM per device.

```python
import jax
import jax.numpy as jnp
from jax import lax

D = 1152
H = 4
HD = 256
FF = 6912
WINDOW = 512
LENGTH = 2048
SEQS = 2


def document_layout(key):
    cut_points = jax.random.randint(jax.random.fold_in(key, 17), (SEQS, 3), 1, LENGTH)
    first_whole = jnp.arange(SEQS)[:, None] == 0
    cut_points = jnp.where(first_whole, LENGTH, cut_points)
    token_index = jnp.arange(LENGTH)
    passed = token_index[None, :, None] >= cut_points[:, None, :]
    numbers = jnp.sum(passed.astype(jnp.int32), axis=-1)
    begins = jnp.max(jnp.where(passed, cut_points[:, None, :], 0), axis=-1)
    return ((token_index[None, :] - begins).astype(jnp.int32), numbers.astype(jnp.int32))


def draw_positions(key, part):
    return document_layout(key)[0]


def draw_seg_ids(key, part):
    return document_layout(key)[1]


def with_spikes(values, own_key, source, target, parts, factor):
    owner, partner = [(jnp.arange(values.shape[dim]) // (values.shape[dim] // parts)).reshape([-1 if axis == dim else 1 for axis in range(values.ndim)]) for dim in (source, target)]
    chosen = jax.random.permutation(own_key, parts)[partner]
    strong = (owner == chosen) | (owner == (partner + parts // 2) % parts)
    return jnp.where(strong, factor * values, values)


def levels(rng, shape, pieces, low, largest):
    def one(dim, blocks):
        draws = jax.random.uniform(jax.random.fold_in(jax.random.fold_in(rng, 6), dim), (blocks,), jnp.float32, low / len(pieces), largest / len(pieces))
        return jnp.repeat(jnp.exp(draws), shape[dim] // blocks).reshape((-1,) + (1,) * (len(shape) - dim - 1))

    factor_of = one(*pieces[0])
    for cut in pieces[1:]:
        factor_of = factor_of * one(*cut)
    return factor_of


def gaussian(own_key, dims, width, limit, shards=(), kind=jnp.bfloat16):
    drawn = jax.random.normal(own_key, dims, jnp.float32) * width
    if len(shards) > 0:
        drawn = levels(own_key, dims, shards, -0.22, 0.18) * drawn
    return jnp.clip(drawn, min=-limit, max=limit).astype(kind)


def bell_draw_with(rng, dims, scale, reach, split, heavy, kind=jnp.bfloat16):
    values = scale * jax.random.normal(rng, dims, jnp.float32)
    if split:
        values = values * levels(rng, dims, split, -0.22, 0.18)
    return jnp.clip(with_spikes(values, jax.random.fold_in(rng, 3), *heavy), -reach, reach).astype(kind)


def setup_inputs(seed: int = 0) -> dict:
    splits = jax.random.split(jax.random.key(seed), 12)
    return {
        "activations": gaussian(splits[0], (SEQS, LENGTH, D), 1.0, 6.0, ((0, 2), (1, 4))),
        "positions": draw_positions(jax.random.fold_in(splits[11], 71), 0),
        "seg_ids": draw_seg_ids(jax.random.fold_in(splits[11], 71), 0),
        "norm_gains": jnp.clip(1.0 + 0.1 * jax.random.normal(splits[3], (4, D), jnp.float32), 0.5, 1.5).astype(jnp.bfloat16),
        "head_gains": jnp.clip(1.0 + 0.15 * jax.random.normal(splits[4], (2, HD), jnp.float32), 0.25, 1.75).astype(jnp.bfloat16),
        "w_query": gaussian(splits[5], (D, H * HD), D ** -0.5, 0.1875, ((0, 8), (1, 4))),
        "w_keyval": gaussian(splits[6], (D, 2 * HD), D ** -0.5, 0.1875, ((0, 8),)),
        "w_out": gaussian(splits[7], (D, H * HD), (H * HD) ** -0.5, 0.1875, ((0, 8), (1, 4))),
        "w_gateup": gaussian(splits[8], (D, 2, FF), D ** -0.5, 0.1875, ((0, 8), (2, 4))),
        "w_down": gaussian(splits[9], (D, FF), FF ** -0.5, 0.078125, ((0, 8), (1, 4))),
        "cotangent": bell_draw_with(splits[10], (SEQS, LENGTH, D), 1.0, 6.0, ((0, 2), (1, 4)), (1, 2, 4, 2.0)),
    }


EPSILON = 1e-06
HIGHEST = lax.Precision.HIGHEST

@jax.custom_vjp
def low(v):
    return lax.optimization_barrier(v.astype(jnp.bfloat16)).astype(jnp.float32)

@jax.custom_vjp
def low_back(v):
    return v

def low_keep(v):
    return (low(v), None)

def low_pass(kept, grad):
    return (grad,)

def back_keep(v):
    return (v, None)

def back_low(kept, grad):
    return (low(grad),)
low.defvjp(low_keep, low_pass)
low_back.defvjp(back_keep, back_low)

def rms_norm(values, gain):
    factor = lax.rsqrt(lax.optimization_barrier(jnp.mean(values * values, axis=-1, keepdims=True)) + EPSILON)
    return values * factor * gain

def rotate(tensor, places):
    width_all = tensor.shape[-1]
    half_width = width_all // 2
    freqs = jnp.power(10000.0, -jnp.arange(half_width, dtype=jnp.float32) * 2.0 / width_all)
    angles = places.astype(jnp.float32)[:, None] * freqs[None, :]
    cosine = jnp.cos(angles)[:, None, :]
    sine = jnp.sin(angles)[:, None, :]
    first_half = tensor[..., :half_width]
    second_half = tensor[..., half_width:]
    return jnp.concatenate([first_half * cosine - second_half * sine, second_half * cosine + first_half * sine], axis=-1)

def glu(gate_up):
    return jax.nn.gelu(gate_up[:, 0], approximate=True) * gate_up[:, 1]

def attend(queries, keys, values, places, documents):
    length = queries.shape[0]
    block_rows = 512 if length % 512 == 0 else length
    pad_keys = jnp.concatenate([jnp.zeros((WINDOW, HD), jnp.float32), keys], axis=0)
    pad_values = jnp.concatenate([jnp.zeros((WINDOW, HD), jnp.float32), values], axis=0)
    pad_places = jnp.concatenate([jnp.zeros((WINDOW,), jnp.int32), places.astype(jnp.int32)])
    pad_documents = jnp.concatenate([jnp.full((WINDOW,), -1, jnp.int32), documents.astype(jnp.int32)])
    scale_factor = HD ** (-0.5)

    def one_block(start):
        block_queries = lax.dynamic_slice_in_dim(queries, start, block_rows, 0)
        block_places = lax.dynamic_slice_in_dim(places.astype(jnp.int32), start, block_rows, 0)
        block_documents = lax.dynamic_slice_in_dim(documents.astype(jnp.int32), start, block_rows, 0)
        near_keys = lax.dynamic_slice_in_dim(pad_keys, start, WINDOW + block_rows, 0)
        near_values = lax.dynamic_slice_in_dim(pad_values, start, WINDOW + block_rows, 0)
        near_places = lax.dynamic_slice_in_dim(pad_places, start, WINDOW + block_rows, 0)
        near_documents = lax.dynamic_slice_in_dim(pad_documents, start, WINDOW + block_rows, 0)
        scores = jnp.einsum('qhd,kd->hqk', block_queries, near_keys, precision=HIGHEST) * scale_factor
        scores = low_back(scores)
        spacing = block_places[:, None] - near_places[None, :]
        visible = (block_documents[:, None] == near_documents[None, :]) & (spacing >= 0) & (spacing < WINDOW)
        scores = jnp.where(visible[None], scores, -1e+30)
        row_top = lax.optimization_barrier(jnp.max(scores, axis=-1, keepdims=True))
        raised = jnp.exp(scores - row_top)
        probs = low(raised / lax.optimization_barrier(jnp.sum(raised, axis=-1, keepdims=True)))
        return jnp.einsum('hqk,kd->qhd', probs, near_values, precision=HIGHEST)
    starts = (jnp.arange(length // block_rows) * block_rows).astype(jnp.int32)
    mixed = lax.map(jax.checkpoint(one_block), starts)
    return mixed.reshape(length, -1)

def mlp_tail(hidden, gains, w_gateup, w_down):
    normed_mlp = low(rms_norm(hidden, gains[2]))
    gate_up = low_back(jnp.einsum('ld,dkf->lkf', normed_mlp, w_gateup, precision=HIGHEST))
    active = low(glu(gate_up))
    down = low_back(lax.dot_general(active, w_down, (((1,), (1,)), ((), ())), precision=HIGHEST, preferred_element_type=jnp.float32))
    return hidden + rms_norm(down, gains[3])

def layer(inputs, places, documents, norm_gains, head_gains, w_query, w_keyval, w_out, w_gateup, w_down):
    length = inputs.shape[0]
    normed = low(rms_norm(inputs, norm_gains[0]))
    query_raw = jnp.dot(normed, w_query, precision=HIGHEST, preferred_element_type=jnp.float32).reshape(length, H, HD)
    keyval_raw = jnp.dot(normed, w_keyval, precision=HIGHEST, preferred_element_type=jnp.float32)
    queries = low(rotate(rms_norm(low_back(query_raw), head_gains[0]), places))
    keys = low(rotate(rms_norm(low_back(keyval_raw[:, None, :HD]), head_gains[1]), places))[:, 0]
    values = low(low_back(keyval_raw[:, HD:]))
    mixed = low(low_back(attend(queries, keys, values, places, documents)))
    branch = low_back(lax.dot_general(mixed, w_out, (((1,), (1,)), ((), ())), precision=HIGHEST, preferred_element_type=jnp.float32))
    hidden = inputs + rms_norm(branch, norm_gains[1])
    tail_rows = 4096 if length % 4096 == 0 else length

    def tail_block(hidden_block):
        return mlp_tail(hidden_block, norm_gains, w_gateup, w_down)
    result = lax.map(jax.checkpoint(tail_block), hidden.reshape(length // tail_rows, tail_rows, -1))
    return result.reshape(length, -1)

def reference(activations, positions, seg_ids, norm_gains, head_gains, w_query, w_keyval, w_out, w_gateup, w_down, cotangent):
    params = tuple((item.astype(jnp.float32) for item in (norm_gains, head_gains, w_query, w_keyval, w_out, w_gateup, w_down)))

    def per_sequence(totals, item):
        seq_inputs, seq_places, seq_documents, seq_cotangent = item

        def run(inputs, *weights):
            return layer(inputs, seq_places, seq_documents, *weights)
        result, back = jax.vjp(run, seq_inputs.astype(jnp.float32), *params)
        grads = back(seq_cotangent.astype(jnp.float32))
        totals = tuple((total + grad for total, grad in zip(totals, grads[1:])))
        return (totals, (result.astype(jnp.bfloat16), grads[0].astype(jnp.bfloat16)))
    zero_totals = tuple((jnp.zeros(item.shape, jnp.float32) for item in params))
    totals, outputs = lax.scan(per_sequence, zero_totals, (activations, positions, seg_ids, cotangent))
    return (outputs[0], outputs[1], totals[0], totals[1], totals[2], totals[3], totals[4], totals[5], totals[6])
```

```python
import jax
import jax.numpy as jnp
from jax import lax
from jax.sharding import PartitionSpec as P

HD = 256
WINDOW = 512


EPSILON = 1e-06


def from_behind(block, axis, distance):
    devices = range(lax.axis_size(axis))
    route = [(i - distance, i) for i in devices if i - distance in devices]
    return lax.ppermute(block, axis, route)


def rms_norm(values, gain):
    factor = lax.rsqrt(jnp.mean(values * values, axis=-1, keepdims=True) + EPSILON)
    return values * factor * gain


def rotate(tensor, places):
    width_all = tensor.shape[-1]
    half_width = width_all // 2
    freqs = jnp.power(10000.0, -jnp.arange(half_width, dtype=jnp.float32) * 2.0 / width_all)
    angles = places.astype(jnp.float32)[:, None] * freqs[None, :]
    cosine = jnp.cos(angles)[:, None, :]
    sine = jnp.sin(angles)[:, None, :]
    first_half = tensor[..., :half_width]
    second_half = tensor[..., half_width:]
    return jnp.concatenate(
        [first_half * cosine - second_half * sine, second_half * cosine + first_half * sine],
        axis=-1,
    )


def glu(gate_up):
    return jax.nn.gelu(gate_up[:, 0], approximate=True) * gate_up[:, 1]


def contract_last(left_side, right_side):
    return lax.dot_general(
        left_side, right_side, (((1,), (1,)), ((), ())), preferred_element_type=jnp.float32
    )


def contract_first(left_side, right_side):
    return lax.dot_general(
        left_side, right_side, (((0,), (0,)), ((), ())), preferred_element_type=jnp.float32
    )


def shards(
    activations,
    positions,
    seg_ids,
    norm_gains,
    head_gains,
    w_query,
    w_keyval,
    w_out,
    w_gateup,
    w_down,
    cotangent,
):
    tokens = activations.shape[1]
    local_heads = w_query.shape[1] // HD
    inputs = activations[0].astype(jnp.float32)
    places = positions[0]
    documents = seg_ids[0]
    gains_all, heads_all, query_all, keyval_all, out_all = (
        lax.all_gather(norm_gains, ("fsdp", "context"), axis=1, tiled=True),
        lax.all_gather(head_gains, ("fsdp", "context"), axis=1, tiled=True),
        lax.all_gather(w_query, ("fsdp", "context"), axis=0, tiled=True),
        lax.all_gather(w_keyval, ("fsdp", "context"), axis=0, tiled=True),
        lax.all_gather(w_out, ("fsdp", "context"), axis=0, tiled=True),
    )
    gains_f = gains_all.astype(jnp.float32)
    heads_f = heads_all.astype(jnp.float32)
    normed_f, input_back = jax.vjp(rms_norm, inputs, gains_f[0])
    normed = normed_f.astype(jnp.bfloat16)
    query_raw = jnp.dot(normed, query_all, preferred_element_type=jnp.float32).reshape(
        tokens, local_heads, HD
    )
    keyval_raw = jnp.dot(normed, keyval_all, preferred_element_type=jnp.float32)

    def prepare(raw_heads, head_gain):
        return rotate(rms_norm(raw_heads, head_gain), places)

    query_rot, query_back = jax.vjp(prepare, query_raw, heads_f[0])
    key_rot, key_back = jax.vjp(prepare, keyval_raw[:, None, :HD], heads_f[1])
    queries = query_rot.astype(jnp.bfloat16)
    own_keyval = jnp.concatenate([key_rot[:, 0], keyval_raw[:, HD:]], axis=1).astype(jnp.bfloat16)
    labels = jnp.stack([places, documents])
    keep_from = tokens - tokens
    left_keyval, left_labels = from_behind((own_keyval, labels), "context", 1)
    keys_all = jnp.concatenate([left_keyval, own_keyval], axis=0)
    key_places = jnp.concatenate([left_labels[0], places])
    key_documents = jnp.concatenate([left_labels[1], documents])
    has_left = lax.axis_index("context") > 0
    key_live = jnp.concatenate([jnp.full((tokens,), has_left), jnp.ones((tokens,), dtype=bool)])
    scale_factor = HD ** (-0.5)
    block_rows = 512
    block_starts = jnp.arange(tokens // block_rows) * block_rows

    def block_scores():
        spacing = places[:, None] - key_places[None, :]
        visible = (
            key_live[None, :]
            & (documents[:, None] == key_documents[None, :])
            & (spacing >= 0)
            & (spacing < WINDOW)
        )
        raw_scores = (
            jnp.einsum("qhd,kd->hqk", queries, keys_all[:, :HD], preferred_element_type=jnp.float32)
            * scale_factor
        )
        return (jnp.where(visible[None], raw_scores, -1e30), keys_all, queries)

    def forward_block(start):
        scores, near_keyval, query_block = block_scores()
        row_top = jnp.max(scores, axis=-1, keepdims=True)
        raised = jnp.exp(scores - row_top)
        row_total = jnp.sum(raised, axis=-1, keepdims=True)
        probs = raised / row_total
        mixed_block = jnp.einsum(
            "hqk,kd->qhd",
            probs.astype(jnp.bfloat16),
            near_keyval[:, HD:],
            preferred_element_type=jnp.float32,
        )
        return (mixed_block.astype(jnp.bfloat16), row_top + jnp.log(row_total))

    mixed_blocks, log_blocks = lax.map(forward_block, block_starts)
    mixed_low = mixed_blocks.reshape(tokens, local_heads * HD)
    branch = lax.psum(contract_last(mixed_low, out_all).astype(jnp.bfloat16), "tensor").astype(jnp.float32)
    post_attn, post_attn_back = jax.vjp(rms_norm, branch, gains_f[1])
    hidden = inputs + post_attn
    normed_mlp_f, pre_mlp_back = jax.vjp(rms_norm, hidden, gains_f[2])
    normed_mlp = normed_mlp_f.astype(jnp.bfloat16)
    columns = normed_mlp
    gate_up = jnp.einsum(
        "bn,nkf->bkf",
        columns,
        lax.all_gather(w_gateup, ("fsdp", "context"), axis=0, tiled=True),
        preferred_element_type=jnp.float32,
    )
    active_f, glu_back = jax.vjp(glu, gate_up)
    active = active_f.astype(jnp.bfloat16)
    down = lax.psum(
        contract_last(
            active, lax.all_gather(w_down, ("fsdp", "context"), axis=0, tiled=True)
        ).astype(jnp.bfloat16),
        "tensor",
    ).astype(jnp.float32)
    post_mlp, post_mlp_back = jax.vjp(rms_norm, down, gains_f[3])
    result = hidden + post_mlp
    grad_out = cotangent[0].astype(jnp.float32)
    d_down, gain_post_mlp = post_mlp_back(grad_out)
    down_low = d_down.astype(jnp.bfloat16)
    columns = down_low
    d_active = jnp.dot(
        columns,
        lax.all_gather(w_down, ("fsdp", "context"), axis=0, tiled=True),
        preferred_element_type=jnp.float32,
    )
    d_gate_up = glu_back(d_active)[0].astype(jnp.bfloat16)
    d_normed_part = jnp.einsum(
        "bkf,nkf->bn",
        d_gate_up,
        lax.all_gather(w_gateup, ("fsdp", "context"), axis=0, tiled=True),
        preferred_element_type=jnp.float32,
    )
    d_normed_mlp = lax.psum(d_normed_part.astype(jnp.bfloat16), "tensor").astype(jnp.float32)
    d_hidden_norm, gain_pre_mlp = pre_mlp_back(d_normed_mlp)
    d_hidden = grad_out + d_hidden_norm
    features = normed_mlp
    grad_cols = down_low
    gate_up_term = jnp.einsum(
        "bn,bkf->nkf", features, d_gate_up, preferred_element_type=jnp.float32
    )
    down_term = contract_first(grad_cols, active)
    scatter = lambda part: lax.psum_scatter(
        part.astype(jnp.bfloat16), ("fsdp", "context"), scatter_dimension=0, tiled=True
    ).astype(jnp.float32)
    gate_grad = scatter(gate_up_term[:, 0])
    up_grad = scatter(gate_up_term[:, 1])
    down_grad = scatter(down_term)
    d_branch, gain_post_attn = post_attn_back(d_hidden)
    branch_low = d_branch.astype(jnp.bfloat16)
    d_mixed = jnp.dot(branch_low, out_all, preferred_element_type=jnp.float32)
    d_mixed_low = d_mixed.astype(jnp.bfloat16).reshape(tokens, local_heads, HD)

    def backward_block(carry, item):
        start, log_block = item
        scores, near_keyval, query_block = block_scores()
        probs_again = jnp.exp(scores - log_block)
        d_probs = jnp.einsum(
            "qhd,kd->hqk", d_mixed_low, near_keyval[:, HD:], preferred_element_type=jnp.float32
        )
        row_inner = jnp.sum(probs_again * d_probs, axis=-1, keepdims=True)
        d_scores = (probs_again * (d_probs - row_inner)).astype(jnp.bfloat16)
        d_query_block = (
            jnp.einsum(
                "hqk,kd->qhd", d_scores, near_keyval[:, :HD], preferred_element_type=jnp.float32
            )
            * scale_factor
        )
        d_keys = (
            jnp.einsum("hqk,qhd->kd", d_scores, query_block, preferred_element_type=jnp.float32)
            * scale_factor
        )
        d_values = jnp.einsum(
            "hqk,qhd->kd",
            probs_again.astype(jnp.bfloat16),
            d_mixed_low,
            preferred_element_type=jnp.float32,
        )
        updated = carry + jnp.concatenate([d_keys, d_values], axis=1)
        return (updated, d_query_block)

    d_keyval, d_query_blocks = lax.scan(
        backward_block,
        jnp.zeros((tokens + tokens, 2 * HD), jnp.float32),
        (block_starts, log_blocks),
    )
    d_queries = d_query_blocks.reshape(tokens, local_heads, HD)
    returned = from_behind(d_keyval[:tokens].astype(jnp.bfloat16), "context", -1).astype(
        jnp.float32
    )
    own_grad = d_keyval[tokens:].at[keep_from:].add(returned)
    d_query_raw, gain_query = query_back(d_queries)
    d_query_low = d_query_raw.reshape(tokens, local_heads * HD).astype(jnp.bfloat16)
    d_normed_query, keyval_grad, gain_query_all = (
        lax.psum(contract_last(d_query_low, query_all).astype(jnp.bfloat16), "tensor").astype(
            jnp.float32
        ),
        lax.psum(own_grad.astype(jnp.bfloat16), "tensor").astype(jnp.float32),
        lax.psum(gain_query.astype(jnp.bfloat16), "tensor").astype(jnp.float32),
    )
    d_key_raw, gain_key = key_back(keyval_grad[:, None, :HD])
    d_keyval_low = jnp.concatenate([d_key_raw[:, 0], keyval_grad[:, HD:]], axis=1).astype(
        jnp.bfloat16
    )
    d_normed = d_normed_query + contract_last(d_keyval_low, keyval_all)
    d_input_norm, gain_input = input_back(d_normed)
    input_total = d_hidden + d_input_norm
    features = normed
    grad_cols = branch_low
    attn_grads = lax.psum_scatter(
        jnp.stack(
            [contract_first(features, d_query_low), contract_first(grad_cols, mixed_low)], axis=1
        ).astype(jnp.bfloat16),
        ("fsdp", "context"),
        scatter_dimension=0,
        tiled=True,
    ).astype(jnp.float32)
    keyval_term = contract_first(normed, d_keyval_low)
    gain_terms = jnp.stack([gain_input, gain_post_attn, gain_pre_mlp, gain_post_mlp])
    head_terms = jnp.stack([gain_query_all, gain_key])
    gain_grad, head_grad, keyval_weight_grad = (
        lax.psum_scatter(
            gain_terms.astype(jnp.bfloat16), ("fsdp", "context"), scatter_dimension=1, tiled=True
        ).astype(jnp.float32),
        lax.psum_scatter(
            head_terms.astype(jnp.bfloat16), ("fsdp", "context"), scatter_dimension=1, tiled=True
        ).astype(jnp.float32),
        lax.psum_scatter(
            keyval_term.astype(jnp.bfloat16), ("fsdp", "context"), scatter_dimension=0, tiled=True
        ).astype(jnp.float32),
    )
    return (
        result[None].astype(jnp.bfloat16),
        input_total[None].astype(jnp.bfloat16),
        gain_grad,
        head_grad,
        attn_grads[:, 0],
        keyval_weight_grad,
        attn_grads[:, 1],
        jnp.stack([gate_grad, up_grad], axis=1),
        down_grad,
    )


def solution(mesh):
    return jax.shard_map(
        shards,
        mesh=mesh,
        in_specs=(
            P("fsdp", "context", None),
            P("fsdp", "context"),
            P("fsdp", "context"),
            P(None, ("fsdp", "context")),
            P(None, ("fsdp", "context")),
            P(("fsdp", "context"), "tensor"),
            P(("fsdp", "context"), None),
            P(("fsdp", "context"), "tensor"),
            P(("fsdp", "context"), None, "tensor"),
            P(("fsdp", "context"), "tensor"),
            P("fsdp", "context", None),
        ),
        out_specs=(
            P("fsdp", "context", None),
            P("fsdp", "context", None),
            P(None, ("fsdp", "context")),
            P(None, ("fsdp", "context")),
            P(("fsdp", "context"), "tensor"),
            P(("fsdp", "context"), None),
            P(("fsdp", "context"), "tensor"),
            P(("fsdp", "context"), None, "tensor"),
            P(("fsdp", "context"), "tensor"),
        ),
        check_vma=False,
    )
```

```python
import functools

import jax
import jax.numpy as jnp
from jax import lax
from jax.experimental import pallas as pl
from jax.experimental.pallas import tpu as pltpu
from jax.sharding import PartitionSpec as P

HD = 256
WINDOW = 512


EPSILON = 1e-06


def from_behind(block, axis, distance):
    devices = range(lax.axis_size(axis))
    route = [(i - distance, i) for i in devices if i - distance in devices]
    return lax.ppermute(block, axis, route)


def rms_norm(values, gain):
    factor = lax.rsqrt(jnp.mean(values * values, axis=-1, keepdims=True) + EPSILON)
    return values * factor * gain


def rotate(tensor, places):
    width_all = tensor.shape[-1]
    half_width = width_all // 2
    freqs = jnp.power(10000.0, -jnp.arange(half_width, dtype=jnp.float32) * 2.0 / width_all)
    angles = places.astype(jnp.float32)[:, None] * freqs[None, :]
    cosine = jnp.cos(angles)[:, None, :]
    sine = jnp.sin(angles)[:, None, :]
    first_half = tensor[..., :half_width]
    second_half = tensor[..., half_width:]
    return jnp.concatenate(
        [first_half * cosine - second_half * sine, second_half * cosine + first_half * sine],
        axis=-1,
    )


def glu(gate_up):
    return jax.nn.gelu(gate_up[:, 0], approximate=True) * gate_up[:, 1]


def contract_last(left_side, right_side):
    return lax.dot_general(
        left_side, right_side, (((1,), (1,)), ((), ())), preferred_element_type=jnp.float32
    )


def contract_first(left_side, right_side):
    return lax.dot_general(
        left_side, right_side, (((0,), (0,)), ((), ())), preferred_element_type=jnp.float32
    )


MESH = pl.DeviceIdType.MESH
F32 = jnp.float32
BF16 = jnp.bfloat16
LANES = 128
SEMAPHORES = 112


def mm(left, right):
    return jnp.dot(left, right, preferred_element_type=F32)


def rms_factor(values):
    return lax.rsqrt(jnp.mean(values * values, axis=-1, keepdims=True) + EPSILON)


def rms_backward(grad, values, factor, gain):
    unit = values * factor
    scaled = grad * gain
    inner = jnp.mean(scaled * unit, axis=-1, keepdims=True)
    return factor * (scaled - unit * inner), jnp.sum(grad * unit, axis=0, keepdims=True)


def turn(values, cosine, sine):
    half = values.shape[-1] // 2
    first, second = values[:, :half], values[:, half:]
    return jnp.concatenate([first * cosine - second * sine, second * cosine + first * sine], axis=1)


def turn_back(values, cosine, sine):
    half = values.shape[-1] // 2
    first, second = values[:, :half], values[:, half:]
    return jnp.concatenate([first * cosine + second * sine, second * cosine - first * sine], axis=1)


def fused_kernel(
    sizes,
    act,
    cosine,
    sine,
    seg_row,
    seg_col,
    cot_all,
    w_attn,
    w_ff,
    out_block,
    out_input,
    out_gains,
    out_ff,
    out_attn,
    out_kv,
    cot,
    wa,
    wf,
    seg_left,
    gain_rows,
    head_rows,
    nrm,
    qraw,
    kraw,
    qs,
    kv,
    probs,
    mix,
    p4,
    p4_core,
    p4_sum,
    p4_chip,
    hid,
    bran,
    xg,
    gel,
    upg,
    active,
    p8,
    p8_core,
    p8_sum,
    p8_chip,
    dd,
    dhid,
    db,
    dscore,
    dmix,
    dq,
    kvp,
    kvp_core,
    kvp_sum,
    kvp_chip,
    ret_out,
    ret_in,
    dkv,
    gall_x,
    gall_z,
    ga,
    ga_x,
    ga_z,
    kvg,
    ff_stage,
    gain_mine,
    gain_tensor,
    gain_x,
    gain_z,
    block_all,
    input_all,
    ss,
    rs,
    ls,
):
    C = sizes["context"]
    T, D, R, U = sizes["tokens"], sizes["width"], sizes["rows"], sizes["units"]
    S = T // 4
    f = lax.axis_index("fsdp")
    c = lax.axis_index("context")
    t = lax.axis_index("tensor")
    y, core = t // 2, t % 2
    m = c % 2
    base = c - m
    partner = {"tensor": y * 2 + (1 - core)}
    across = {"fsdp": 1 - f}
    counter = [0]
    sent = []

    def slots(count):
        first = counter[0]
        counter[0] += count
        assert counter[0] <= SEMAPHORES
        return first

    def copy(k, src, dst, device):
        return pltpu.make_async_remote_copy(
            src_ref=src,
            dst_ref=dst,
            send_sem=ss.at[k],
            recv_sem=rs.at[k],
            device_id=device,
            device_id_type=MESH,
        )

    def send(k, src, dst, device):
        moved = copy(k, src, dst, device)
        moved.start()
        sent.append(moved)

    def arrive(k, dst):
        copy(k, dst, dst, partner).wait_recv()

    def settle():
        for moved in sent:
            moved.wait_send()
        sent.clear()

    def along(step):
        return {"context": (c + step) % C}

    def rows_of(ff, cc):
        return pl.ds(pl.multiple_of((ff * C + cc) * R, R), R)

    def chip_of(k, count):
        if count == 2:
            return {"tensor": k * 2 + core}
        return {"context": base + k // 2, "tensor": (k % 2) * 2 + core}

    barrier = pltpu.get_barrier_semaphore()
    greeted = [along(step) for step in range(1, C)] + [across]
    greeted += [{"tensor": (t + step) % 4} for step in range(1, 4)]
    greeted += [{"context": base + 1 - m, "tensor": (1 - y) * 2 + core}]
    for device in greeted:
        pl.semaphore_signal(barrier, inc=1, device_id=device, device_id_type=MESH)
    pl.semaphore_wait(barrier, len(greeted))

    mine = rows_of(f, c)
    own_attn = pltpu.make_async_copy(w_attn, wa.at[mine], ls.at[0])
    own_attn.start()
    ka = slots(2 * C)
    for step in range(1, C):
        send(ka + step, w_attn, wa.at[mine], along(step))
    send(ka, w_attn, wa.at[mine], across)
    ks = slots(1)

    @pl.when(c < C - 1)
    def _():
        copy(ks, seg_row, seg_left, {"context": c + 1}).start()

    shard = pl.ds(pl.multiple_of(t * S, S), S)
    own_cot = pltpu.make_async_copy(cot_all.at[shard], cot, ls.at[2])
    own_cot.start()
    own_ff = pltpu.make_async_copy(w_ff.at[m], wf.at[:, mine], ls.at[1])
    own_ff.start()
    own_attn.wait()
    for step in range(1, C):
        block = wa.at[rows_of(f, (c - step + C) % C)]
        arrive(ka + step, block)
        send(ka + C + step, block, block, across)
    arrive(ka, wa.at[rows_of(1 - f, c)])
    for step in range(1, C):
        arrive(ka + C + step, wa.at[rows_of(1 - f, (c - step + C) % C)])

    @pl.when(c > 0)
    def _():
        arrive(ks, seg_left)

    @pl.when(c == 0)
    def _():
        seg_left[...] = jnp.full(seg_left.shape, -1, jnp.int32)
        kv[0:T] = jnp.zeros((T, 2 * HD), BF16)

    gain_t = jnp.transpose(wa[:, 4 * HD :].astype(F32))
    gain_rows[...] = gain_t[0:8]
    narrow = HD // (2 * C)
    here = lax.broadcasted_iota(jnp.int32, (D, HD), 0)
    want = lax.broadcasted_iota(jnp.int32, (D, HD), 1)
    shift = narrow.bit_length() - 1
    want = lax.shift_right_logical(want, shift) * R + (want & (narrow - 1))
    pick = jnp.where(here == want, 1.0, 0.0).astype(BF16)
    head_rows[...] = mm(gain_t[0:16].astype(BF16), pick)[0:8]

    def gain(index):
        return gain_rows[index : index + 1]

    def head_gain(index):
        return head_rows[4 + index : 5 + index]

    half = T // 2

    def project(i, _):
        rows = pl.ds(pl.multiple_of(i * half, half), half)
        values = act[rows].astype(F32)
        low = (values * rms_factor(values) * gain(0)).astype(BF16)
        nrm[rows] = low
        raw_q = mm(low, wa[:, 0:HD])
        raw_kv = mm(low, wa[:, HD : 3 * HD])
        raw_k = raw_kv[:, :HD]
        qraw[rows] = raw_q
        kraw[rows] = raw_k
        cos, sin = cosine[rows], sine[rows]
        qs[rows] = turn(raw_q * rms_factor(raw_q) * head_gain(0), cos, sin).astype(BF16)
        own = pl.ds(pl.multiple_of(T + i * half, half), half)
        kv[own, 0:HD] = turn(raw_k * rms_factor(raw_k) * head_gain(1), cos, sin).astype(BF16)
        kv[own, HD:] = raw_kv[:, HD:].astype(BF16)
        return 0

    lax.fori_loop(0, 2, project, 0)

    kk = slots(2)
    my_half = pl.ds(pl.multiple_of(core * half, half), half)
    other_half = pl.ds(pl.multiple_of((1 - core) * half, half), half)
    own_half = pl.ds(pl.multiple_of(T + core * half, half), half)

    @pl.when(c < C - 1)
    def _():
        copy(kk, kv.at[own_half], kv.at[my_half], {"context": c + 1}).start()

    kf = slots(2 * C)
    for step in range(1, C):
        send(kf + step, w_ff.at[(c + step) % 2], wf.at[:, mine], along(step))
    send(kf, w_ff.at[m], wf.at[:, mine], across)

    @pl.when(c > 0)
    def _():
        arrive(kk, kv.at[my_half])
        moved = copy(kk + 1, kv.at[my_half], kv.at[my_half], partner)
        moved.start()
        arrive(kk + 1, kv.at[other_half])
        moved.wait_send()

    scale = HD**-0.5
    no_left = jnp.where(c > 0, 0, 2 * T)
    k4 = slots(2)

    def attend(i, _):
        rows = pl.ds(pl.multiple_of(i * half, half), half)
        q = qs[rows]
        labels = seg_col[rows]
        row = lax.broadcasted_iota(jnp.int32, (half, T), 0) + i * half
        col = lax.broadcasted_iota(jnp.int32, (half, T), 1)
        left = contract_last(q, kv[0:T, 0:HD]) * scale
        left = jnp.where((labels == seg_left[0:1]) & (col > row + no_left), left, -1e30)
        own = contract_last(q, kv[T:, 0:HD]) * scale
        own = jnp.where((labels == seg_row[0:1]) & (col <= row), own, -1e30)
        top = jnp.maximum(
            jnp.max(left, axis=1, keepdims=True), jnp.max(own, axis=1, keepdims=True)
        )
        left, own = jnp.exp(left - top), jnp.exp(own - top)
        total = jnp.sum(left, axis=1, keepdims=True) + jnp.sum(own, axis=1, keepdims=True)
        left, own = left / total, own / total
        probs[rows, 0:T] = left
        probs[rows, T:] = own
        mixed = mm(left.astype(BF16), kv[0:T, HD:]) + mm(own.astype(BF16), kv[T:, HD:])
        mixed = mixed.astype(BF16)
        mix[rows] = mixed
        part = contract_last(mixed, wa[:, 3 * HD : 4 * HD]).astype(BF16)
        p4[i, 0] = part[0:S]
        p4[i, 1] = part[S:]
        copy(k4 + i, p4.at[i, 1 - core], p4_core.at[i], partner).start()
        return 0

    lax.fori_loop(0, 2, attend, 0)

    def relay_ff(step):
        block = wf.at[:, rows_of(f, (c - step + C) % C)]
        arrive(kf + step, block)
        send(kf + C + step, block, block, across)

    def sum4(k):
        kc = slots(1)
        arrive(k + (1 - y), p4_core.at[1 - y])
        p4_sum[...] = (
            p4[1 - y, core].astype(F32) + p4_core[1 - y].astype(F32)
        ).astype(BF16)
        copy(kc, p4_sum, p4_chip, chip_of(1 - y, 2)).start()
        arrive(k + y, p4_core.at[y])
        return kc

    def finish4(kc):
        arrive(kc, p4_chip)
        return (
            p4[y, core].astype(F32)
            + p4_core[y].astype(F32)
            + p4_chip[...].astype(F32)
        )

    kc = sum4(k4)
    relay_ff(1)
    branch = finish4(kc)
    copy(kc, p4_sum, p4_chip, chip_of(1 - y, 2)).wait_send()
    for i in range(2):
        copy(k4 + i, p4.at[i, 1 - core], p4_core.at[i], partner).wait_send()

    bran[...] = branch
    hidden = act[shard].astype(F32) + branch * rms_factor(branch) * gain(1)
    hid[...] = hidden
    low = (hidden * rms_factor(hidden) * gain(2)).astype(BF16)

    me = m * 2 + y

    def gather8(full, value):
        kg = slots(8)
        full[me, core] = value
        send(kg + 4, full.at[me, core], full.at[me, core], partner)
        for i in range(1, 4):
            send(kg + i, full.at[me, core], full.at[me, core], chip_of((me + i) % 4, 4))
        return kg

    def pass8(kg, full, i):
        k = (me - i + 4) % 4
        arrive(kg + i, full.at[k, core])
        copy(kg + 4 + i, full.at[k, core], full.at[k, core], partner).start()

    def meet8(kg, full, i):
        k = (me - i + 4) % 4
        arrive(kg + 4 + i, full.at[k, 1 - core])

    def settle8(kg, full):
        for i in range(1, 4):
            k = (me - i + 4) % 4
            copy(kg + 4 + i, full.at[k, core], full.at[k, core], partner).wait_send()

    def give8(ko, i):
        k = (me - i + 4) % 4
        copy(ko + i, p8.at[k, 1 - core], p8_core.at[i], partner).start()

    def push8(ko, i):
        k = (me - i + 4) % 4
        arrive(ko + i, p8_core.at[i])
        p8_sum[i - 1] = (
            p8[k, core].astype(F32) + p8_core[i].astype(F32)
        ).astype(BF16)
        copy(ko + 4 + i, p8_sum.at[i - 1], p8_chip.at[i - 1], chip_of(k, 4)).start()

    def finish8(ko):
        arrive(ko, p8_core.at[0])
        total = p8[me, core].astype(F32) + p8_core[0].astype(F32)
        for i in range(1, 4):
            arrive(ko + 4 + i, p8_chip.at[i - 1])
            total = total + p8_chip[i - 1].astype(F32)
        for i in range(4):
            copy(ko + i, p8.at[0, 1 - core], p8_core.at[i], partner).wait_send()
        for i in range(1, 4):
            copy(ko + 4 + i, p8_sum.at[0], p8_chip.at[0], partner).wait_send()
        return total

    kx = gather8(xg, low)
    for step in range(2, C):
        relay_ff(step)
    own_ff.wait()
    own_cot.wait()
    arrive(kf, wf.at[:, rows_of(1 - f, c)])
    for step in range(1, C):
        arrive(kf + C + step, wf.at[:, rows_of(1 - f, (c - step + C) % C)])

    root = 0.7978845608028654
    ko = slots(8)

    def forward(i, _):
        k = (me - i + 4) % 4
        meet8(kx, xg, i)
        x = xg[k].reshape(2 * S, D)
        gate = mm(x, wf[0])
        up = mm(x, wf[1])

        @pl.when(i < 3)
        def _():
            pass8(kx, xg, i + 1)

        square = gate * gate
        bent = jnp.tanh(root * gate * (1.0 + 0.044715 * square))
        ramp = 0.5 * (1.0 + bent)
        gelu = gate * ramp
        slope = ramp + 0.5 * gate * (1.0 - bent * bent) * root * (1.0 + 3 * 0.044715 * square)
        gel[k] = gelu.astype(BF16)
        upg[k] = (up * slope).astype(BF16)
        low = (gelu * up).astype(BF16)
        active[k] = low
        p8[k] = contract_last(low, wf[2]).astype(BF16).reshape(2, S, D)
        give8(ko, i)

        @pl.when(i > 1)
        def _():
            push8(ko, i - 1)

        return 0

    lax.fori_loop(0, 4, forward, 0)
    push8(ko, 3)
    settle8(kx, xg)
    down = finish8(ko)

    factor = rms_factor(down)
    grad = cot[...].astype(F32)
    result = (hid[...] + down * factor * gain(3)).astype(BF16)
    d_down, gain_3 = rms_backward(grad, down, factor, gain(3))
    gain_mine[3:4] = gain_3
    kd = gather8(dd, d_down.astype(BF16))

    def share4(full, value):
        kb = slots(4)
        full[y, core] = value
        for i in range(1, 4):
            send(kb + i, full.at[y, core], full.at[y, core], {"tensor": (t + i) % 4})
        return kb

    def meet4(kb, full):
        for i in range(1, 4):
            k = (t - i + 4) % 4
            arrive(kb + i, full.at[k // 2, k % 2])

    kr = share4(block_all, result)
    ko2 = slots(8)

    def backward(i, _):
        k = (me - i + 4) % 4
        meet8(kd, dd, i)
        low = dd[k].reshape(2 * S, D)
        d_active = mm(low, wf[2])

        @pl.when(i < 3)
        def _():
            pass8(kd, dd, i + 1)

        d_gate = (d_active * upg[k].astype(F32)).astype(BF16)
        d_up = (d_active * gel[k].astype(F32)).astype(BF16)
        upg[k] = d_gate
        gel[k] = d_up
        p8[k] = (
            (contract_last(d_gate, wf[0]) + contract_last(d_up, wf[1]))
            .astype(BF16)
            .reshape(2, S, D)
        )
        give8(ko2, i)

        @pl.when(i > 1)
        def _():
            push8(ko2, i - 1)

        return 0

    lax.fori_loop(0, 4, backward, 0)
    push8(ko2, 3)
    settle8(kd, dd)

    settle()
    gall = wf
    kw = slots(3)
    kz = slots(3 * C)
    mine_x = pl.ds(pl.multiple_of(f * C * R, C * R), C * R)
    theirs_x = pl.ds(pl.multiple_of((1 - f) * C * R, C * R), C * R)

    def weight_grad(w, left, right):
        def tile(n, _):
            cols = pl.ds(pl.multiple_of(n * LANES, LANES), LANES)
            block = left[:, :, :, cols].reshape(8 * S, LANES)
            gall[w, pl.ds(pl.multiple_of(n * LANES, LANES), LANES)] = contract_first(
                block, right[...].reshape(8 * S, U)
            ).astype(BF16)
            return 0

        lax.fori_loop(0, D // LANES, tile, 0)
        send(kw + w, gall.at[w, theirs_x], gall_x.at[w], across)

    def weight_push(w):
        arrive(kw + w, gall_x.at[w])

        def add(n, _):
            rows = pl.ds(pl.multiple_of(f * C * R + n * R, R), R)
            part = pl.ds(pl.multiple_of(n * R, R), R)
            gall[w, rows] = (
                gall[w, rows].astype(F32) + gall_x[w, part].astype(F32)
            ).astype(BF16)
            return 0

        lax.fori_loop(0, C, add, 0)
        for step in range(1, C):
            send(
                kz + w * C + step,
                gall.at[w, rows_of(f, (c + step) % C)],
                gall_z.at[step - 1, w],
                along(step),
            )

    def weight_end(w):
        same = gall[w, rows_of(f, c)].astype(F32)
        other = jnp.zeros((R, U), F32)
        for step in range(1, C):
            arrive(kz + w * C + step, gall_z.at[step - 1, w])
            if step % 2:
                other = other + gall_z[step - 1, w].astype(F32)
            else:
                same = same + gall_z[step - 1, w].astype(F32)
        ff_stage[m] = same
        ff_stage[1 - m] = other
        saved = pltpu.make_async_copy(ff_stage, out_ff.at[w], ls.at[5])
        saved.start()
        saved.wait()

    weight_grad(2, dd, active)
    d_normed = finish8(ko2)
    hidden = hid[...]
    d_hidden, gain_2 = rms_backward(d_normed, hidden, rms_factor(hidden), gain(2))
    d_hidden = cot[...].astype(F32) + d_hidden
    dhid[...] = d_hidden
    gain_mine[2:3] = gain_2
    branch = bran[...]
    d_branch, gain_1 = rms_backward(d_hidden, branch, rms_factor(branch), gain(1))
    gain_mine[1:2] = gain_1
    kb = share4(db, d_branch.astype(BF16))
    weight_grad(0, xg, upg)
    meet4(kb, db)

    def scores_back(i, gain_q):
        rows = pl.ds(pl.multiple_of(i * half, half), half)
        d_mixed = mm(db[i].reshape(half, D), wa[:, 3 * HD : 4 * HD]).astype(BF16)
        dmix[rows] = d_mixed
        p = probs[rows]
        d_probs = contract_last(d_mixed, kv[:, HD:])
        inner = jnp.sum(p * d_probs, axis=1, keepdims=True)
        low = (p * (d_probs - inner)).astype(BF16)
        dscore[rows] = low
        d_q = mm(low, kv[:, 0:HD]) * scale
        raw = qraw[rows]
        factor = rms_factor(raw)
        d_raw, part = rms_backward(
            turn_back(d_q, cosine[rows], sine[rows]), raw, factor, head_gain(0)
        )
        dq[rows] = d_raw.astype(BF16)
        return gain_q + part

    gain_q = lax.fori_loop(0, 2, scores_back, jnp.zeros((1, HD), F32))
    kp = slots(3)

    def keys_back(n, _):
        cols = pl.ds(pl.multiple_of(n * half, half), half)
        d_k = contract_first(dscore[:, cols], qs[...]) * scale
        d_v = contract_first(probs[:, cols].astype(BF16), dmix[...])
        both = jnp.concatenate([d_k, d_v], axis=1).astype(BF16)
        kvp[n % 2, 0, n // 2] = both[0:S]
        kvp[n % 2, 1, n // 2] = both[S:]
        return 0

    lax.fori_loop(0, 4, keys_back, 0)
    for i in range(2):
        send(kp + i, kvp.at[i, 1 - core], kvp_core.at[i], partner)

    k4 = slots(2)

    def query_back(i, _):
        rows = pl.ds(pl.multiple_of(i * half, half), half)
        part = contract_last(dq[rows], wa[:, 0:HD]).astype(BF16)
        p4[i, 0] = part[0:S]
        p4[i, 1] = part[S:]
        copy(k4 + i, p4.at[i, 1 - core], p4_core.at[i], partner).start()
        return 0

    lax.fori_loop(0, 2, query_back, 0)

    arrive(kp + (1 - y), kvp_core.at[1 - y])
    kvp_sum[...] = (kvp[1 - y, core].astype(F32) + kvp_core[1 - y].astype(F32)).astype(BF16)
    send(kp + 2, kvp_sum, kvp_chip, chip_of(1 - y, 2))
    kc = sum4(k4)
    arrive(kp + y, kvp_core.at[y])
    arrive(kp + 2, kvp_chip)
    d_left = (
        kvp[y, core, 0].astype(F32) + kvp_core[y, 0].astype(F32) + kvp_chip[0].astype(F32)
    )
    kt = slots(1)
    ret_out[...] = d_left.astype(BF16)

    @pl.when(c > 0)
    def _():
        copy(kt, ret_out, ret_in, {"context": c - 1}).start()

    weight_grad(1, xg, gel)
    weight_push(2)

    @pl.when(c < C - 1)
    def _():
        arrive(kt, ret_in)

    @pl.when(c == C - 1)
    def _():
        ret_in[...] = jnp.zeros((S, 2 * HD), BF16)

    d_kv = (
        kvp[y, core, 1].astype(F32)
        + kvp_core[y, 1].astype(F32)
        + kvp_chip[1].astype(F32)
        + ret_in[...].astype(F32)
    )
    raw = kraw[shard]
    d_raw, gain_k = rms_backward(
        turn_back(d_kv[:, :HD], cosine[shard], sine[shard]), raw, rms_factor(raw), head_gain(1)
    )
    d_kv = jnp.concatenate([d_raw, d_kv[:, HD:]], axis=1).astype(BF16)
    kq = share4(dkv, d_kv)
    d_normed = finish4(kc) + contract_last(d_kv, wa[:, HD : 3 * HD])
    copy(kc, p4_sum, p4_chip, chip_of(1 - y, 2)).wait_send()
    for i in range(2):
        copy(k4 + i, p4.at[i, 1 - core], p4_core.at[i], partner).wait_send()
    values = act[shard].astype(F32)
    d_input, gain_0 = rms_backward(d_normed, values, rms_factor(values), gain(0))
    ki = share4(input_all, (dhid[...] + d_input).astype(BF16))
    gain_mine[0:1] = gain_0
    gain_mine[4:8] = jnp.zeros((4, D), F32)
    gain_mine[4:5, 0:HD] = gain_q
    gain_mine[5:6, 0:HD] = gain_k
    kn = slots(4 + 1 + C)
    for i in range(1, 4):
        send(kn + i, gain_mine, gain_tensor.at[i], {"tensor": (t + i) % 4})

    meet4(kq, dkv)
    kv_cols = pl.ds(pl.multiple_of(t * LANES, LANES), LANES)

    def attn_grad(n, _):
        cols = pl.ds(pl.multiple_of(n * LANES, LANES), LANES)
        rows = pl.ds(pl.multiple_of(n * LANES, LANES), LANES)
        left = nrm[:, cols]
        ga[rows, 0:HD] = contract_first(
            db[:, :, :, cols].reshape(T, LANES), mix[...]
        ).astype(BF16)
        ga[rows, HD : 2 * HD] = contract_first(left, dq[...]).astype(BF16)
        ga[rows, 2 * HD :] = contract_first(
            left, dkv[:, :, :, kv_cols].reshape(T, LANES)
        ).astype(BF16)
        return 0

    lax.fori_loop(0, D // LANES, attn_grad, 0)
    ke = slots(1 + C)
    send(ke, ga.at[theirs_x], ga_x, across)
    weight_push(0)
    weight_push(1)
    total = gain_mine[...]
    for i in range(1, 4):
        arrive(kn + i, gain_tensor.at[i])
    for i in range(1, 4):
        total = total + gain_tensor[i]
    gain_tensor[0] = total
    send(kn, gain_tensor.at[0], gain_x.at[0], across)
    arrive(ke, ga_x)
    ga[mine_x] = (ga[mine_x].astype(F32) + ga_x[...].astype(F32)).astype(BF16)
    for step in range(1, C):
        send(ke + step, ga.at[rows_of(f, (c + step) % C)], ga_z.at[step - 1], along(step))
    arrive(kn, gain_x.at[0])
    gain_x[1] = total + gain_x[0]
    for step in range(1, C):
        send(kn + 4 + step, gain_x.at[1], gain_z.at[step], along(step))
    attn = ga[rows_of(f, c)].astype(F32)
    for step in range(1, C):
        arrive(ke + step, ga_z.at[step - 1])
        attn = attn + ga_z[step - 1].astype(F32)
    out_attn[...] = attn[:, 0 : 2 * HD]
    kvg[t] = attn[:, 2 * HD :]
    kh = slots(4)
    for i in range(1, 4):
        send(kh + i, kvg.at[t], kvg.at[t], {"tensor": (t + i) % 4})
    total = gain_x[1]
    for step in range(1, C):
        arrive(kn + 4 + step, gain_z.at[step])
        total = total + gain_z[step]
    out_gains[...] = total
    meet4(kr, block_all)
    save_block = pltpu.make_async_copy(block_all, out_block, ls.at[3])
    save_block.start()
    meet4(ki, input_all)
    save_input = pltpu.make_async_copy(input_all, out_input, ls.at[4])
    save_input.start()
    for w in (2, 0, 1):
        weight_end(w)
    for i in range(1, 4):
        arrive(kh + i, kvg.at[(t - i + 4) % 4])
    out_kv[...] = kvg[...]
    save_block.wait()
    save_input.wait()
    settle()

    @pl.when(c < C - 1)
    def _():
        copy(ks, seg_row, seg_left, {"context": c + 1}).wait_send()
        copy(kk, kv.at[own_half], kv.at[my_half], {"context": c + 1}).wait_send()

    @pl.when(c > 0)
    def _():
        copy(kt, ret_out, ret_in, {"context": c - 1}).wait_send()


def fused(
    mesh,
    activations,
    positions,
    seg_ids,
    norm_gains,
    head_gains,
    w_query,
    w_keyval,
    w_out,
    w_gateup,
    w_down,
    cotangent,
):
    C = mesh.shape["context"]
    T, D = activations.shape[1:]
    R, units = w_down.shape
    U = -(-units // (2 * LANES)) * LANES
    S = T // 4
    narrow = head_gains.shape[1]
    gains = jnp.concatenate(
        [
            norm_gains.T,
            jnp.pad(head_gains.T, ((0, R - narrow), (0, 0))),
            jnp.zeros((R, LANES - 6), BF16),
        ],
        axis=1,
    )
    w_attn = jnp.concatenate([w_query, w_keyval, w_out, gains], axis=1)
    both = jnp.concatenate([w_gateup, w_down[:, None]], axis=1)
    both = jnp.pad(both, ((0, 0), (0, 0), (0, 2 * U - units)))
    w_ff = both.reshape(R, 3, 2, U).transpose(2, 1, 0, 3)
    freqs = jnp.power(10000.0, -jnp.arange(HD // 2, dtype=F32) * 2.0 / HD)
    angles = positions[0].astype(F32)[:, None] * freqs[None, :]
    seg_row = jnp.broadcast_to(seg_ids, (8, T))
    seg_col = seg_ids[0][:, None]
    operands = (
        activations[0],
        jnp.cos(angles),
        jnp.sin(angles),
        seg_row,
        seg_col,
        cotangent[0],
        w_attn,
        w_ff,
    )
    scratch = [
        pltpu.VMEM((S, D), BF16),
        pltpu.VMEM((D, D), BF16),
        pltpu.VMEM((3, D, U), BF16),
        pltpu.VMEM((8, T), jnp.int32),
        pltpu.VMEM((8, D), F32),
        pltpu.VMEM((8, HD), F32),
        pltpu.VMEM((T, D), BF16),
        pltpu.VMEM((T, HD), F32),
        pltpu.VMEM((T, HD), F32),
        pltpu.VMEM((T, HD), BF16),
        pltpu.VMEM((2 * T, 2 * HD), BF16),
        pltpu.VMEM((T, 2 * T), F32),
        pltpu.VMEM((T, HD), BF16),
        pltpu.VMEM((2, 2, S, D), BF16),
        pltpu.VMEM((2, S, D), BF16),
        pltpu.VMEM((S, D), BF16),
        pltpu.VMEM((S, D), BF16),
        pltpu.VMEM((S, D), F32),
        pltpu.VMEM((S, D), F32),
        pltpu.VMEM((4, 2, S, D), BF16),
        pltpu.VMEM((4, 2 * S, U), BF16),
        pltpu.VMEM((4, 2 * S, U), BF16),
        pltpu.VMEM((4, 2 * S, U), BF16),
        pltpu.VMEM((4, 2, S, D), BF16),
        pltpu.VMEM((4, S, D), BF16),
        pltpu.VMEM((3, S, D), BF16),
        pltpu.VMEM((3, S, D), BF16),
        pltpu.VMEM((4, 2, S, D), BF16),
        pltpu.VMEM((S, D), F32),
        pltpu.VMEM((2, 2, S, D), BF16),
        pltpu.VMEM((T, 2 * T), BF16),
        pltpu.VMEM((T, HD), BF16),
        pltpu.VMEM((T, HD), BF16),
        pltpu.VMEM((2, 2, 2, S, 2 * HD), BF16),
        pltpu.VMEM((2, 2, S, 2 * HD), BF16),
        pltpu.VMEM((2, S, 2 * HD), BF16),
        pltpu.VMEM((2, S, 2 * HD), BF16),
        pltpu.VMEM((S, 2 * HD), BF16),
        pltpu.VMEM((S, 2 * HD), BF16),
        pltpu.VMEM((2, 2, S, 2 * HD), BF16),
        pltpu.VMEM((3, C * R, U), BF16),
        pltpu.VMEM((C - 1, 3, R, U), BF16),
        pltpu.VMEM((D, 2 * HD + LANES), BF16),
        pltpu.VMEM((C * R, 2 * HD + LANES), BF16),
        pltpu.VMEM((C - 1, R, 2 * HD + LANES), BF16),
        pltpu.VMEM((4, R, LANES), F32),
        pltpu.VMEM((2, R, U), F32),
        pltpu.VMEM((8, D), F32),
        pltpu.VMEM((4, 8, D), F32),
        pltpu.VMEM((2, 8, D), F32),
        pltpu.VMEM((C, 8, D), F32),
        pltpu.VMEM((2, 2, S, D), BF16),
        pltpu.VMEM((2, 2, S, D), BF16),
        pltpu.SemaphoreType.DMA((SEMAPHORES,)),
        pltpu.SemaphoreType.DMA((SEMAPHORES,)),
        pltpu.SemaphoreType.DMA((6,)),
    ]
    vmem = pl.BlockSpec(memory_space=pltpu.VMEM)
    anywhere = pl.BlockSpec(memory_space=pl.ANY)
    results = (
        jax.ShapeDtypeStruct((2, 2, S, D), BF16),
        jax.ShapeDtypeStruct((2, 2, S, D), BF16),
        jax.ShapeDtypeStruct((8, D), F32),
        jax.ShapeDtypeStruct((3, 2, R, U), F32),
        jax.ShapeDtypeStruct((R, 2 * HD), F32),
        jax.ShapeDtypeStruct((4, R, LANES), F32),
    )
    sizes = {"context": C, "tokens": T, "width": D, "rows": R, "units": U}
    block_out, input_grad, gain_sums, ff_grads, attn_grads, kv_grads = pl.pallas_call(
        functools.partial(fused_kernel, sizes),
        out_shape=results,
        in_specs=[vmem] * 5 + [anywhere] * 3,
        out_specs=[anywhere] * 2 + [vmem, anywhere, vmem, vmem],
        scratch_shapes=scratch,
        compiler_params=pltpu.CompilerParams(
            collective_id=0, has_side_effects=True, vmem_limit_bytes=67043328
        ),
    )(*operands)
    owner = lax.axis_index(("fsdp", "context"))
    norm_grad = lax.dynamic_slice(gain_sums, (0, owner * R), (4, R))
    head_grad = lax.dynamic_slice(gain_sums, (4, owner * narrow), (2, narrow))
    ff = ff_grads.transpose(2, 0, 1, 3).reshape(R, 3, 2 * U)[:, :, :units]
    return (
        block_out.reshape(1, T, D),
        input_grad.reshape(1, T, D),
        norm_grad,
        head_grad,
        attn_grads[:, HD:],
        kv_grads.transpose(1, 0, 2).reshape(R, 2 * HD),
        attn_grads[:, :HD],
        ff[:, :2],
        ff[:, 2],
    )


def block(mesh, *arrays):
    tokens, rows = arrays[0].shape[1], arrays[9].shape[0]
    fits = (
        mesh.shape["fsdp"] == 2
        and mesh.shape["tensor"] == 4
        and mesh.shape["context"] == 4
        and tokens == WINDOW
        and rows % 16 == 0
        and arrays[5].shape[1] == HD
        and arrays[6].shape[1] == 4 * LANES
    )
    return fused(mesh, *arrays) if fits else shards(*arrays)


def shards(
    activations,
    positions,
    seg_ids,
    norm_gains,
    head_gains,
    w_query,
    w_keyval,
    w_out,
    w_gateup,
    w_down,
    cotangent,
):
    tokens = activations.shape[1]
    local_heads = w_query.shape[1] // HD
    inputs = activations[0].astype(jnp.float32)
    places = positions[0]
    documents = seg_ids[0]
    gains_all, heads_all, query_all, keyval_all, out_all = (
        lax.all_gather(norm_gains, ("fsdp", "context"), axis=1, tiled=True),
        lax.all_gather(head_gains, ("fsdp", "context"), axis=1, tiled=True),
        lax.all_gather(w_query, ("fsdp", "context"), axis=0, tiled=True),
        lax.all_gather(w_keyval, ("fsdp", "context"), axis=0, tiled=True),
        lax.all_gather(w_out, ("fsdp", "context"), axis=0, tiled=True),
    )
    gains_f = gains_all.astype(jnp.float32)
    heads_f = heads_all.astype(jnp.float32)
    normed_f, input_back = jax.vjp(rms_norm, inputs, gains_f[0])
    normed = normed_f.astype(jnp.bfloat16)
    query_raw = jnp.dot(normed, query_all, preferred_element_type=jnp.float32).reshape(
        tokens, local_heads, HD
    )
    keyval_raw = jnp.dot(normed, keyval_all, preferred_element_type=jnp.float32)

    def prepare(raw_heads, head_gain):
        return rotate(rms_norm(raw_heads, head_gain), places)

    query_rot, query_back = jax.vjp(prepare, query_raw, heads_f[0])
    key_rot, key_back = jax.vjp(prepare, keyval_raw[:, None, :HD], heads_f[1])
    queries = query_rot.astype(jnp.bfloat16)
    own_keyval = jnp.concatenate([key_rot[:, 0], keyval_raw[:, HD:]], axis=1).astype(jnp.bfloat16)
    labels = jnp.stack([places, documents])
    keep_from = tokens - tokens
    left_keyval, left_labels = from_behind((own_keyval, labels), "context", 1)
    keys_all = jnp.concatenate([left_keyval, own_keyval], axis=0)
    key_places = jnp.concatenate([left_labels[0], places])
    key_documents = jnp.concatenate([left_labels[1], documents])
    has_left = lax.axis_index("context") > 0
    key_live = jnp.concatenate([jnp.full((tokens,), has_left), jnp.ones((tokens,), dtype=bool)])
    scale_factor = HD ** (-0.5)
    block_rows = 512
    block_starts = jnp.arange(tokens // block_rows) * block_rows

    def block_scores():
        spacing = places[:, None] - key_places[None, :]
        visible = (
            key_live[None, :]
            & (documents[:, None] == key_documents[None, :])
            & (spacing >= 0)
            & (spacing < WINDOW)
        )
        raw_scores = (
            jnp.einsum("qhd,kd->hqk", queries, keys_all[:, :HD], preferred_element_type=jnp.float32)
            * scale_factor
        )
        return (jnp.where(visible[None], raw_scores, -1e30), keys_all, queries)

    def forward_block(start):
        scores, near_keyval, query_block = block_scores()
        row_top = jnp.max(scores, axis=-1, keepdims=True)
        raised = jnp.exp(scores - row_top)
        row_total = jnp.sum(raised, axis=-1, keepdims=True)
        probs = raised / row_total
        mixed_block = jnp.einsum(
            "hqk,kd->qhd",
            probs.astype(jnp.bfloat16),
            near_keyval[:, HD:],
            preferred_element_type=jnp.float32,
        )
        return (mixed_block.astype(jnp.bfloat16), row_top + jnp.log(row_total))

    mixed_blocks, log_blocks = lax.map(forward_block, block_starts)
    mixed_low = mixed_blocks.reshape(tokens, local_heads * HD)
    branch = lax.psum(contract_last(mixed_low, out_all).astype(jnp.bfloat16), "tensor").astype(jnp.float32)
    post_attn, post_attn_back = jax.vjp(rms_norm, branch, gains_f[1])
    hidden = inputs + post_attn
    normed_mlp_f, pre_mlp_back = jax.vjp(rms_norm, hidden, gains_f[2])
    normed_mlp = normed_mlp_f.astype(jnp.bfloat16)
    columns = normed_mlp
    gate_up = jnp.einsum(
        "bn,nkf->bkf",
        columns,
        lax.all_gather(w_gateup, ("fsdp", "context"), axis=0, tiled=True),
        preferred_element_type=jnp.float32,
    )
    active_f, glu_back = jax.vjp(glu, gate_up)
    active = active_f.astype(jnp.bfloat16)
    down = lax.psum(
        contract_last(
            active, lax.all_gather(w_down, ("fsdp", "context"), axis=0, tiled=True)
        ).astype(jnp.bfloat16),
        "tensor",
    ).astype(jnp.float32)
    post_mlp, post_mlp_back = jax.vjp(rms_norm, down, gains_f[3])
    result = hidden + post_mlp
    grad_out = cotangent[0].astype(jnp.float32)
    d_down, gain_post_mlp = post_mlp_back(grad_out)
    down_low = d_down.astype(jnp.bfloat16)
    columns = down_low
    d_active = jnp.dot(
        columns,
        lax.all_gather(w_down, ("fsdp", "context"), axis=0, tiled=True),
        preferred_element_type=jnp.float32,
    )
    d_gate_up = glu_back(d_active)[0].astype(jnp.bfloat16)
    d_normed_part = jnp.einsum(
        "bkf,nkf->bn",
        d_gate_up,
        lax.all_gather(w_gateup, ("fsdp", "context"), axis=0, tiled=True),
        preferred_element_type=jnp.float32,
    )
    d_normed_mlp = lax.psum(d_normed_part.astype(jnp.bfloat16), "tensor").astype(jnp.float32)
    d_hidden_norm, gain_pre_mlp = pre_mlp_back(d_normed_mlp)
    d_hidden = grad_out + d_hidden_norm
    features = normed_mlp
    grad_cols = down_low
    gate_up_term = jnp.einsum(
        "bn,bkf->nkf", features, d_gate_up, preferred_element_type=jnp.float32
    )
    down_term = contract_first(grad_cols, active)
    scatter = lambda part: lax.psum_scatter(
        part.astype(jnp.bfloat16), ("fsdp", "context"), scatter_dimension=0, tiled=True
    ).astype(jnp.float32)
    gate_grad = scatter(gate_up_term[:, 0])
    up_grad = scatter(gate_up_term[:, 1])
    down_grad = scatter(down_term)
    d_branch, gain_post_attn = post_attn_back(d_hidden)
    branch_low = d_branch.astype(jnp.bfloat16)
    d_mixed = jnp.dot(branch_low, out_all, preferred_element_type=jnp.float32)
    d_mixed_low = d_mixed.astype(jnp.bfloat16).reshape(tokens, local_heads, HD)

    def backward_block(carry, item):
        start, log_block = item
        scores, near_keyval, query_block = block_scores()
        probs_again = jnp.exp(scores - log_block)
        d_probs = jnp.einsum(
            "qhd,kd->hqk", d_mixed_low, near_keyval[:, HD:], preferred_element_type=jnp.float32
        )
        row_inner = jnp.sum(probs_again * d_probs, axis=-1, keepdims=True)
        d_scores = (probs_again * (d_probs - row_inner)).astype(jnp.bfloat16)
        d_query_block = (
            jnp.einsum(
                "hqk,kd->qhd", d_scores, near_keyval[:, :HD], preferred_element_type=jnp.float32
            )
            * scale_factor
        )
        d_keys = (
            jnp.einsum("hqk,qhd->kd", d_scores, query_block, preferred_element_type=jnp.float32)
            * scale_factor
        )
        d_values = jnp.einsum(
            "hqk,qhd->kd",
            probs_again.astype(jnp.bfloat16),
            d_mixed_low,
            preferred_element_type=jnp.float32,
        )
        updated = carry + jnp.concatenate([d_keys, d_values], axis=1)
        return (updated, d_query_block)

    d_keyval, d_query_blocks = lax.scan(
        backward_block,
        jnp.zeros((tokens + tokens, 2 * HD), jnp.float32),
        (block_starts, log_blocks),
    )
    d_queries = d_query_blocks.reshape(tokens, local_heads, HD)
    returned = from_behind(d_keyval[:tokens].astype(jnp.bfloat16), "context", -1).astype(
        jnp.float32
    )
    own_grad = d_keyval[tokens:].at[keep_from:].add(returned)
    d_query_raw, gain_query = query_back(d_queries)
    d_query_low = d_query_raw.reshape(tokens, local_heads * HD).astype(jnp.bfloat16)
    d_normed_query, keyval_grad, gain_query_all = (
        lax.psum(contract_last(d_query_low, query_all).astype(jnp.bfloat16), "tensor").astype(
            jnp.float32
        ),
        lax.psum(own_grad.astype(jnp.bfloat16), "tensor").astype(jnp.float32),
        lax.psum(gain_query.astype(jnp.bfloat16), "tensor").astype(jnp.float32),
    )
    d_key_raw, gain_key = key_back(keyval_grad[:, None, :HD])
    d_keyval_low = jnp.concatenate([d_key_raw[:, 0], keyval_grad[:, HD:]], axis=1).astype(
        jnp.bfloat16
    )
    d_normed = d_normed_query + contract_last(d_keyval_low, keyval_all)
    d_input_norm, gain_input = input_back(d_normed)
    input_total = d_hidden + d_input_norm
    features = normed
    grad_cols = branch_low
    attn_grads = lax.psum_scatter(
        jnp.stack(
            [contract_first(features, d_query_low), contract_first(grad_cols, mixed_low)], axis=1
        ).astype(jnp.bfloat16),
        ("fsdp", "context"),
        scatter_dimension=0,
        tiled=True,
    ).astype(jnp.float32)
    keyval_term = contract_first(normed, d_keyval_low)
    gain_terms = jnp.stack([gain_input, gain_post_attn, gain_pre_mlp, gain_post_mlp])
    head_terms = jnp.stack([gain_query_all, gain_key])
    gain_grad, head_grad, keyval_weight_grad = (
        lax.psum_scatter(
            gain_terms.astype(jnp.bfloat16), ("fsdp", "context"), scatter_dimension=1, tiled=True
        ).astype(jnp.float32),
        lax.psum_scatter(
            head_terms.astype(jnp.bfloat16), ("fsdp", "context"), scatter_dimension=1, tiled=True
        ).astype(jnp.float32),
        lax.psum_scatter(
            keyval_term.astype(jnp.bfloat16), ("fsdp", "context"), scatter_dimension=0, tiled=True
        ).astype(jnp.float32),
    )
    return (
        result[None].astype(jnp.bfloat16),
        input_total[None].astype(jnp.bfloat16),
        gain_grad,
        head_grad,
        attn_grads[:, 0],
        keyval_weight_grad,
        attn_grads[:, 1],
        jnp.stack([gate_grad, up_grad], axis=1),
        down_grad,
    )


def solution(mesh):
    return jax.shard_map(
        functools.partial(block, mesh),
        mesh=mesh,
        in_specs=(
            P("fsdp", "context", None),
            P("fsdp", "context"),
            P("fsdp", "context"),
            P(None, ("fsdp", "context")),
            P(None, ("fsdp", "context")),
            P(("fsdp", "context"), "tensor"),
            P(("fsdp", "context"), None),
            P(("fsdp", "context"), "tensor"),
            P(("fsdp", "context"), None, "tensor"),
            P(("fsdp", "context"), "tensor"),
            P("fsdp", "context", None),
        ),
        out_specs=(
            P("fsdp", "context", None),
            P("fsdp", "context", None),
            P(None, ("fsdp", "context")),
            P(None, ("fsdp", "context")),
            P(("fsdp", "context"), "tensor"),
            P(("fsdp", "context"), None),
            P(("fsdp", "context"), "tensor"),
            P(("fsdp", "context"), None, "tensor"),
            P(("fsdp", "context"), "tensor"),
        ),
        check_vma=False,
    )
```

```python
import functools

import jax
import jax.numpy as jnp
from jax import lax
from jax.experimental import pallas as pl
from jax.experimental.pallas import tpu as pltpu
from jax.sharding import PartitionSpec as P

HD = 256
WINDOW = 512


EPSILON = 1e-06


def from_behind(block, axis, distance):
    devices = range(lax.axis_size(axis))
    route = [(i - distance, i) for i in devices if i - distance in devices]
    return lax.ppermute(block, axis, route)


def rms_norm(values, gain):
    factor = lax.rsqrt(jnp.mean(values * values, axis=-1, keepdims=True) + EPSILON)
    return values * factor * gain


def rotate(tensor, places):
    width_all = tensor.shape[-1]
    half_width = width_all // 2
    freqs = jnp.power(10000.0, -jnp.arange(half_width, dtype=jnp.float32) * 2.0 / width_all)
    angles = places.astype(jnp.float32)[:, None] * freqs[None, :]
    cosine = jnp.cos(angles)[:, None, :]
    sine = jnp.sin(angles)[:, None, :]
    first_half = tensor[..., :half_width]
    second_half = tensor[..., half_width:]
    return jnp.concatenate(
        [first_half * cosine - second_half * sine, second_half * cosine + first_half * sine],
        axis=-1,
    )


def glu(gate_up):
    return jax.nn.gelu(gate_up[:, 0], approximate=True) * gate_up[:, 1]


def contract_last(left_side, right_side):
    return lax.dot_general(
        left_side, right_side, (((1,), (1,)), ((), ())), preferred_element_type=jnp.float32
    )


def contract_first(left_side, right_side):
    return lax.dot_general(
        left_side, right_side, (((0,), (0,)), ((), ())), preferred_element_type=jnp.float32
    )


MESH = pl.DeviceIdType.MESH
F32 = jnp.float32
BF16 = jnp.bfloat16
LANES = 128
SEMAPHORES = 160


def mm(left, right):
    return jnp.dot(left, right, preferred_element_type=F32)


def rms_factor(values):
    return lax.rsqrt(jnp.mean(values * values, axis=-1, keepdims=True) + EPSILON)


def rms_backward(grad, values, factor, gain):
    unit = values * factor
    scaled = grad * gain
    inner = jnp.mean(scaled * unit, axis=-1, keepdims=True)
    return factor * (scaled - unit * inner), jnp.sum(grad * unit, axis=0, keepdims=True)


def turn(values, cosine, sine):
    half = values.shape[-1] // 2
    first, second = values[:, :half], values[:, half:]
    return jnp.concatenate([first * cosine - second * sine, second * cosine + first * sine], axis=1)


def turn_back(values, cosine, sine):
    half = values.shape[-1] // 2
    first, second = values[:, :half], values[:, half:]
    return jnp.concatenate([first * cosine + second * sine, second * cosine - first * sine], axis=1)


def fused_kernel(
    sizes,
    act,
    cosine,
    sine,
    seg_row,
    seg_col,
    cot_all,
    w_query,
    w_keyval,
    w_out,
    gain_cols,
    w_ff,
    out_block,
    out_input,
    out_gains,
    out_ff,
    out_attn,
    out_kv,
    cot,
    wa,
    wf,
    seg_left,
    gain_rows,
    head_rows,
    nrm,
    qraw,
    kv_raw,
    qs,
    kv,
    probs,
    mix,
    p4,
    p4_core,
    p4_sum,
    p4_chip,
    hid,
    bran,
    xg,
    gel,
    upg,
    active,
    p8,
    p8_core,
    p8_sum,
    p8_chip,
    dd,
    dhid,
    db,
    dscore,
    dmix,
    dq,
    kvp,
    kvp_core,
    kvp_sum,
    kvp_chip,
    ret_out,
    ret_in,
    dkv_mine,
    dkv_cols,
    gall_x,
    gall_z,
    ga,
    ga_x,
    ga_z,
    kvg,
    ff_stage,
    gain_mine,
    gain_tensor,
    gain_x,
    gain_z,
    block_all,
    input_all,
    ss,
    rs,
    ls,
):
    C = sizes["context"]
    T, D, R, U = sizes["tokens"], sizes["width"], sizes["rows"], sizes["units"]
    S = T // 4
    f = lax.axis_index("fsdp")
    c = lax.axis_index("context")
    t = lax.axis_index("tensor")
    y, core = t // 2, t % 2
    m = c % 2
    base = c - m
    partner = {"tensor": y * 2 + (1 - core)}
    across = {"fsdp": 1 - f}
    counter = [0]
    sent = []

    def slots(count):
        first = counter[0]
        counter[0] += count
        assert counter[0] <= SEMAPHORES
        return first

    def copy(k, src, dst, device):
        return pltpu.make_async_remote_copy(
            src_ref=src,
            dst_ref=dst,
            send_sem=ss.at[k],
            recv_sem=rs.at[k],
            device_id=device,
            device_id_type=MESH,
        )

    def send(k, src, dst, device):
        moved = copy(k, src, dst, device)
        moved.start()
        sent.append(moved)

    def arrive(k, dst):
        copy(k, dst, dst, partner).wait_recv()

    def settle():
        for moved in sent:
            moved.wait_send()
        sent.clear()

    def along(step):
        return {"context": (c + step) % C}

    def rows_of(ff, cc):
        return pl.ds(pl.multiple_of((ff * C + cc) * R, R), R)

    def chip_of(k, count):
        if count == 2:
            return {"tensor": k * 2 + core}
        return {"context": base + k // 2, "tensor": (k % 2) * 2 + core}

    barrier = pltpu.get_barrier_semaphore()
    greeted = [along(step) for step in range(1, C)] + [across]
    greeted += [{"tensor": (t + step) % 4} for step in range(1, 4)]
    greeted += [{"context": base + 1 - m, "tensor": (1 - y) * 2 + core}]
    for device in greeted:
        pl.semaphore_signal(barrier, inc=1, device_id=device, device_id_type=MESH)
    pl.semaphore_wait(barrier, len(greeted))

    mine = rows_of(f, c)
    kv_cols = pl.ds(pl.multiple_of(t * LANES, LANES), LANES)
    attn_parts = (
        (w_query, slice(0, HD)),
        (w_keyval.at[:, kv_cols], slice(HD, HD + LANES)),
        (w_out, slice(HD + LANES, 2 * HD + LANES)),
        (gain_cols, slice(2 * HD + LANES, 2 * HD + 2 * LANES)),
    )
    q_cols, kv_part, o_cols = (cols for _, cols in attn_parts[:3])
    local = []
    for n, (part, cols) in enumerate(attn_parts):
        local.append(pltpu.make_async_copy(part, wa.at[mine, cols], ls.at[6 + n]))
        local[-1].start()
    ka = slots(4 * C)
    kar = slots(C)
    for step in range(1, C):
        for n, (part, cols) in enumerate(attn_parts):
            send(ka + 4 * step + n, part, wa.at[mine, cols], along(step))
    for n, (part, cols) in enumerate(attn_parts):
        send(ka + n, part, wa.at[mine, cols], across)
    ks = slots(1)

    @pl.when(c < C - 1)
    def _():
        copy(ks, seg_row, seg_left, {"context": c + 1}).start()

    kf = slots(6 * C)

    def send_ff(w):
        k = kf + 2 * C * w
        for step in range(1, C):
            send(k + step, w_ff.at[(c + step) % 2, w], wf.at[w, mine], along(step))
        send(k, w_ff.at[m, w], wf.at[w, mine], across)

    def relay_ff(w, step):
        k = kf + 2 * C * w
        part = wf.at[w, rows_of(f, (c - step + C) % C)]
        arrive(k + step, part)
        copy(k + C + step, part, part, across).start()

    def meet_ff(w):
        k = kf + 2 * C * w
        arrive(k, wf.at[w, rows_of(1 - f, c)])
        for step in range(1, C):
            arrive(k + C + step, wf.at[w, rows_of(1 - f, (c - step + C) % C)])

    def settle_ff(w):
        k = kf + 2 * C * w
        for step in range(1, C):
            part = wf.at[w, rows_of(f, (c - step + C) % C)]
            copy(k + C + step, part, part, across).wait_send()

    send_ff(0)
    shard = pl.ds(pl.multiple_of(t * S, S), S)
    own_cot = pltpu.make_async_copy(cot_all.at[shard], cot, ls.at[2])
    own_cot.start()
    own_ff = pltpu.make_async_copy(w_ff.at[m], wf.at[:, mine], ls.at[1])
    own_ff.start()
    for step in range(1, C):
        other = rows_of(f, (c - step + C) % C)
        for n, (_, cols) in enumerate(attn_parts):
            arrive(ka + 4 * step + n, wa.at[other, cols])
        send(kar + step, wa.at[other], wa.at[other], across)
    for moved in local:
        moved.wait()
    for n, (_, cols) in enumerate(attn_parts):
        arrive(ka + n, wa.at[rows_of(1 - f, c), cols])
    for step in range(1, C):
        arrive(kar + step, wa.at[rows_of(1 - f, (c - step + C) % C)])

    @pl.when(c > 0)
    def _():
        arrive(ks, seg_left)

    @pl.when(c == 0)
    def _():
        seg_left[...] = jnp.full(seg_left.shape, -1, jnp.int32)
        kv[0:T] = jnp.zeros((T, 2 * HD), BF16)

    gain_t = jnp.transpose(wa[:, 2 * HD + LANES :].astype(F32))
    gain_rows[...] = gain_t[0:8]
    narrow = HD // (2 * C)
    here = lax.broadcasted_iota(jnp.int32, (D, HD), 0)
    want = lax.broadcasted_iota(jnp.int32, (D, HD), 1)
    shift = narrow.bit_length() - 1
    want = lax.shift_right_logical(want, shift) * R + (want & (narrow - 1))
    pick = jnp.where(here == want, 1.0, 0.0).astype(BF16)
    head_rows[...] = mm(gain_t[0:16].astype(BF16), pick)[0:8]

    def gain(index):
        return gain_rows[index : index + 1]

    def head_gain(index):
        return head_rows[4 + index : 5 + index]

    half = T // 2

    def project(i, _):
        rows = pl.ds(pl.multiple_of(i * half, half), half)
        values = act[rows].astype(F32)
        low = (values * rms_factor(values) * gain(0)).astype(BF16)
        nrm[rows] = low
        kv_raw[t, rows] = mm(low, wa[:, kv_part]).astype(BF16)
        return 0

    lax.fori_loop(0, 2, project, 0)
    ku = slots(4)
    for i in range(1, 4):
        send(ku + i, kv_raw.at[t], kv_raw.at[t], {"tensor": (t + i) % 4})

    def query(i, _):
        rows = pl.ds(pl.multiple_of(i * half, half), half)
        raw_q = mm(nrm[rows], wa[:, q_cols])
        qraw[rows] = raw_q
        qs[rows] = turn(
            raw_q * rms_factor(raw_q) * head_gain(0), cosine[rows], sine[rows]
        ).astype(BF16)
        return 0

    lax.fori_loop(0, 2, query, 0)
    for i in range(1, 4):
        arrive(ku + i, kv_raw.at[(t - i + 4) % 4])

    def key(i, _):
        rows = pl.ds(pl.multiple_of(i * half, half), half)
        raw_k = jnp.concatenate([kv_raw[0, rows], kv_raw[1, rows]], axis=1).astype(F32)
        own = pl.ds(pl.multiple_of(T + i * half, half), half)
        kv[own, 0:HD] = turn(
            raw_k * rms_factor(raw_k) * head_gain(1), cosine[rows], sine[rows]
        ).astype(BF16)
        kv[own, HD : HD + LANES] = kv_raw[2, rows]
        kv[own, HD + LANES :] = kv_raw[3, rows]
        return 0

    lax.fori_loop(0, 2, key, 0)
    kk = slots(2)
    my_half = pl.ds(pl.multiple_of(core * half, half), half)
    other_half = pl.ds(pl.multiple_of((1 - core) * half, half), half)
    own_half = pl.ds(pl.multiple_of(T + core * half, half), half)

    @pl.when(c < C - 1)
    def _():
        copy(kk, kv.at[own_half], kv.at[my_half], {"context": c + 1}).start()

    send_ff(1)
    for step in range(1, C):
        relay_ff(0, step)

    @pl.when(c > 0)
    def _():
        arrive(kk, kv.at[my_half])
        moved = copy(kk + 1, kv.at[my_half], kv.at[my_half], partner)
        moved.start()
        arrive(kk + 1, kv.at[other_half])
        moved.wait_send()

    scale = HD**-0.5
    no_left = jnp.where(c > 0, 0, 2 * T)
    k4 = slots(2)

    def attend(i, _):
        rows = pl.ds(pl.multiple_of(i * half, half), half)
        q = qs[rows]
        labels = seg_col[rows]
        row = lax.broadcasted_iota(jnp.int32, (half, T), 0) + i * half
        col = lax.broadcasted_iota(jnp.int32, (half, T), 1)
        left = contract_last(q, kv[0:T, 0:HD]) * scale
        left = jnp.where((labels == seg_left[0:1]) & (col > row + no_left), left, -1e30)
        own = contract_last(q, kv[T:, 0:HD]) * scale
        own = jnp.where((labels == seg_row[0:1]) & (col <= row), own, -1e30)
        top = jnp.maximum(
            jnp.max(left, axis=1, keepdims=True), jnp.max(own, axis=1, keepdims=True)
        )
        left, own = jnp.exp(left - top), jnp.exp(own - top)
        total = jnp.sum(left, axis=1, keepdims=True) + jnp.sum(own, axis=1, keepdims=True)
        left, own = left / total, own / total
        probs[rows, 0:T] = left
        probs[rows, T:] = own
        mixed = mm(left.astype(BF16), kv[0:T, HD:]) + mm(own.astype(BF16), kv[T:, HD:])
        mixed = mixed.astype(BF16)
        mix[rows] = mixed
        part = contract_last(mixed, wa[:, o_cols]).astype(BF16)
        p4[i, 0] = part[0:S]
        p4[i, 1] = part[S:]
        copy(k4 + i, p4.at[i, 1 - core], p4_core.at[i], partner).start()
        return 0

    lax.fori_loop(0, 2, attend, 0)

    def sum4(k):
        kc = slots(1)
        arrive(k + (1 - y), p4_core.at[1 - y])
        p4_sum[...] = (
            p4[1 - y, core].astype(F32) + p4_core[1 - y].astype(F32)
        ).astype(BF16)
        copy(kc, p4_sum, p4_chip, chip_of(1 - y, 2)).start()
        arrive(k + y, p4_core.at[y])
        return kc

    def finish4(kc):
        arrive(kc, p4_chip)
        return (
            p4[y, core].astype(F32)
            + p4_core[y].astype(F32)
            + p4_chip[...].astype(F32)
        )

    kc = sum4(k4)
    relay_ff(1, 1)
    relay_ff(1, 2)
    branch = finish4(kc)
    copy(kc, p4_sum, p4_chip, chip_of(1 - y, 2)).wait_send()
    for i in range(2):
        copy(k4 + i, p4.at[i, 1 - core], p4_core.at[i], partner).wait_send()

    bran[...] = branch
    hidden = act[shard].astype(F32) + branch * rms_factor(branch) * gain(1)
    hid[...] = hidden
    low = (hidden * rms_factor(hidden) * gain(2)).astype(BF16)

    me = m * 2 + y

    def gather8(full, value):
        kg = slots(8)
        full[me, core] = value
        send(kg + 4, full.at[me, core], full.at[me, core], partner)
        for i in range(1, 4):
            send(kg + i, full.at[me, core], full.at[me, core], chip_of((me + i) % 4, 4))
        return kg

    def pass8(kg, full, i):
        k = (me - i + 4) % 4
        arrive(kg + i, full.at[k, core])
        copy(kg + 4 + i, full.at[k, core], full.at[k, core], partner).start()

    def meet8(kg, full, i):
        k = (me - i + 4) % 4
        arrive(kg + 4 + i, full.at[k, 1 - core])

    def settle8(kg, full):
        for i in range(1, 4):
            k = (me - i + 4) % 4
            copy(kg + 4 + i, full.at[k, core], full.at[k, core], partner).wait_send()

    def give8(ko, i):
        k = (me - i + 4) % 4
        copy(ko + i, p8.at[k, 1 - core], p8_core.at[i], partner).start()

    def push8(ko, i):
        k = (me - i + 4) % 4
        arrive(ko + i, p8_core.at[i])
        p8_sum[i - 1] = (
            p8[k, core].astype(F32) + p8_core[i].astype(F32)
        ).astype(BF16)
        copy(ko + 4 + i, p8_sum.at[i - 1], p8_chip.at[i - 1], chip_of(k, 4)).start()

    def finish8(ko):
        arrive(ko, p8_core.at[0])
        total = p8[me, core].astype(F32) + p8_core[0].astype(F32)
        for i in range(1, 4):
            arrive(ko + 4 + i, p8_chip.at[i - 1])
            total = total + p8_chip[i - 1].astype(F32)
        for i in range(4):
            copy(ko + i, p8.at[0, 1 - core], p8_core.at[i], partner).wait_send()
        for i in range(1, 4):
            copy(ko + 4 + i, p8_sum.at[0], p8_chip.at[0], partner).wait_send()
        return total

    kx = gather8(xg, low)
    send_ff(2)
    relay_ff(1, 3)
    own_ff.wait()
    own_cot.wait()
    meet_ff(0)
    meet_ff(1)
    root = 0.7978845608028654
    ko = slots(8)

    def forward(i, _):
        k = (me - i + 4) % 4
        meet8(kx, xg, i)
        x = xg[k].reshape(2 * S, D)
        gate = mm(x, wf[0])
        up = mm(x, wf[1])

        @pl.when(i < 3)
        def _():
            pass8(kx, xg, i + 1)

        square = gate * gate
        bent = jnp.tanh(root * gate * (1.0 + 0.044715 * square))
        ramp = 0.5 * (1.0 + bent)
        gelu = gate * ramp
        slope = ramp + 0.5 * gate * (1.0 - bent * bent) * root * (1.0 + 3 * 0.044715 * square)
        gel[k] = gelu.astype(BF16)
        upg[k] = (up * slope).astype(BF16)
        active[k] = (gelu * up).astype(BF16)

        @pl.when(i > 0)
        def _():
            relay_ff(2, i)

        return 0

    lax.fori_loop(0, 4, forward, 0)
    meet_ff(2)

    def lower(i, _):
        k = (me - i + 4) % 4
        p8[k] = contract_last(active[k], wf[2]).astype(BF16).reshape(2, S, D)
        give8(ko, i)

        @pl.when(i > 1)
        def _():
            push8(ko, i - 1)

        return 0

    lax.fori_loop(0, 4, lower, 0)
    push8(ko, 3)
    settle8(kx, xg)
    down = finish8(ko)

    factor = rms_factor(down)
    grad = cot[...].astype(F32)
    result = (hid[...] + down * factor * gain(3)).astype(BF16)
    d_down, gain_3 = rms_backward(grad, down, factor, gain(3))
    gain_mine[3:4] = gain_3
    kd = gather8(dd, d_down.astype(BF16))

    def share4(full):
        kb = slots(3)
        send(kb, full.at[y, core], full.at[y, core], chip_of(1 - y, 2))
        send(kb + 1, full.at[y, core], full.at[y, core], partner)
        return kb

    def meet4(kb, full):
        arrive(kb, full.at[1 - y, core])
        send(kb + 2, full.at[1 - y, core], full.at[1 - y, core], partner)
        arrive(kb + 1, full.at[y, 1 - core])
        arrive(kb + 2, full.at[1 - y, 1 - core])

    block_all[y, core] = result
    ko2 = slots(8)

    def backward(i, _):
        k = (me - i + 4) % 4
        meet8(kd, dd, i)
        low = dd[k].reshape(2 * S, D)
        d_active = mm(low, wf[2])

        @pl.when(i < 3)
        def _():
            pass8(kd, dd, i + 1)

        d_gate = (d_active * upg[k].astype(F32)).astype(BF16)
        d_up = (d_active * gel[k].astype(F32)).astype(BF16)
        upg[k] = d_gate
        gel[k] = d_up
        p8[k] = (
            (contract_last(d_gate, wf[0]) + contract_last(d_up, wf[1]))
            .astype(BF16)
            .reshape(2, S, D)
        )
        give8(ko2, i)

        @pl.when(i > 1)
        def _():
            push8(ko2, i - 1)

        return 0

    lax.fori_loop(0, 4, backward, 0)
    push8(ko2, 3)
    settle8(kd, dd)

    settle()
    for w in range(3):
        settle_ff(w)
    gall = wf
    mine_x = pl.ds(pl.multiple_of(f * C * R, C * R), C * R)
    theirs_x = pl.ds(pl.multiple_of((1 - f) * C * R, C * R), C * R)
    chunks = (
        (2, 0, 256),
        (2, 256, 512),
        (2, 512, U),
        (0, 0, 512),
        (0, 512, U),
        (1, 0, 512),
        (1, 512, U),
    )
    kw = slots(len(chunks))
    kz = slots(len(chunks) * C)

    def weight_grad(w, left, right, early):
        def tile(n, _):
            cols = pl.ds(pl.multiple_of(n * LANES, LANES), LANES)
            block = left[:, :, :, cols].reshape(8 * S, LANES)
            gall[w, cols] = contract_first(block, right[...].reshape(8 * S, U)).astype(BF16)
            return 0

        first = D // LANES // 2
        lax.fori_loop(0, first + 1, lambda n, _: tile(n + first * (1 - f), _), 0)
        for q in early:
            weight_send(q)
        lax.fori_loop(0, first, lambda n, _: tile(n + (first + 1) * f, _), 0)

    def weight_send(q):
        w, low, high = chunks[q]
        send(kw + q, gall.at[w, theirs_x, low:high], gall_x.at[w, :, low:high], across)

    def weight_push(q):
        w, low, high = chunks[q]
        arrive(kw + q, gall_x.at[w, :, low:high])

        def add(n, _):
            rows = pl.ds(pl.multiple_of(f * C * R + n * R, R), R)
            part = pl.ds(pl.multiple_of(n * R, R), R)
            gall[w, rows, low:high] = (
                gall[w, rows, low:high].astype(F32) + gall_x[w, part, low:high].astype(F32)
            ).astype(BF16)
            return 0

        lax.fori_loop(0, C, add, 0)
        for step in range(1, C):
            send(
                kz + q * C + step,
                gall.at[w, rows_of(f, (c + step) % C), low:high],
                gall_z.at[step - 1, w, :, low:high],
                along(step),
            )

    def weight_end(w):
        for q, (chunk, low, high) in enumerate(chunks):
            for step in range(1, C):
                if chunk == w:
                    arrive(kz + q * C + step, gall_z.at[step - 1, w, :, low:high])
        same = gall[w, rows_of(f, c)].astype(F32)
        other = jnp.zeros((R, U), F32)
        for step in range(1, C):
            if step % 2:
                other = other + gall_z[step - 1, w].astype(F32)
            else:
                same = same + gall_z[step - 1, w].astype(F32)
        ff_stage[m] = same
        ff_stage[1 - m] = other
        saved = pltpu.make_async_copy(ff_stage, out_ff.at[w], ls.at[5])
        saved.start()
        saved.wait()

    weight_grad(2, dd, active, (0, 1, 2))
    d_normed = finish8(ko2)
    hidden = hid[...]
    d_hidden, gain_2 = rms_backward(d_normed, hidden, rms_factor(hidden), gain(2))
    d_hidden = cot[...].astype(F32) + d_hidden
    dhid[...] = d_hidden
    gain_mine[2:3] = gain_2
    branch = bran[...]
    d_branch, gain_1 = rms_backward(d_hidden, branch, rms_factor(branch), gain(1))
    gain_mine[1:2] = gain_1
    db[y, core] = d_branch.astype(BF16)
    kb = share4(db)
    weight_grad(0, xg, upg, (3, 4))
    weight_push(0)
    weight_grad(1, xg, gel, (5,))
    weight_push(1)
    meet4(kb, db)

    def scores_back(i, gain_q):
        rows = pl.ds(pl.multiple_of(i * half, half), half)
        d_mixed = mm(db[i].reshape(half, D), wa[:, o_cols]).astype(BF16)
        dmix[rows] = d_mixed
        p = probs[rows]
        d_probs = contract_last(d_mixed, kv[:, HD:])
        inner = jnp.sum(p * d_probs, axis=1, keepdims=True)
        low = (p * (d_probs - inner)).astype(BF16)
        dscore[rows] = low
        d_q = mm(low, kv[:, 0:HD]) * scale
        raw = qraw[rows]
        factor = rms_factor(raw)
        d_raw, part = rms_backward(
            turn_back(d_q, cosine[rows], sine[rows]), raw, factor, head_gain(0)
        )
        dq[rows] = d_raw.astype(BF16)
        return gain_q + part

    gain_q = lax.fori_loop(0, 2, scores_back, jnp.zeros((1, HD), F32))
    kp = slots(3)

    def keys_back(n, _):
        cols = pl.ds(pl.multiple_of(n * half, half), half)
        d_k = contract_first(dscore[:, cols], qs[...]) * scale
        d_v = contract_first(probs[:, cols].astype(BF16), dmix[...])
        both = jnp.concatenate([d_k, d_v], axis=1).astype(BF16)
        kvp[n % 2, 0, n // 2] = both[0:S]
        kvp[n % 2, 1, n // 2] = both[S:]
        return 0

    lax.fori_loop(0, 4, keys_back, 0)
    for i in range(2):
        send(kp + i, kvp.at[i, 1 - core], kvp_core.at[i], partner)

    weight_push(2)
    arrive(kp + (1 - y), kvp_core.at[1 - y])
    kvp_sum[...] = (kvp[1 - y, core].astype(F32) + kvp_core[1 - y].astype(F32)).astype(BF16)
    send(kp + 2, kvp_sum, kvp_chip, chip_of(1 - y, 2))
    arrive(kp + y, kvp_core.at[y])
    arrive(kp + 2, kvp_chip)
    d_left = (
        kvp[y, core, 0].astype(F32) + kvp_core[y, 0].astype(F32) + kvp_chip[0].astype(F32)
    )
    kt = slots(1)
    ret_out[...] = d_left.astype(BF16)

    @pl.when(c > 0)
    def _():
        copy(kt, ret_out, ret_in, {"context": c - 1}).start()

    weight_push(3)

    @pl.when(c < C - 1)
    def _():
        arrive(kt, ret_in)

    @pl.when(c == C - 1)
    def _():
        ret_in[...] = jnp.zeros((S, 2 * HD), BF16)

    d_kv = (
        kvp[y, core, 1].astype(F32)
        + kvp_core[y, 1].astype(F32)
        + kvp_chip[1].astype(F32)
        + ret_in[...].astype(F32)
    )
    raw = jnp.concatenate([kv_raw[0, shard], kv_raw[1, shard]], axis=1).astype(F32)
    d_raw, gain_k = rms_backward(
        turn_back(d_kv[:, :HD], cosine[shard], sine[shard]), raw, rms_factor(raw), head_gain(1)
    )
    d_kv = jnp.concatenate([d_raw, d_kv[:, HD:]], axis=1).astype(BF16)
    for i in range(4):
        dkv_mine[i] = d_kv[:, i * LANES : (i + 1) * LANES]
    kq = slots(4)
    for i in range(1, 4):
        k = (t + i) % 4
        send(kq + i, dkv_mine.at[k], dkv_cols.at[t], {"tensor": k})
    dkv_cols[t] = dkv_mine[t]
    for i in range(1, 4):
        arrive(kq + i, dkv_cols.at[(t - i + 4) % 4])

    k4 = slots(2)

    def query_back(i, _):
        rows = pl.ds(pl.multiple_of(i * half, half), half)
        pair = pl.ds(i * 2, 2)
        part = contract_last(dq[rows], wa[:, q_cols])
        part = part + contract_last(dkv_cols[pair].reshape(half, LANES), wa[:, kv_part])
        part = part.astype(BF16)
        p4[i, 0] = part[0:S]
        p4[i, 1] = part[S:]
        copy(k4 + i, p4.at[i, 1 - core], p4_core.at[i], partner).start()
        return 0

    lax.fori_loop(0, 2, query_back, 0)

    def attn_grad(n, _):
        cols = pl.ds(pl.multiple_of(n * LANES, LANES), LANES)
        left = nrm[:, cols]
        ga[cols, 0:HD] = contract_first(
            db[:, :, :, cols].reshape(T, LANES), mix[...]
        ).astype(BF16)
        ga[cols, HD : 2 * HD] = contract_first(left, dq[...]).astype(BF16)
        ga[cols, 2 * HD :] = contract_first(left, dkv_cols[...].reshape(T, LANES)).astype(BF16)
        return 0

    lax.fori_loop(0, D // LANES, attn_grad, 0)
    ke = slots(1 + C)
    send(ke, ga.at[theirs_x], ga_x, across)
    weight_send(6)
    kc = sum4(k4)
    weight_push(4)
    d_normed = finish4(kc)
    copy(kc, p4_sum, p4_chip, chip_of(1 - y, 2)).wait_send()
    for i in range(2):
        copy(k4 + i, p4.at[i, 1 - core], p4_core.at[i], partner).wait_send()
    values = act[shard].astype(F32)
    d_input, gain_0 = rms_backward(d_normed, values, rms_factor(values), gain(0))
    input_all[y, core] = (dhid[...] + d_input).astype(BF16)
    ki = share4(input_all)
    kr = share4(block_all)
    gain_mine[0:1] = gain_0
    gain_mine[4:8] = jnp.zeros((4, D), F32)
    gain_mine[4:5, 0:HD] = gain_q
    gain_mine[5:6, 0:HD] = gain_k
    kn = slots(4 + 1 + C)
    for i in range(1, 4):
        send(kn + i, gain_mine, gain_tensor.at[i], {"tensor": (t + i) % 4})
    weight_push(5)
    total = gain_mine[...]
    for i in range(1, 4):
        arrive(kn + i, gain_tensor.at[i])
        total = total + gain_tensor[i]
    gain_tensor[0] = total
    send(kn, gain_tensor.at[0], gain_x.at[0], across)
    meet4(ki, input_all)
    save_input = pltpu.make_async_copy(input_all, out_input, ls.at[4])
    save_input.start()
    meet4(kr, block_all)
    save_block = pltpu.make_async_copy(block_all, out_block, ls.at[3])
    save_block.start()
    arrive(ke, ga_x)
    ga[mine_x] = (ga[mine_x].astype(F32) + ga_x[...].astype(F32)).astype(BF16)
    for step in range(1, C):
        send(ke + step, ga.at[rows_of(f, (c + step) % C)], ga_z.at[step - 1], along(step))
    weight_push(6)
    arrive(kn, gain_x.at[0])
    gain_x[1] = total + gain_x[0]
    for step in range(1, C):
        send(kn + 4 + step, gain_x.at[1], gain_z.at[step], along(step))
    weight_end(2)
    weight_end(0)
    attn = ga[rows_of(f, c)].astype(F32)
    for step in range(1, C):
        arrive(ke + step, ga_z.at[step - 1])
        attn = attn + ga_z[step - 1].astype(F32)
    out_attn[...] = attn[:, 0 : 2 * HD]
    kvg[t] = attn[:, 2 * HD :]
    kh = slots(4)
    for i in range(1, 4):
        send(kh + i, kvg.at[t], kvg.at[t], {"tensor": (t + i) % 4})
    weight_end(1)
    total = gain_x[1]
    for step in range(1, C):
        arrive(kn + 4 + step, gain_z.at[step])
        total = total + gain_z[step]
    out_gains[...] = total
    for i in range(1, 4):
        arrive(kh + i, kvg.at[(t - i + 4) % 4])
    out_kv[...] = kvg[...]
    save_block.wait()
    save_input.wait()
    settle()

    @pl.when(c < C - 1)
    def _():
        copy(ks, seg_row, seg_left, {"context": c + 1}).wait_send()
        copy(kk, kv.at[own_half], kv.at[my_half], {"context": c + 1}).wait_send()

    @pl.when(c > 0)
    def _():
        copy(kt, ret_out, ret_in, {"context": c - 1}).wait_send()


def fused(
    mesh,
    activations,
    positions,
    seg_ids,
    norm_gains,
    head_gains,
    w_query,
    w_keyval,
    w_out,
    w_gateup,
    w_down,
    cotangent,
):
    C = mesh.shape["context"]
    T, D = activations.shape[1:]
    R, units = w_down.shape
    U = -(-units // (2 * LANES)) * LANES
    S = T // 4
    narrow = head_gains.shape[1]
    gains = jnp.concatenate(
        [
            norm_gains.T,
            jnp.pad(head_gains.T, ((0, R - narrow), (0, 0))),
            jnp.zeros((R, LANES - 6), BF16),
        ],
        axis=1,
    )
    both = jnp.concatenate([w_gateup, w_down[:, None]], axis=1)
    both = jnp.pad(both, ((0, 0), (0, 0), (0, 2 * U - units)))
    w_ff = both.reshape(R, 3, 2, U).transpose(2, 1, 0, 3)
    freqs = jnp.power(10000.0, -jnp.arange(HD // 2, dtype=F32) * 2.0 / HD)
    angles = positions[0].astype(F32)[:, None] * freqs[None, :]
    seg_row = jnp.broadcast_to(seg_ids, (8, T))
    seg_col = seg_ids[0][:, None]
    operands = (
        activations[0],
        jnp.cos(angles),
        jnp.sin(angles),
        seg_row,
        seg_col,
        cotangent[0],
        w_query,
        w_keyval,
        w_out,
        gains,
        w_ff,
    )
    scratch = [
        pltpu.VMEM((S, D), BF16),
        pltpu.VMEM((D, 2 * HD + 2 * LANES), BF16),
        pltpu.VMEM((3, D, U), BF16),
        pltpu.VMEM((8, T), jnp.int32),
        pltpu.VMEM((8, D), F32),
        pltpu.VMEM((8, HD), F32),
        pltpu.VMEM((T, D), BF16),
        pltpu.VMEM((T, HD), F32),
        pltpu.VMEM((4, T, LANES), BF16),
        pltpu.VMEM((T, HD), BF16),
        pltpu.VMEM((2 * T, 2 * HD), BF16),
        pltpu.VMEM((T, 2 * T), F32),
        pltpu.VMEM((T, HD), BF16),
        pltpu.VMEM((2, 2, S, D), BF16),
        pltpu.VMEM((2, S, D), BF16),
        pltpu.VMEM((S, D), BF16),
        pltpu.VMEM((S, D), BF16),
        pltpu.VMEM((S, D), F32),
        pltpu.VMEM((S, D), F32),
        pltpu.VMEM((4, 2, S, D), BF16),
        pltpu.VMEM((4, 2 * S, U), BF16),
        pltpu.VMEM((4, 2 * S, U), BF16),
        pltpu.VMEM((4, 2 * S, U), BF16),
        pltpu.VMEM((4, 2, S, D), BF16),
        pltpu.VMEM((4, S, D), BF16),
        pltpu.VMEM((3, S, D), BF16),
        pltpu.VMEM((3, S, D), BF16),
        pltpu.VMEM((4, 2, S, D), BF16),
        pltpu.VMEM((S, D), F32),
        pltpu.VMEM((2, 2, S, D), BF16),
        pltpu.VMEM((T, 2 * T), BF16),
        pltpu.VMEM((T, HD), BF16),
        pltpu.VMEM((T, HD), BF16),
        pltpu.VMEM((2, 2, 2, S, 2 * HD), BF16),
        pltpu.VMEM((2, 2, S, 2 * HD), BF16),
        pltpu.VMEM((2, S, 2 * HD), BF16),
        pltpu.VMEM((2, S, 2 * HD), BF16),
        pltpu.VMEM((S, 2 * HD), BF16),
        pltpu.VMEM((S, 2 * HD), BF16),
        pltpu.VMEM((4, S, LANES), BF16),
        pltpu.VMEM((4, S, LANES), BF16),
        pltpu.VMEM((3, C * R, U), BF16),
        pltpu.VMEM((C - 1, 3, R, U), BF16),
        pltpu.VMEM((D, 2 * HD + LANES), BF16),
        pltpu.VMEM((C * R, 2 * HD + LANES), BF16),
        pltpu.VMEM((C - 1, R, 2 * HD + LANES), BF16),
        pltpu.VMEM((4, R, LANES), F32),
        pltpu.VMEM((2, R, U), F32),
        pltpu.VMEM((8, D), F32),
        pltpu.VMEM((4, 8, D), F32),
        pltpu.VMEM((2, 8, D), F32),
        pltpu.VMEM((C, 8, D), F32),
        pltpu.VMEM((2, 2, S, D), BF16),
        pltpu.VMEM((2, 2, S, D), BF16),
        pltpu.SemaphoreType.DMA((SEMAPHORES,)),
        pltpu.SemaphoreType.DMA((SEMAPHORES,)),
        pltpu.SemaphoreType.DMA((10,)),
    ]
    vmem = pl.BlockSpec(memory_space=pltpu.VMEM)
    anywhere = pl.BlockSpec(memory_space=pl.ANY)
    results = (
        jax.ShapeDtypeStruct((2, 2, S, D), BF16),
        jax.ShapeDtypeStruct((2, 2, S, D), BF16),
        jax.ShapeDtypeStruct((8, D), F32),
        jax.ShapeDtypeStruct((3, 2, R, U), F32),
        jax.ShapeDtypeStruct((R, 2 * HD), F32),
        jax.ShapeDtypeStruct((4, R, LANES), F32),
    )
    sizes = {"context": C, "tokens": T, "width": D, "rows": R, "units": U}
    block_out, input_grad, gain_sums, ff_grads, attn_grads, kv_grads = pl.pallas_call(
        functools.partial(fused_kernel, sizes),
        out_shape=results,
        in_specs=[vmem] * 5 + [anywhere] * 6,
        out_specs=[anywhere] * 2 + [vmem, anywhere, vmem, vmem],
        scratch_shapes=scratch,
        compiler_params=pltpu.CompilerParams(
            collective_id=0, has_side_effects=True, vmem_limit_bytes=67043328
        ),
    )(*operands)
    owner = lax.axis_index(("fsdp", "context"))
    norm_grad = lax.dynamic_slice(gain_sums, (0, owner * R), (4, R))
    head_grad = lax.dynamic_slice(gain_sums, (4, owner * narrow), (2, narrow))
    ff = ff_grads.transpose(2, 0, 1, 3).reshape(R, 3, 2 * U)[:, :, :units]
    return (
        block_out.reshape(1, T, D),
        input_grad.reshape(1, T, D),
        norm_grad,
        head_grad,
        attn_grads[:, HD:],
        kv_grads.transpose(1, 0, 2).reshape(R, 2 * HD),
        attn_grads[:, :HD],
        ff[:, :2],
        ff[:, 2],
    )


def block(mesh, *arrays):
    tokens, rows = arrays[0].shape[1], arrays[9].shape[0]
    fits = (
        mesh.shape["fsdp"] == 2
        and mesh.shape["tensor"] == 4
        and mesh.shape["context"] == 4
        and tokens == WINDOW
        and rows % 16 == 0
        and arrays[5].shape[1] == HD
        and arrays[6].shape[1] == 4 * LANES
    )
    return fused(mesh, *arrays) if fits else shards(*arrays)


def shards(
    activations,
    positions,
    seg_ids,
    norm_gains,
    head_gains,
    w_query,
    w_keyval,
    w_out,
    w_gateup,
    w_down,
    cotangent,
):
    tokens = activations.shape[1]
    local_heads = w_query.shape[1] // HD
    inputs = activations[0].astype(jnp.float32)
    places = positions[0]
    documents = seg_ids[0]
    gains_all, heads_all, query_all, keyval_all, out_all = (
        lax.all_gather(norm_gains, ("fsdp", "context"), axis=1, tiled=True),
        lax.all_gather(head_gains, ("fsdp", "context"), axis=1, tiled=True),
        lax.all_gather(w_query, ("fsdp", "context"), axis=0, tiled=True),
        lax.all_gather(w_keyval, ("fsdp", "context"), axis=0, tiled=True),
        lax.all_gather(w_out, ("fsdp", "context"), axis=0, tiled=True),
    )
    gains_f = gains_all.astype(jnp.float32)
    heads_f = heads_all.astype(jnp.float32)
    normed_f, input_back = jax.vjp(rms_norm, inputs, gains_f[0])
    normed = normed_f.astype(jnp.bfloat16)
    query_raw = jnp.dot(normed, query_all, preferred_element_type=jnp.float32).reshape(
        tokens, local_heads, HD
    )
    keyval_raw = jnp.dot(normed, keyval_all, preferred_element_type=jnp.float32)

    def prepare(raw_heads, head_gain):
        return rotate(rms_norm(raw_heads, head_gain), places)

    query_rot, query_back = jax.vjp(prepare, query_raw, heads_f[0])
    key_rot, key_back = jax.vjp(prepare, keyval_raw[:, None, :HD], heads_f[1])
    queries = query_rot.astype(jnp.bfloat16)
    own_keyval = jnp.concatenate([key_rot[:, 0], keyval_raw[:, HD:]], axis=1).astype(jnp.bfloat16)
    labels = jnp.stack([places, documents])
    keep_from = tokens - tokens
    left_keyval, left_labels = from_behind((own_keyval, labels), "context", 1)
    keys_all = jnp.concatenate([left_keyval, own_keyval], axis=0)
    key_places = jnp.concatenate([left_labels[0], places])
    key_documents = jnp.concatenate([left_labels[1], documents])
    has_left = lax.axis_index("context") > 0
    key_live = jnp.concatenate([jnp.full((tokens,), has_left), jnp.ones((tokens,), dtype=bool)])
    scale_factor = HD ** (-0.5)
    block_rows = 512
    block_starts = jnp.arange(tokens // block_rows) * block_rows

    def block_scores():
        spacing = places[:, None] - key_places[None, :]
        visible = (
            key_live[None, :]
            & (documents[:, None] == key_documents[None, :])
            & (spacing >= 0)
            & (spacing < WINDOW)
        )
        raw_scores = (
            jnp.einsum("qhd,kd->hqk", queries, keys_all[:, :HD], preferred_element_type=jnp.float32)
            * scale_factor
        )
        return (jnp.where(visible[None], raw_scores, -1e30), keys_all, queries)

    def forward_block(start):
        scores, near_keyval, query_block = block_scores()
        row_top = jnp.max(scores, axis=-1, keepdims=True)
        raised = jnp.exp(scores - row_top)
        row_total = jnp.sum(raised, axis=-1, keepdims=True)
        probs = raised / row_total
        mixed_block = jnp.einsum(
            "hqk,kd->qhd",
            probs.astype(jnp.bfloat16),
            near_keyval[:, HD:],
            preferred_element_type=jnp.float32,
        )
        return (mixed_block.astype(jnp.bfloat16), row_top + jnp.log(row_total))

    mixed_blocks, log_blocks = lax.map(forward_block, block_starts)
    mixed_low = mixed_blocks.reshape(tokens, local_heads * HD)
    branch = lax.psum(contract_last(mixed_low, out_all).astype(jnp.bfloat16), "tensor").astype(jnp.float32)
    post_attn, post_attn_back = jax.vjp(rms_norm, branch, gains_f[1])
    hidden = inputs + post_attn
    normed_mlp_f, pre_mlp_back = jax.vjp(rms_norm, hidden, gains_f[2])
    normed_mlp = normed_mlp_f.astype(jnp.bfloat16)
    columns = normed_mlp
    gate_up = jnp.einsum(
        "bn,nkf->bkf",
        columns,
        lax.all_gather(w_gateup, ("fsdp", "context"), axis=0, tiled=True),
        preferred_element_type=jnp.float32,
    )
    active_f, glu_back = jax.vjp(glu, gate_up)
    active = active_f.astype(jnp.bfloat16)
    down = lax.psum(
        contract_last(
            active, lax.all_gather(w_down, ("fsdp", "context"), axis=0, tiled=True)
        ).astype(jnp.bfloat16),
        "tensor",
    ).astype(jnp.float32)
    post_mlp, post_mlp_back = jax.vjp(rms_norm, down, gains_f[3])
    result = hidden + post_mlp
    grad_out = cotangent[0].astype(jnp.float32)
    d_down, gain_post_mlp = post_mlp_back(grad_out)
    down_low = d_down.astype(jnp.bfloat16)
    columns = down_low
    d_active = jnp.dot(
        columns,
        lax.all_gather(w_down, ("fsdp", "context"), axis=0, tiled=True),
        preferred_element_type=jnp.float32,
    )
    d_gate_up = glu_back(d_active)[0].astype(jnp.bfloat16)
    d_normed_part = jnp.einsum(
        "bkf,nkf->bn",
        d_gate_up,
        lax.all_gather(w_gateup, ("fsdp", "context"), axis=0, tiled=True),
        preferred_element_type=jnp.float32,
    )
    d_normed_mlp = lax.psum(d_normed_part.astype(jnp.bfloat16), "tensor").astype(jnp.float32)
    d_hidden_norm, gain_pre_mlp = pre_mlp_back(d_normed_mlp)
    d_hidden = grad_out + d_hidden_norm
    features = normed_mlp
    grad_cols = down_low
    gate_up_term = jnp.einsum(
        "bn,bkf->nkf", features, d_gate_up, preferred_element_type=jnp.float32
    )
    down_term = contract_first(grad_cols, active)
    scatter = lambda part: lax.psum_scatter(
        part.astype(jnp.bfloat16), ("fsdp", "context"), scatter_dimension=0, tiled=True
    ).astype(jnp.float32)
    gate_grad = scatter(gate_up_term[:, 0])
    up_grad = scatter(gate_up_term[:, 1])
    down_grad = scatter(down_term)
    d_branch, gain_post_attn = post_attn_back(d_hidden)
    branch_low = d_branch.astype(jnp.bfloat16)
    d_mixed = jnp.dot(branch_low, out_all, preferred_element_type=jnp.float32)
    d_mixed_low = d_mixed.astype(jnp.bfloat16).reshape(tokens, local_heads, HD)

    def backward_block(carry, item):
        start, log_block = item
        scores, near_keyval, query_block = block_scores()
        probs_again = jnp.exp(scores - log_block)
        d_probs = jnp.einsum(
            "qhd,kd->hqk", d_mixed_low, near_keyval[:, HD:], preferred_element_type=jnp.float32
        )
        row_inner = jnp.sum(probs_again * d_probs, axis=-1, keepdims=True)
        d_scores = (probs_again * (d_probs - row_inner)).astype(jnp.bfloat16)
        d_query_block = (
            jnp.einsum(
                "hqk,kd->qhd", d_scores, near_keyval[:, :HD], preferred_element_type=jnp.float32
            )
            * scale_factor
        )
        d_keys = (
            jnp.einsum("hqk,qhd->kd", d_scores, query_block, preferred_element_type=jnp.float32)
            * scale_factor
        )
        d_values = jnp.einsum(
            "hqk,qhd->kd",
            probs_again.astype(jnp.bfloat16),
            d_mixed_low,
            preferred_element_type=jnp.float32,
        )
        updated = carry + jnp.concatenate([d_keys, d_values], axis=1)
        return (updated, d_query_block)

    d_keyval, d_query_blocks = lax.scan(
        backward_block,
        jnp.zeros((tokens + tokens, 2 * HD), jnp.float32),
        (block_starts, log_blocks),
    )
    d_queries = d_query_blocks.reshape(tokens, local_heads, HD)
    returned = from_behind(d_keyval[:tokens].astype(jnp.bfloat16), "context", -1).astype(
        jnp.float32
    )
    own_grad = d_keyval[tokens:].at[keep_from:].add(returned)
    d_query_raw, gain_query = query_back(d_queries)
    d_query_low = d_query_raw.reshape(tokens, local_heads * HD).astype(jnp.bfloat16)
    d_normed_query, keyval_grad, gain_query_all = (
        lax.psum(contract_last(d_query_low, query_all).astype(jnp.bfloat16), "tensor").astype(
            jnp.float32
        ),
        lax.psum(own_grad.astype(jnp.bfloat16), "tensor").astype(jnp.float32),
        lax.psum(gain_query.astype(jnp.bfloat16), "tensor").astype(jnp.float32),
    )
    d_key_raw, gain_key = key_back(keyval_grad[:, None, :HD])
    d_keyval_low = jnp.concatenate([d_key_raw[:, 0], keyval_grad[:, HD:]], axis=1).astype(
        jnp.bfloat16
    )
    d_normed = d_normed_query + contract_last(d_keyval_low, keyval_all)
    d_input_norm, gain_input = input_back(d_normed)
    input_total = d_hidden + d_input_norm
    features = normed
    grad_cols = branch_low
    attn_grads = lax.psum_scatter(
        jnp.stack(
            [contract_first(features, d_query_low), contract_first(grad_cols, mixed_low)], axis=1
        ).astype(jnp.bfloat16),
        ("fsdp", "context"),
        scatter_dimension=0,
        tiled=True,
    ).astype(jnp.float32)
    keyval_term = contract_first(normed, d_keyval_low)
    gain_terms = jnp.stack([gain_input, gain_post_attn, gain_pre_mlp, gain_post_mlp])
    head_terms = jnp.stack([gain_query_all, gain_key])
    gain_grad, head_grad, keyval_weight_grad = (
        lax.psum_scatter(
            gain_terms.astype(jnp.bfloat16), ("fsdp", "context"), scatter_dimension=1, tiled=True
        ).astype(jnp.float32),
        lax.psum_scatter(
            head_terms.astype(jnp.bfloat16), ("fsdp", "context"), scatter_dimension=1, tiled=True
        ).astype(jnp.float32),
        lax.psum_scatter(
            keyval_term.astype(jnp.bfloat16), ("fsdp", "context"), scatter_dimension=0, tiled=True
        ).astype(jnp.float32),
    )
    return (
        result[None].astype(jnp.bfloat16),
        input_total[None].astype(jnp.bfloat16),
        gain_grad,
        head_grad,
        attn_grads[:, 0],
        keyval_weight_grad,
        attn_grads[:, 1],
        jnp.stack([gate_grad, up_grad], axis=1),
        down_grad,
    )


def solution(mesh):
    return jax.shard_map(
        functools.partial(block, mesh),
        mesh=mesh,
        in_specs=(
            P("fsdp", "context", None),
            P("fsdp", "context"),
            P("fsdp", "context"),
            P(None, ("fsdp", "context")),
            P(None, ("fsdp", "context")),
            P(("fsdp", "context"), "tensor"),
            P(("fsdp", "context"), None),
            P(("fsdp", "context"), "tensor"),
            P(("fsdp", "context"), None, "tensor"),
            P(("fsdp", "context"), "tensor"),
            P("fsdp", "context", None),
        ),
        out_specs=(
            P("fsdp", "context", None),
            P("fsdp", "context", None),
            P(None, ("fsdp", "context")),
            P(None, ("fsdp", "context")),
            P(("fsdp", "context"), "tensor"),
            P(("fsdp", "context"), None),
            P(("fsdp", "context"), "tensor"),
            P(("fsdp", "context"), None, "tensor"),
            P(("fsdp", "context"), "tensor"),
        ),
        check_vma=False,
    )
```

```python
import functools
import math

import jax
import jax.numpy as jnp
from jax import lax
from jax.experimental import pallas as pl
from jax.experimental.pallas import tpu as pltpu
from jax.sharding import PartitionSpec as P

HD = 256
WINDOW = 512


EPSILON = 1e-06


def from_behind(block, axis, distance):
    devices = range(lax.axis_size(axis))
    route = [(i - distance, i) for i in devices if i - distance in devices]
    return lax.ppermute(block, axis, route)


def rms_norm(values, gain):
    factor = lax.rsqrt(jnp.mean(values * values, axis=-1, keepdims=True) + EPSILON)
    return values * factor * gain


def rotate(tensor, places):
    width_all = tensor.shape[-1]
    half_width = width_all // 2
    freqs = jnp.power(10000.0, -jnp.arange(half_width, dtype=jnp.float32) * 2.0 / width_all)
    angles = places.astype(jnp.float32)[:, None] * freqs[None, :]
    cosine = jnp.cos(angles)[:, None, :]
    sine = jnp.sin(angles)[:, None, :]
    first_half = tensor[..., :half_width]
    second_half = tensor[..., half_width:]
    return jnp.concatenate(
        [first_half * cosine - second_half * sine, second_half * cosine + first_half * sine],
        axis=-1,
    )


def glu(gate_up):
    return jax.nn.gelu(gate_up[:, 0], approximate=True) * gate_up[:, 1]


def contract_last(left_side, right_side):
    return lax.dot_general(
        left_side, right_side, (((1,), (1,)), ((), ())), preferred_element_type=jnp.float32
    )


def contract_first(left_side, right_side):
    return lax.dot_general(
        left_side, right_side, (((0,), (0,)), ((), ())), preferred_element_type=jnp.float32
    )


MESH = pl.DeviceIdType.MESH
F32 = jnp.float32
BF16 = jnp.bfloat16
LANES = 128
SEMAPHORES = 171


def mm(left, right):
    return jnp.dot(left, right, preferred_element_type=F32)


def rms_factor(values):
    return lax.rsqrt(jnp.mean(values * values, axis=-1, keepdims=True) + EPSILON)


def rms_backward(grad, values, factor, gain):
    unit = values * factor
    scaled = grad * gain
    inner = jnp.mean(scaled * unit, axis=-1, keepdims=True)
    return factor * (scaled - unit * inner), jnp.sum(grad * unit, axis=0, keepdims=True)


def turn(values, cosine, sine):
    half = values.shape[-1] // 2
    first, second = values[:, :half], values[:, half:]
    return jnp.concatenate([first * cosine - second * sine, second * cosine + first * sine], axis=1)


def turn_back(values, cosine, sine):
    half = values.shape[-1] // 2
    first, second = values[:, :half], values[:, half:]
    return jnp.concatenate([first * cosine + second * sine, second * cosine - first * sine], axis=1)


def emit_kernel(count, *refs):
    sources, results, held = refs[:count], refs[count : 2 * count], refs[2 * count : 3 * count]
    incoming, outgoing = refs[3 * count :]
    reads = [pltpu.make_async_copy(sources[n], held[n], incoming.at[n]) for n in range(count)]
    writes = [pltpu.make_async_copy(held[n], results[n], outgoing.at[n]) for n in range(count)]
    for moved in reads:
        moved.start()
    for n in range(count):
        reads[n].wait()
        writes[n].start()
    for moved in writes:
        moved.wait()


def fused_kernel(
    sizes,
    act,
    positions,
    seg_ids,
    norm_gains,
    head_gains,
    w_gateup,
    w_down,
    cot_all,
    w_query,
    w_keyval,
    w_out,
    out_block,
    out_input,
    out_norm,
    out_head,
    out_query,
    out_kv,
    out_out,
    out_gateup,
    out_down,
    cosine,
    sine,
    seg_row,
    seg_col,
    gain_pack,
    gain_cols,
    w_ff,
    cot,
    wa,
    wf,
    seg_left,
    gain_rows,
    head_rows,
    nrm,
    qraw,
    kv_raw,
    qs,
    kv,
    probs,
    mix,
    p4,
    p4_core,
    p4_sum,
    p4_chip,
    hid,
    bran,
    xg,
    gel,
    upg,
    active,
    p8,
    p8_core,
    p8_sum,
    p8_chip,
    dd,
    dhid,
    db,
    dscore,
    dmix,
    dq,
    kvp,
    kvp_core,
    kvp_sum,
    kvp_chip,
    ret_out,
    ret_in,
    dkv_mine,
    dkv_cols,
    gall_x,
    gall_z,
    ga,
    ga_x,
    ga_z,
    kvg,
    ff_stage,
    gain_mine,
    gain_tensor,
    gain_x,
    gain_z,
    block_all,
    input_all,
    st_out,
    st_query,
    st_norm,
    st_head,
    st_kv,
    ss,
    rs,
    ls,
):
    C = sizes["context"]
    T, D, R, U = sizes["tokens"], sizes["width"], sizes["rows"], sizes["units"]
    units = w_down.shape[1]
    narrow = HD // (2 * C)
    S = T // 4
    f = lax.axis_index("fsdp")
    c = lax.axis_index("context")
    t = lax.axis_index("tensor")
    y, core = t // 2, t % 2
    m = c % 2
    base = c - m
    partner = {"tensor": y * 2 + (1 - core)}
    across = {"fsdp": 1 - f}
    counter = [0]
    sent = []

    def slots(count):
        first = counter[0]
        counter[0] += count
        assert counter[0] <= SEMAPHORES
        return first

    def copy(k, src, dst, device):
        return pltpu.make_async_remote_copy(
            src_ref=src,
            dst_ref=dst,
            send_sem=ss.at[k],
            recv_sem=rs.at[k],
            device_id=device,
            device_id_type=MESH,
        )

    def send(k, src, dst, device):
        moved = copy(k, src, dst, device)
        moved.start()
        sent.append(moved)

    def arrive(k, dst):
        copy(k, dst, dst, partner).wait_recv()

    def settle():
        for moved in sent:
            moved.wait_send()
        sent.clear()

    def along(step):
        return {"context": (c + step) % C}

    def rows_of(ff, cc):
        return pl.ds(pl.multiple_of((ff * C + cc) * R, R), R)

    def chip_of(k, count):
        if count == 2:
            return {"tensor": k * 2 + core}
        return {"context": base + k // 2, "tensor": (k % 2) * 2 + core}

    barrier = pltpu.get_barrier_semaphore()
    greeted = [along(step) for step in range(1, C)] + [across]
    greeted += [{"tensor": (t + step) % 4} for step in range(1, 4)]
    greeted += [{"context": base + 1 - m, "tensor": (1 - y) * 2 + core}]
    for device in greeted:
        pl.semaphore_signal(barrier, inc=1, device_id=device, device_id_type=MESH)
    gain_pack[...] = jnp.zeros(gain_pack.shape, F32)
    gain_pack[0:4, 0:R] = norm_gains[...].astype(F32)
    gain_pack[4:6, 0:narrow] = head_gains[...].astype(F32)
    gain_cols[...] = jnp.transpose(gain_pack[...])[0:R].astype(BF16)
    seg_row[...] = jnp.broadcast_to(seg_ids[...], seg_row.shape)
    pl.semaphore_wait(barrier, len(greeted))

    mine = rows_of(f, c)
    kv_cols = pl.ds(pl.multiple_of(t * LANES, LANES), LANES)
    attn_parts = (
        (w_query, slice(0, HD)),
        (w_keyval.at[:, kv_cols], slice(HD, HD + LANES)),
        (w_out, slice(HD + LANES, 2 * HD + LANES)),
        (gain_cols, slice(2 * HD + LANES, 2 * HD + 2 * LANES)),
    )
    q_cols, kv_part, o_cols = (cols for _, cols in attn_parts[:3])
    local = []
    for n, (part, cols) in enumerate(attn_parts):
        local.append(pltpu.make_async_copy(part, wa.at[mine, cols], ls.at[6 + n]))
        local[-1].start()
    ka = slots(4 * C)
    kar = slots(C - 1)
    for step in range(1, C):
        for n, (part, cols) in enumerate(attn_parts):
            send(ka + 4 * step + n, part, wa.at[mine, cols], along(step))
    for n, (part, cols) in enumerate(attn_parts):
        send(ka + n, part, wa.at[mine, cols], across)
    ks = slots(1)

    @pl.when(c < C - 1)
    def _():
        copy(ks, seg_row, seg_left, {"context": c + 1}).start()

    pieces = ((0, 0, 512), (0, 512, U), (1, 0, 512), (1, 512, U), (2, 0, 512), (2, 512, U))
    kf = slots((2 * C - 1) * len(pieces))

    def piece(p, rows):
        w, low, high = pieces[p]
        return wf.at[w, rows, low:high]

    def send_ff(p):
        k = kf + (2 * C - 1) * p
        w, low, high = pieces[p]
        for step in range(1, C):
            send(k + step, w_ff.at[(c + step) % 2, w, :, low:high], piece(p, mine), along(step))
        send(k, w_ff.at[m, w, :, low:high], piece(p, mine), across)

    def relay_ff(p):
        k = kf + (2 * C - 1) * p
        for step in range(1, C):
            part = piece(p, rows_of(f, (c - step + C) % C))
            arrive(k + step, part)
            send(k + C - 1 + step, part, part, across)

    def meet_ff(p):
        k = kf + (2 * C - 1) * p
        arrive(k, piece(p, rows_of(1 - f, c)))
        for step in range(1, C):
            arrive(k + C - 1 + step, piece(p, rows_of(1 - f, (c - step + C) % C)))

    for w in range(3):
        whole = w_down[...] if w == 2 else w_gateup[:, w, :]
        w_ff[0, w] = whole[:, 0:U]
        w_ff[1, w, :, 0 : units - U] = whole[:, U:units]
        w_ff[1, w, :, units - U :] = jnp.zeros((R, 2 * U - units), BF16)
    seg_col[...] = jnp.transpose(seg_row[...].astype(F32))[:, 0:1].astype(jnp.int32)
    place = jnp.broadcast_to(positions[...].astype(F32), (8, T))
    index = lax.broadcasted_iota(jnp.int32, (1, HD // 2), 1).astype(F32)
    angle = jnp.transpose(place)[:, 0:1] * jnp.exp(index * (-2.0 * math.log(10000.0) / HD))
    cosine[...] = jnp.cos(angle)
    sine[...] = jnp.sin(angle)
    shard = pl.ds(pl.multiple_of(t * S, S), S)
    own_cot = pltpu.make_async_copy(cot_all.at[shard], cot, ls.at[2])
    own_cot.start()
    own_ff = pltpu.make_async_copy(w_ff.at[m], wf.at[:, mine], ls.at[1])
    own_ff.start()
    for step in range(1, C):
        other = rows_of(f, (c - step + C) % C)
        for n, (_, cols) in enumerate(attn_parts):
            arrive(ka + 4 * step + n, wa.at[other, cols])
        send(kar + step - 1, wa.at[other], wa.at[other], across)
    for moved in local:
        moved.wait()
    send_ff(0)
    for n, (_, cols) in enumerate(attn_parts):
        arrive(ka + n, wa.at[rows_of(1 - f, c), cols])
    for step in range(1, C):
        arrive(kar + step - 1, wa.at[rows_of(1 - f, (c - step + C) % C)])

    @pl.when(c > 0)
    def _():
        arrive(ks, seg_left)

    @pl.when(c == 0)
    def _():
        seg_left[...] = jnp.full(seg_left.shape, -1, jnp.int32)
        kv[0:T] = jnp.zeros((T, 2 * HD), BF16)

    gain_t = jnp.transpose(wa[:, 2 * HD + LANES :].astype(F32))
    gain_rows[...] = gain_t[0:8]
    here = lax.broadcasted_iota(jnp.int32, (D, HD), 0)
    want = lax.broadcasted_iota(jnp.int32, (D, HD), 1)
    shift = narrow.bit_length() - 1
    want = lax.shift_right_logical(want, shift) * R + (want & (narrow - 1))
    pick = jnp.where(here == want, 1.0, 0.0).astype(BF16)
    head_rows[...] = mm(gain_t[0:16].astype(BF16), pick)[0:8]

    def gain(index):
        return gain_rows[index : index + 1]

    def head_gain(index):
        return head_rows[4 + index : 5 + index]

    half = T // 2

    def project(i, _):
        rows = pl.ds(pl.multiple_of(i * half, half), half)
        values = act[rows].astype(F32)
        low = (values * rms_factor(values) * gain(0)).astype(BF16)
        nrm[rows] = low
        kv_raw[t, rows] = mm(low, wa[:, kv_part]).astype(BF16)
        return 0

    lax.fori_loop(0, 2, project, 0)
    ku = slots(4)
    for i in range(1, 4):
        send(ku + i, kv_raw.at[t], kv_raw.at[t], {"tensor": (t + i) % 4})

    def query(i, _):
        rows = pl.ds(pl.multiple_of(i * half, half), half)
        raw_q = mm(nrm[rows], wa[:, q_cols])
        qraw[rows] = raw_q
        qs[rows] = turn(
            raw_q * rms_factor(raw_q) * head_gain(0), cosine[rows], sine[rows]
        ).astype(BF16)
        return 0

    lax.fori_loop(0, 2, query, 0)
    for i in range(1, 4):
        arrive(ku + i, kv_raw.at[(t - i + 4) % 4])

    def key(i, _):
        rows = pl.ds(pl.multiple_of(i * half, half), half)
        raw_k = jnp.concatenate([kv_raw[0, rows], kv_raw[1, rows]], axis=1).astype(F32)
        own = pl.ds(pl.multiple_of(T + i * half, half), half)
        kv[own, 0:HD] = turn(
            raw_k * rms_factor(raw_k) * head_gain(1), cosine[rows], sine[rows]
        ).astype(BF16)
        kv[own, HD : HD + LANES] = kv_raw[2, rows]
        kv[own, HD + LANES :] = kv_raw[3, rows]
        return 0

    lax.fori_loop(0, 2, key, 0)
    kk = slots(2)
    my_half = pl.ds(pl.multiple_of(core * half, half), half)
    other_half = pl.ds(pl.multiple_of((1 - core) * half, half), half)
    own_half = pl.ds(pl.multiple_of(T + core * half, half), half)

    @pl.when(c < C - 1)
    def _():
        copy(kk, kv.at[own_half], kv.at[my_half], {"context": c + 1}).start()

    send_ff(1)
    send_ff(2)
    relay_ff(0)

    @pl.when(c > 0)
    def _():
        arrive(kk, kv.at[my_half])
        moved = copy(kk + 1, kv.at[my_half], kv.at[my_half], partner)
        moved.start()
        arrive(kk + 1, kv.at[other_half])
        moved.wait_send()

    scale = HD**-0.5
    no_left = jnp.where(c > 0, 0, 2 * T)
    k4 = slots(2)

    def attend(i, _):
        rows = pl.ds(pl.multiple_of(i * half, half), half)
        q = qs[rows]
        labels = seg_col[rows]
        row = lax.broadcasted_iota(jnp.int32, (half, T), 0) + i * half
        col = lax.broadcasted_iota(jnp.int32, (half, T), 1)
        left = contract_last(q, kv[0:T, 0:HD]) * scale
        left = jnp.where((labels == seg_left[0:1]) & (col > row + no_left), left, -1e30)
        own = contract_last(q, kv[T:, 0:HD]) * scale
        own = jnp.where((labels == seg_row[0:1]) & (col <= row), own, -1e30)
        top = jnp.maximum(
            jnp.max(left, axis=1, keepdims=True), jnp.max(own, axis=1, keepdims=True)
        )
        left, own = jnp.exp(left - top), jnp.exp(own - top)
        total = jnp.sum(left, axis=1, keepdims=True) + jnp.sum(own, axis=1, keepdims=True)
        left, own = left / total, own / total
        probs[rows, 0:T] = left
        probs[rows, T:] = own
        mixed = mm(left.astype(BF16), kv[0:T, HD:]) + mm(own.astype(BF16), kv[T:, HD:])
        mixed = mixed.astype(BF16)
        mix[rows] = mixed
        part = contract_last(mixed, wa[:, o_cols]).astype(BF16)
        p4[i, 0] = part[0:S]
        p4[i, 1] = part[S:]
        copy(k4 + i, p4.at[i, 1 - core], p4_core.at[i], partner).start()
        return 0

    lax.fori_loop(0, 2, attend, 0)

    def sum4(k):
        kc = slots(1)
        arrive(k + (1 - y), p4_core.at[1 - y])
        p4_sum[...] = (
            p4[1 - y, core].astype(F32) + p4_core[1 - y].astype(F32)
        ).astype(BF16)
        copy(kc, p4_sum, p4_chip, chip_of(1 - y, 2)).start()
        arrive(k + y, p4_core.at[y])
        return kc

    def finish4(kc):
        arrive(kc, p4_chip)
        return (
            p4[y, core].astype(F32)
            + p4_core[y].astype(F32)
            + p4_chip[...].astype(F32)
        )

    kc = sum4(k4)
    relay_ff(1)
    branch = finish4(kc)
    copy(kc, p4_sum, p4_chip, chip_of(1 - y, 2)).wait_send()
    for i in range(2):
        copy(k4 + i, p4.at[i, 1 - core], p4_core.at[i], partner).wait_send()

    bran[...] = branch
    hidden = act[shard].astype(F32) + branch * rms_factor(branch) * gain(1)
    hid[...] = hidden
    low = (hidden * rms_factor(hidden) * gain(2)).astype(BF16)

    me = m * 2 + y

    def gather8(full, value):
        kg = slots(8)
        full[me, core] = value
        send(kg + 4, full.at[me, core], full.at[me, core], partner)
        for i in range(1, 4):
            send(kg + i, full.at[me, core], full.at[me, core], chip_of((me + i) % 4, 4))
        return kg

    def pass8(kg, full, i):
        k = (me - i + 4) % 4
        arrive(kg + i, full.at[k, core])
        copy(kg + 4 + i, full.at[k, core], full.at[k, core], partner).start()

    def meet8(kg, full, i):
        k = (me - i + 4) % 4
        arrive(kg + 4 + i, full.at[k, 1 - core])

    def settle8(kg, full):
        for i in range(1, 4):
            k = (me - i + 4) % 4
            copy(kg + 4 + i, full.at[k, core], full.at[k, core], partner).wait_send()

    def give8(ko, i):
        k = (me - i + 4) % 4
        copy(ko + i, p8.at[k, 1 - core], p8_core.at[i], partner).start()

    def push8(ko, i):
        k = (me - i + 4) % 4
        arrive(ko + i, p8_core.at[i])
        p8_sum[i - 1] = (
            p8[k, core].astype(F32) + p8_core[i].astype(F32)
        ).astype(BF16)
        copy(ko + 4 + i, p8_sum.at[i - 1], p8_chip.at[i - 1], chip_of(k, 4)).start()

    def finish8(ko):
        arrive(ko, p8_core.at[0])
        total = p8[me, core].astype(F32) + p8_core[0].astype(F32)
        for i in range(1, 4):
            arrive(ko + 4 + i, p8_chip.at[i - 1])
            total = total + p8_chip[i - 1].astype(F32)
        for i in range(4):
            copy(ko + i, p8.at[0, 1 - core], p8_core.at[i], partner).wait_send()
        for i in range(1, 4):
            copy(ko + 4 + i, p8_sum.at[0], p8_chip.at[0], partner).wait_send()
        return total

    kx = slots(7)
    beside, beyond = m * 2 + 1 - y, (1 - m) * 2 + y
    corner = (1 - m) * 2 + 1 - y
    xg[me, core] = low
    send(kx + 2, xg.at[me, core], xg.at[me, core], chip_of(beyond, 4))
    send(kx + 1, xg.at[me, core], xg.at[me, core], chip_of(beside, 4))
    send(kx, xg.at[me, core], xg.at[me, core], partner)
    send_ff(3)
    send_ff(4)
    relay_ff(2)
    for i, k in ((1, beside), (2, beyond), (3, corner)):
        part = xg.at[k, core]
        arrive(kx + i, part)
        if i == 2:
            send(kx + 3, part, part, chip_of(beside, 4))
        send(kx + 3 + i, part, part, partner)
    send_ff(5)
    relay_ff(3)
    own_ff.wait()
    own_cot.wait()
    for p in range(4):
        meet_ff(p)
    arrive(kx, xg.at[me, 1 - core])
    for i, k in ((1, beside), (2, beyond), (3, corner)):
        arrive(kx + 3 + i, xg.at[k, 1 - core])
    root = 0.7978845608028654
    ko = slots(8)

    def forward(i, _):
        k = (me - i + 4) % 4
        x = xg[k].reshape(2 * S, D)
        gate = mm(x, wf[0])
        up = mm(x, wf[1])
        square = gate * gate
        bent = jnp.tanh(root * gate * (1.0 + 0.044715 * square))
        ramp = 0.5 * (1.0 + bent)
        gelu = gate * ramp
        slope = ramp + 0.5 * gate * (1.0 - bent * bent) * root * (1.0 + 3 * 0.044715 * square)
        gel[k] = gelu.astype(BF16)
        upg[k] = (up * slope).astype(BF16)
        active[k] = (gelu * up).astype(BF16)
        return 0

    lax.fori_loop(0, 2, forward, 0)
    relay_ff(4)
    lax.fori_loop(2, 4, forward, 0)
    relay_ff(5)
    meet_ff(4)
    meet_ff(5)

    def lower(i, _):
        k = (me - i + 4) % 4
        p8[k] = contract_last(active[k], wf[2]).astype(BF16).reshape(2, S, D)
        give8(ko, i)

        @pl.when(i > 1)
        def _():
            push8(ko, i - 1)

        return 0

    lax.fori_loop(0, 4, lower, 0)
    push8(ko, 3)
    down = finish8(ko)

    factor = rms_factor(down)
    grad = cot[...].astype(F32)
    result = (hid[...] + down * factor * gain(3)).astype(BF16)
    d_down, gain_3 = rms_backward(grad, down, factor, gain(3))
    gain_mine[3:4] = gain_3
    kd = gather8(dd, d_down.astype(BF16))

    def share4(full):
        kb = slots(3)
        send(kb, full.at[y, core], full.at[y, core], chip_of(1 - y, 2))
        send(kb + 1, full.at[y, core], full.at[y, core], partner)
        return kb

    def meet4(kb, full):
        arrive(kb, full.at[1 - y, core])
        send(kb + 2, full.at[1 - y, core], full.at[1 - y, core], partner)
        arrive(kb + 1, full.at[y, 1 - core])
        arrive(kb + 2, full.at[1 - y, 1 - core])

    block_all[y, core] = result
    ko2 = slots(8)

    def backward(i, _):
        k = (me - i + 4) % 4
        meet8(kd, dd, i)
        low = dd[k].reshape(2 * S, D)
        d_active = mm(low, wf[2])

        @pl.when(i < 3)
        def _():
            pass8(kd, dd, i + 1)

        d_gate = (d_active * upg[k].astype(F32)).astype(BF16)
        d_up = (d_active * gel[k].astype(F32)).astype(BF16)
        upg[k] = d_gate
        gel[k] = d_up
        p8[k] = (
            (contract_last(d_gate, wf[0]) + contract_last(d_up, wf[1]))
            .astype(BF16)
            .reshape(2, S, D)
        )
        give8(ko2, i)

        @pl.when(i > 1)
        def _():
            push8(ko2, i - 1)

        return 0

    lax.fori_loop(0, 4, backward, 0)
    push8(ko2, 3)
    settle8(kd, dd)

    settle()
    gall = wf
    mine_x = pl.ds(pl.multiple_of(f * C * R, C * R), C * R)
    theirs_x = pl.ds(pl.multiple_of((1 - f) * C * R, C * R), C * R)
    ff_chunk = lambda w, low, high: (
        gall.at[w, :, low:high],
        gall_x.at[w, :, low:high],
        gall_z.at[:, w, :, low:high],
    )
    attn_chunk = lambda low, high: (
        ga.at[:, low:high],
        ga_x.at[:, low:high],
        ga_z.at[:, :, low:high],
    )
    chunks = (
        ff_chunk(2, 0, 256),
        ff_chunk(2, 256, 512),
        ff_chunk(2, 512, U),
        ff_chunk(0, 0, 512),
        ff_chunk(0, 512, U),
        attn_chunk(0, HD),
        ff_chunk(1, 0, 640),
        attn_chunk(HD, 2 * HD + LANES),
        ff_chunk(1, 640, U),
    )
    kw = slots(len(chunks))
    kz = slots(len(chunks) * (C - 1))

    def weight_grad(w, left, right, early):
        def tile(n, _):
            cols = pl.ds(pl.multiple_of(n * LANES, LANES), LANES)
            block = left[:, :, :, cols].reshape(8 * S, LANES)
            gall[w, cols] = contract_first(block, right[...].reshape(8 * S, U)).astype(BF16)
            return 0

        first = D // LANES // 2
        lax.fori_loop(0, first + 1, lambda n, _: tile(n + first * (1 - f), _), 0)
        for q in early:
            weight_send(q)
        lax.fori_loop(0, first, lambda n, _: tile(n + (first + 1) * f, _), 0)

    def weight_send(q):
        full, from_x, _ = chunks[q]
        send(kw + q, full.at[theirs_x], from_x, across)

    def weight_push(q):
        full, from_x, from_z = chunks[q]
        arrive(kw + q, from_x)

        def add(n, _):
            rows = pl.ds(pl.multiple_of(f * C * R + n * R, R), R)
            part = pl.ds(pl.multiple_of(n * R, R), R)
            full[rows] = (full[rows].astype(F32) + from_x[part].astype(F32)).astype(BF16)
            return 0

        lax.fori_loop(0, C, add, 0)
        for step in range(1, C):
            send(
                kz + q * (C - 1) + step - 1,
                full.at[rows_of(f, (c + step) % C)],
                from_z.at[step - 1],
                along(step),
            )

    def weight_meet(*which):
        for q in which:
            for step in range(1, C):
                arrive(kz + q * (C - 1) + step - 1, chunks[q][2].at[step - 1])

    def weight_end(w):
        same = gall[w, rows_of(f, c)].astype(F32)
        other = jnp.zeros((R, U), F32)
        for step in range(1, C):
            if step % 2:
                other = other + gall_z[step - 1, w].astype(F32)
            else:
                same = same + gall_z[step - 1, w].astype(F32)
        ff_stage[:, 0:U] = jnp.where(m == 0, same, other)
        ff_stage[:, U:units] = jnp.where(m == 0, other, same)[:, 0 : units - U]
        into = out_down if w == 2 else out_gateup.at[:, w]
        saved = pltpu.make_async_copy(ff_stage, into, ls.at[5])
        saved.start()
        saved.wait()

    weight_grad(2, dd, active, (0, 1, 2))
    weight_grad(0, xg, upg, (3, 4))
    weight_push(0)
    d_normed = finish8(ko2)
    hidden = hid[...]
    d_hidden, gain_2 = rms_backward(d_normed, hidden, rms_factor(hidden), gain(2))
    d_hidden = cot[...].astype(F32) + d_hidden
    dhid[...] = d_hidden
    gain_mine[2:3] = gain_2
    branch = bran[...]
    d_branch, gain_1 = rms_backward(d_hidden, branch, rms_factor(branch), gain(1))
    gain_mine[1:2] = gain_1
    db[y, core] = d_branch.astype(BF16)
    kb = share4(db)
    weight_push(1)
    weight_grad(1, xg, gel, ())
    weight_push(2)
    meet4(kb, db)

    def out_grad(n, _):
        cols = pl.ds(pl.multiple_of(n * LANES, LANES), LANES)
        ga[cols, 0:HD] = contract_first(
            db[:, :, :, cols].reshape(T, LANES), mix[...]
        ).astype(BF16)
        return 0

    lax.fori_loop(0, D // LANES, out_grad, 0)
    weight_send(5)
    weight_send(6)

    def scores_back(i, gain_q):
        rows = pl.ds(pl.multiple_of(i * half, half), half)
        d_mixed = mm(db[i].reshape(half, D), wa[:, o_cols]).astype(BF16)
        dmix[rows] = d_mixed
        p = probs[rows]
        d_probs = contract_last(d_mixed, kv[:, HD:])
        inner = jnp.sum(p * d_probs, axis=1, keepdims=True)
        low = (p * (d_probs - inner)).astype(BF16)
        dscore[rows] = low
        d_q = mm(low, kv[:, 0:HD]) * scale
        raw = qraw[rows]
        factor = rms_factor(raw)
        d_raw, part = rms_backward(
            turn_back(d_q, cosine[rows], sine[rows]), raw, factor, head_gain(0)
        )
        dq[rows] = d_raw.astype(BF16)
        return gain_q + part

    gain_q = lax.fori_loop(0, 2, scores_back, jnp.zeros((1, HD), F32))
    kp = slots(3)

    def keys_back(n, _):
        cols = pl.ds(pl.multiple_of(n * half, half), half)
        d_k = contract_first(dscore[:, cols], qs[...]) * scale
        d_v = contract_first(probs[:, cols].astype(BF16), dmix[...])
        both = jnp.concatenate([d_k, d_v], axis=1).astype(BF16)
        kvp[n % 2, 0, n // 2] = both[0:S]
        kvp[n % 2, 1, n // 2] = both[S:]
        return 0

    lax.fori_loop(0, 4, keys_back, 0)
    for i in range(2):
        send(kp + i, kvp.at[i, 1 - core], kvp_core.at[i], partner)

    arrive(kp + (1 - y), kvp_core.at[1 - y])
    kvp_sum[...] = (kvp[1 - y, core].astype(F32) + kvp_core[1 - y].astype(F32)).astype(BF16)
    send(kp + 2, kvp_sum, kvp_chip, chip_of(1 - y, 2))
    kr = share4(block_all)
    weight_push(3)
    arrive(kp + y, kvp_core.at[y])
    arrive(kp + 2, kvp_chip)
    d_left = (
        kvp[y, core, 0].astype(F32) + kvp_core[y, 0].astype(F32) + kvp_chip[0].astype(F32)
    )
    kt = slots(1)
    ret_out[...] = d_left.astype(BF16)

    @pl.when(c > 0)
    def _():
        copy(kt, ret_out, ret_in, {"context": c - 1}).start()

    weight_push(4)
    weight_push(5)

    @pl.when(c < C - 1)
    def _():
        arrive(kt, ret_in)

    @pl.when(c == C - 1)
    def _():
        ret_in[...] = jnp.zeros((S, 2 * HD), BF16)

    d_kv = (
        kvp[y, core, 1].astype(F32)
        + kvp_core[y, 1].astype(F32)
        + kvp_chip[1].astype(F32)
        + ret_in[...].astype(F32)
    )
    raw = jnp.concatenate([kv_raw[0, shard], kv_raw[1, shard]], axis=1).astype(F32)
    d_raw, gain_k = rms_backward(
        turn_back(d_kv[:, :HD], cosine[shard], sine[shard]), raw, rms_factor(raw), head_gain(1)
    )
    d_kv = jnp.concatenate([d_raw, d_kv[:, HD:]], axis=1).astype(BF16)
    for i in range(4):
        dkv_mine[i] = d_kv[:, i * LANES : (i + 1) * LANES]
    kq = slots(4)
    for i in range(1, 4):
        k = (t + i) % 4
        send(kq + i, dkv_mine.at[k], dkv_cols.at[t], {"tensor": k})
    dkv_cols[t] = dkv_mine[t]
    for i in range(1, 4):
        arrive(kq + i, dkv_cols.at[(t - i + 4) % 4])

    k4 = slots(2)

    def query_back(i, _):
        rows = pl.ds(pl.multiple_of(i * half, half), half)
        pair = pl.ds(i * 2, 2)
        part = contract_last(dq[rows], wa[:, q_cols])
        part = part + contract_last(dkv_cols[pair].reshape(half, LANES), wa[:, kv_part])
        part = part.astype(BF16)
        p4[i, 0] = part[0:S]
        p4[i, 1] = part[S:]
        copy(k4 + i, p4.at[i, 1 - core], p4_core.at[i], partner).start()
        return 0

    lax.fori_loop(0, 2, query_back, 0)

    def attn_grad(n, _):
        cols = pl.ds(pl.multiple_of(n * LANES, LANES), LANES)
        left = nrm[:, cols]
        ga[cols, HD : 2 * HD] = contract_first(left, dq[...]).astype(BF16)
        ga[cols, 2 * HD :] = contract_first(left, dkv_cols[...].reshape(T, LANES)).astype(BF16)
        return 0

    lax.fori_loop(0, D // LANES, attn_grad, 0)
    weight_send(7)
    weight_send(8)
    kc = sum4(k4)
    meet4(kr, block_all)
    save_block = pltpu.make_async_copy(block_all, out_block, ls.at[3])
    save_block.start()
    d_normed = finish4(kc)
    copy(kc, p4_sum, p4_chip, chip_of(1 - y, 2)).wait_send()
    for i in range(2):
        copy(k4 + i, p4.at[i, 1 - core], p4_core.at[i], partner).wait_send()
    values = act[shard].astype(F32)
    d_input, gain_0 = rms_backward(d_normed, values, rms_factor(values), gain(0))
    input_all[y, core] = (dhid[...] + d_input).astype(BF16)
    gain_mine[0:1] = gain_0
    gain_mine[4:8] = jnp.zeros((4, D), F32)
    gain_mine[4:5, 0:HD] = gain_q
    gain_mine[5:6, 0:HD] = gain_k
    kn = slots(4 + 1 + C)
    for i in range(1, 4):
        send(kn + i, gain_mine, gain_tensor.at[i], {"tensor": (t + i) % 4})
    ki = share4(input_all)
    weight_push(6)
    total = gain_mine[...]
    for i in range(1, 4):
        arrive(kn + i, gain_tensor.at[i])
        total = total + gain_tensor[i]
    gain_tensor[0] = total
    send(kn, gain_tensor.at[0], gain_x.at[0], across)
    weight_meet(0, 1, 2)
    weight_end(2)
    weight_push(7)
    weight_push(8)
    meet4(ki, input_all)
    save_input = pltpu.make_async_copy(input_all, out_input, ls.at[4])
    save_input.start()
    arrive(kn, gain_x.at[0])
    gain_x[1] = total + gain_x[0]
    for step in range(1, C):
        send(kn + 4 + step, gain_x.at[1], gain_z.at[step], along(step))
    weight_meet(3, 4)
    weight_end(0)
    weight_meet(5, 7)
    attn = ga[rows_of(f, c)].astype(F32)
    for step in range(1, C):
        attn = attn + ga_z[step - 1].astype(F32)
    kvg[t] = attn[:, 2 * HD :]
    kh = slots(4)
    for i in range(1, 4):
        send(kh + i, kvg.at[t], kvg.at[t], {"tensor": (t + i) % 4})
    st_out[...] = attn[:, 0:HD]
    st_query[...] = attn[:, HD : 2 * HD]
    staged = []

    def save(n, src, dst):
        staged.append(pltpu.make_async_copy(src, dst, ls.at[10 + n]))
        staged[-1].start()

    save(0, st_out, out_out)
    save(1, st_query, out_query)
    total = gain_x[1]
    for step in range(1, C):
        arrive(kn + 4 + step, gain_z.at[step])
        total = total + gain_z[step]
    owner = f * C + c
    moved = pltpu.roll(total, (D - owner * R) % D, 1)
    st_norm[...] = moved[0:4, 0:R]
    moved = pltpu.roll(total[:, 0:HD], (HD - owner * narrow) % HD, 1)
    st_head[...] = moved[4:6, 0:narrow]
    save(2, st_norm, out_norm)
    save(3, st_head, out_head)
    weight_meet(6, 8)
    weight_end(1)
    for i in range(1, 4):
        arrive(kh + i, kvg.at[(t - i + 4) % 4])
    for k in range(4):
        st_kv[:, k * LANES : (k + 1) * LANES] = kvg[k]
    save(4, st_kv, out_kv)
    save_block.wait()
    save_input.wait()
    for moved in staged:
        moved.wait()
    settle()

    @pl.when(c < C - 1)
    def _():
        copy(ks, seg_row, seg_left, {"context": c + 1}).wait_send()
        copy(kk, kv.at[own_half], kv.at[my_half], {"context": c + 1}).wait_send()

    @pl.when(c > 0)
    def _():
        copy(kt, ret_out, ret_in, {"context": c - 1}).wait_send()


def fused(
    mesh,
    activations,
    positions,
    seg_ids,
    norm_gains,
    head_gains,
    w_query,
    w_keyval,
    w_out,
    w_gateup,
    w_down,
    cotangent,
):
    C = mesh.shape["context"]
    T, D = activations.shape[1:]
    R, units = w_down.shape
    U = -(-units // (2 * LANES)) * LANES
    S = T // 4
    pack = -(-R // LANES) * LANES
    operands = (
        activations[0],
        positions,
        seg_ids,
        norm_gains,
        head_gains,
        w_gateup,
        w_down,
        cotangent[0],
        w_query,
        w_keyval,
        w_out,
    )
    scratch = [
        pltpu.VMEM((T, HD // 2), F32),
        pltpu.VMEM((T, HD // 2), F32),
        pltpu.VMEM((8, T), jnp.int32),
        pltpu.VMEM((T, 1), jnp.int32),
        pltpu.VMEM((LANES, pack), F32),
        pltpu.VMEM((R, LANES), BF16),
        pltpu.VMEM((2, 3, R, U), BF16),
        pltpu.VMEM((S, D), BF16),
        pltpu.VMEM((D, 2 * HD + 2 * LANES), BF16),
        pltpu.VMEM((3, D, U), BF16),
        pltpu.VMEM((8, T), jnp.int32),
        pltpu.VMEM((8, D), F32),
        pltpu.VMEM((8, HD), F32),
        pltpu.VMEM((T, D), BF16),
        pltpu.VMEM((T, HD), F32),
        pltpu.VMEM((4, T, LANES), BF16),
        pltpu.VMEM((T, HD), BF16),
        pltpu.VMEM((2 * T, 2 * HD), BF16),
        pltpu.VMEM((T, 2 * T), F32),
        pltpu.VMEM((T, HD), BF16),
        pltpu.VMEM((2, 2, S, D), BF16),
        pltpu.VMEM((2, S, D), BF16),
        pltpu.VMEM((S, D), BF16),
        pltpu.VMEM((S, D), BF16),
        pltpu.VMEM((S, D), F32),
        pltpu.VMEM((S, D), F32),
        pltpu.VMEM((4, 2, S, D), BF16),
        pltpu.VMEM((4, 2 * S, U), BF16),
        pltpu.VMEM((4, 2 * S, U), BF16),
        pltpu.VMEM((4, 2 * S, U), BF16),
        pltpu.VMEM((4, 2, S, D), BF16),
        pltpu.VMEM((4, S, D), BF16),
        pltpu.VMEM((3, S, D), BF16),
        pltpu.VMEM((3, S, D), BF16),
        pltpu.VMEM((4, 2, S, D), BF16),
        pltpu.VMEM((S, D), F32),
        pltpu.VMEM((2, 2, S, D), BF16),
        pltpu.VMEM((T, 2 * T), BF16),
        pltpu.VMEM((T, HD), BF16),
        pltpu.VMEM((T, HD), BF16),
        pltpu.VMEM((2, 2, 2, S, 2 * HD), BF16),
        pltpu.VMEM((2, 2, S, 2 * HD), BF16),
        pltpu.VMEM((2, S, 2 * HD), BF16),
        pltpu.VMEM((2, S, 2 * HD), BF16),
        pltpu.VMEM((S, 2 * HD), BF16),
        pltpu.VMEM((S, 2 * HD), BF16),
        pltpu.VMEM((4, S, LANES), BF16),
        pltpu.VMEM((4, S, LANES), BF16),
        pltpu.VMEM((3, C * R, U), BF16),
        pltpu.VMEM((C - 1, 3, R, U), BF16),
        pltpu.VMEM((D, 2 * HD + LANES), BF16),
        pltpu.VMEM((C * R, 2 * HD + LANES), BF16),
        pltpu.VMEM((C - 1, R, 2 * HD + LANES), BF16),
        pltpu.VMEM((4, R, LANES), F32),
        pltpu.VMEM((R, units), F32),
        pltpu.VMEM((8, D), F32),
        pltpu.VMEM((4, 8, D), F32),
        pltpu.VMEM((2, 8, D), F32),
        pltpu.VMEM((C, 8, D), F32),
        pltpu.VMEM((2, 2, S, D), BF16),
        pltpu.VMEM((2, 2, S, D), BF16),
        pltpu.VMEM((R, HD), F32),
        pltpu.VMEM((R, HD), F32),
        pltpu.VMEM(norm_gains.shape, F32),
        pltpu.VMEM(head_gains.shape, F32),
        pltpu.VMEM((R, 2 * HD), F32),
        pltpu.SemaphoreType.DMA((SEMAPHORES,)),
        pltpu.SemaphoreType.DMA((SEMAPHORES,)),
        pltpu.SemaphoreType.DMA((15,)),
    ]
    vmem = pl.BlockSpec(memory_space=pltpu.VMEM)
    anywhere = pl.BlockSpec(memory_space=pl.ANY)
    results = (
        jax.ShapeDtypeStruct((2, 2, S, D), BF16),
        jax.ShapeDtypeStruct((2, 2, S, D), BF16),
        jax.ShapeDtypeStruct(norm_gains.shape, F32),
        jax.ShapeDtypeStruct(head_gains.shape, F32),
        jax.ShapeDtypeStruct(w_query.shape, F32),
        jax.ShapeDtypeStruct(w_keyval.shape, F32),
        jax.ShapeDtypeStruct(w_out.shape, F32),
        jax.ShapeDtypeStruct(w_gateup.shape, F32),
        jax.ShapeDtypeStruct(w_down.shape, F32),
    )
    sizes = {"context": C, "tokens": T, "width": D, "rows": R, "units": U}
    parts = pl.pallas_call(
        functools.partial(fused_kernel, sizes),
        out_shape=results,
        in_specs=[vmem] * 7 + [anywhere] * 4,
        out_specs=[anywhere] * len(results),
        scratch_shapes=scratch,
        compiler_params=pltpu.CompilerParams(
            collective_id=0, has_side_effects=True, vmem_limit_bytes=67043328
        ),
    )(*operands)
    count = len(parts)
    block_out, input_grad, *grads = pl.pallas_call(
        functools.partial(emit_kernel, count),
        out_shape=results,
        in_specs=[anywhere] * count,
        out_specs=[anywhere] * count,
        scratch_shapes=[pltpu.VMEM(part.shape, part.dtype) for part in parts]
        + [pltpu.SemaphoreType.DMA((count,))] * 2,
    )(*parts)
    return block_out.reshape(1, T, D), input_grad.reshape(1, T, D), *grads


def block(mesh, *arrays):
    tokens, rows = arrays[0].shape[1], arrays[9].shape[0]
    fits = (
        mesh.shape["fsdp"] == 2
        and mesh.shape["tensor"] == 4
        and mesh.shape["context"] == 4
        and tokens == WINDOW
        and rows % 16 == 0
        and arrays[5].shape[1] == HD
        and arrays[6].shape[1] == 4 * LANES
    )
    return fused(mesh, *arrays) if fits else shards(*arrays)


def shards(
    activations,
    positions,
    seg_ids,
    norm_gains,
    head_gains,
    w_query,
    w_keyval,
    w_out,
    w_gateup,
    w_down,
    cotangent,
):
    tokens = activations.shape[1]
    local_heads = w_query.shape[1] // HD
    inputs = activations[0].astype(jnp.float32)
    places = positions[0]
    documents = seg_ids[0]
    gains_all, heads_all, query_all, keyval_all, out_all = (
        lax.all_gather(norm_gains, ("fsdp", "context"), axis=1, tiled=True),
        lax.all_gather(head_gains, ("fsdp", "context"), axis=1, tiled=True),
        lax.all_gather(w_query, ("fsdp", "context"), axis=0, tiled=True),
        lax.all_gather(w_keyval, ("fsdp", "context"), axis=0, tiled=True),
        lax.all_gather(w_out, ("fsdp", "context"), axis=0, tiled=True),
    )
    gains_f = gains_all.astype(jnp.float32)
    heads_f = heads_all.astype(jnp.float32)
    normed_f, input_back = jax.vjp(rms_norm, inputs, gains_f[0])
    normed = normed_f.astype(jnp.bfloat16)
    query_raw = jnp.dot(normed, query_all, preferred_element_type=jnp.float32).reshape(
        tokens, local_heads, HD
    )
    keyval_raw = jnp.dot(normed, keyval_all, preferred_element_type=jnp.float32)

    def prepare(raw_heads, head_gain):
        return rotate(rms_norm(raw_heads, head_gain), places)

    query_rot, query_back = jax.vjp(prepare, query_raw, heads_f[0])
    key_rot, key_back = jax.vjp(prepare, keyval_raw[:, None, :HD], heads_f[1])
    queries = query_rot.astype(jnp.bfloat16)
    own_keyval = jnp.concatenate([key_rot[:, 0], keyval_raw[:, HD:]], axis=1).astype(jnp.bfloat16)
    labels = jnp.stack([places, documents])
    keep_from = tokens - tokens
    left_keyval, left_labels = from_behind((own_keyval, labels), "context", 1)
    keys_all = jnp.concatenate([left_keyval, own_keyval], axis=0)
    key_places = jnp.concatenate([left_labels[0], places])
    key_documents = jnp.concatenate([left_labels[1], documents])
    has_left = lax.axis_index("context") > 0
    key_live = jnp.concatenate([jnp.full((tokens,), has_left), jnp.ones((tokens,), dtype=bool)])
    scale_factor = HD ** (-0.5)
    block_rows = 512
    block_starts = jnp.arange(tokens // block_rows) * block_rows

    def block_scores():
        spacing = places[:, None] - key_places[None, :]
        visible = (
            key_live[None, :]
            & (documents[:, None] == key_documents[None, :])
            & (spacing >= 0)
            & (spacing < WINDOW)
        )
        raw_scores = (
            jnp.einsum("qhd,kd->hqk", queries, keys_all[:, :HD], preferred_element_type=jnp.float32)
            * scale_factor
        )
        return (jnp.where(visible[None], raw_scores, -1e30), keys_all, queries)

    def forward_block(start):
        scores, near_keyval, query_block = block_scores()
        row_top = jnp.max(scores, axis=-1, keepdims=True)
        raised = jnp.exp(scores - row_top)
        row_total = jnp.sum(raised, axis=-1, keepdims=True)
        probs = raised / row_total
        mixed_block = jnp.einsum(
            "hqk,kd->qhd",
            probs.astype(jnp.bfloat16),
            near_keyval[:, HD:],
            preferred_element_type=jnp.float32,
        )
        return (mixed_block.astype(jnp.bfloat16), row_top + jnp.log(row_total))

    mixed_blocks, log_blocks = lax.map(forward_block, block_starts)
    mixed_low = mixed_blocks.reshape(tokens, local_heads * HD)
    branch = lax.psum(contract_last(mixed_low, out_all).astype(jnp.bfloat16), "tensor").astype(jnp.float32)
    post_attn, post_attn_back = jax.vjp(rms_norm, branch, gains_f[1])
    hidden = inputs + post_attn
    normed_mlp_f, pre_mlp_back = jax.vjp(rms_norm, hidden, gains_f[2])
    normed_mlp = normed_mlp_f.astype(jnp.bfloat16)
    columns = normed_mlp
    gate_up = jnp.einsum(
        "bn,nkf->bkf",
        columns,
        lax.all_gather(w_gateup, ("fsdp", "context"), axis=0, tiled=True),
        preferred_element_type=jnp.float32,
    )
    active_f, glu_back = jax.vjp(glu, gate_up)
    active = active_f.astype(jnp.bfloat16)
    down = lax.psum(
        contract_last(
            active, lax.all_gather(w_down, ("fsdp", "context"), axis=0, tiled=True)
        ).astype(jnp.bfloat16),
        "tensor",
    ).astype(jnp.float32)
    post_mlp, post_mlp_back = jax.vjp(rms_norm, down, gains_f[3])
    result = hidden + post_mlp
    grad_out = cotangent[0].astype(jnp.float32)
    d_down, gain_post_mlp = post_mlp_back(grad_out)
    down_low = d_down.astype(jnp.bfloat16)
    columns = down_low
    d_active = jnp.dot(
        columns,
        lax.all_gather(w_down, ("fsdp", "context"), axis=0, tiled=True),
        preferred_element_type=jnp.float32,
    )
    d_gate_up = glu_back(d_active)[0].astype(jnp.bfloat16)
    d_normed_part = jnp.einsum(
        "bkf,nkf->bn",
        d_gate_up,
        lax.all_gather(w_gateup, ("fsdp", "context"), axis=0, tiled=True),
        preferred_element_type=jnp.float32,
    )
    d_normed_mlp = lax.psum(d_normed_part.astype(jnp.bfloat16), "tensor").astype(jnp.float32)
    d_hidden_norm, gain_pre_mlp = pre_mlp_back(d_normed_mlp)
    d_hidden = grad_out + d_hidden_norm
    features = normed_mlp
    grad_cols = down_low
    gate_up_term = jnp.einsum(
        "bn,bkf->nkf", features, d_gate_up, preferred_element_type=jnp.float32
    )
    down_term = contract_first(grad_cols, active)
    scatter = lambda part: lax.psum_scatter(
        part.astype(jnp.bfloat16), ("fsdp", "context"), scatter_dimension=0, tiled=True
    ).astype(jnp.float32)
    gate_grad = scatter(gate_up_term[:, 0])
    up_grad = scatter(gate_up_term[:, 1])
    down_grad = scatter(down_term)
    d_branch, gain_post_attn = post_attn_back(d_hidden)
    branch_low = d_branch.astype(jnp.bfloat16)
    d_mixed = jnp.dot(branch_low, out_all, preferred_element_type=jnp.float32)
    d_mixed_low = d_mixed.astype(jnp.bfloat16).reshape(tokens, local_heads, HD)

    def backward_block(carry, item):
        start, log_block = item
        scores, near_keyval, query_block = block_scores()
        probs_again = jnp.exp(scores - log_block)
        d_probs = jnp.einsum(
            "qhd,kd->hqk", d_mixed_low, near_keyval[:, HD:], preferred_element_type=jnp.float32
        )
        row_inner = jnp.sum(probs_again * d_probs, axis=-1, keepdims=True)
        d_scores = (probs_again * (d_probs - row_inner)).astype(jnp.bfloat16)
        d_query_block = (
            jnp.einsum(
                "hqk,kd->qhd", d_scores, near_keyval[:, :HD], preferred_element_type=jnp.float32
            )
            * scale_factor
        )
        d_keys = (
            jnp.einsum("hqk,qhd->kd", d_scores, query_block, preferred_element_type=jnp.float32)
            * scale_factor
        )
        d_values = jnp.einsum(
            "hqk,qhd->kd",
            probs_again.astype(jnp.bfloat16),
            d_mixed_low,
            preferred_element_type=jnp.float32,
        )
        updated = carry + jnp.concatenate([d_keys, d_values], axis=1)
        return (updated, d_query_block)

    d_keyval, d_query_blocks = lax.scan(
        backward_block,
        jnp.zeros((tokens + tokens, 2 * HD), jnp.float32),
        (block_starts, log_blocks),
    )
    d_queries = d_query_blocks.reshape(tokens, local_heads, HD)
    returned = from_behind(d_keyval[:tokens].astype(jnp.bfloat16), "context", -1).astype(
        jnp.float32
    )
    own_grad = d_keyval[tokens:].at[keep_from:].add(returned)
    d_query_raw, gain_query = query_back(d_queries)
    d_query_low = d_query_raw.reshape(tokens, local_heads * HD).astype(jnp.bfloat16)
    d_normed_query, keyval_grad, gain_query_all = (
        lax.psum(contract_last(d_query_low, query_all).astype(jnp.bfloat16), "tensor").astype(
            jnp.float32
        ),
        lax.psum(own_grad.astype(jnp.bfloat16), "tensor").astype(jnp.float32),
        lax.psum(gain_query.astype(jnp.bfloat16), "tensor").astype(jnp.float32),
    )
    d_key_raw, gain_key = key_back(keyval_grad[:, None, :HD])
    d_keyval_low = jnp.concatenate([d_key_raw[:, 0], keyval_grad[:, HD:]], axis=1).astype(
        jnp.bfloat16
    )
    d_normed = d_normed_query + contract_last(d_keyval_low, keyval_all)
    d_input_norm, gain_input = input_back(d_normed)
    input_total = d_hidden + d_input_norm
    features = normed
    grad_cols = branch_low
    attn_grads = lax.psum_scatter(
        jnp.stack(
            [contract_first(features, d_query_low), contract_first(grad_cols, mixed_low)], axis=1
        ).astype(jnp.bfloat16),
        ("fsdp", "context"),
        scatter_dimension=0,
        tiled=True,
    ).astype(jnp.float32)
    keyval_term = contract_first(normed, d_keyval_low)
    gain_terms = jnp.stack([gain_input, gain_post_attn, gain_pre_mlp, gain_post_mlp])
    head_terms = jnp.stack([gain_query_all, gain_key])
    gain_grad, head_grad, keyval_weight_grad = (
        lax.psum_scatter(
            gain_terms.astype(jnp.bfloat16), ("fsdp", "context"), scatter_dimension=1, tiled=True
        ).astype(jnp.float32),
        lax.psum_scatter(
            head_terms.astype(jnp.bfloat16), ("fsdp", "context"), scatter_dimension=1, tiled=True
        ).astype(jnp.float32),
        lax.psum_scatter(
            keyval_term.astype(jnp.bfloat16), ("fsdp", "context"), scatter_dimension=0, tiled=True
        ).astype(jnp.float32),
    )
    return (
        result[None].astype(jnp.bfloat16),
        input_total[None].astype(jnp.bfloat16),
        gain_grad,
        head_grad,
        attn_grads[:, 0],
        keyval_weight_grad,
        attn_grads[:, 1],
        jnp.stack([gate_grad, up_grad], axis=1),
        down_grad,
    )


def solution(mesh):
    return jax.shard_map(
        functools.partial(block, mesh),
        mesh=mesh,
        in_specs=(
            P("fsdp", "context", None),
            P("fsdp", "context"),
            P("fsdp", "context"),
            P(None, ("fsdp", "context")),
            P(None, ("fsdp", "context")),
            P(("fsdp", "context"), "tensor"),
            P(("fsdp", "context"), None),
            P(("fsdp", "context"), "tensor"),
            P(("fsdp", "context"), None, "tensor"),
            P(("fsdp", "context"), "tensor"),
            P("fsdp", "context", None),
        ),
        out_specs=(
            P("fsdp", "context", None),
            P("fsdp", "context", None),
            P(None, ("fsdp", "context")),
            P(None, ("fsdp", "context")),
            P(("fsdp", "context"), "tensor"),
            P(("fsdp", "context"), None),
            P(("fsdp", "context"), "tensor"),
            P(("fsdp", "context"), None, "tensor"),
            P(("fsdp", "context"), "tensor"),
        ),
        check_vma=False,
    )
```

```python
import functools
import math

import jax
import jax.numpy as jnp
from jax import lax
from jax.experimental import pallas as pl
from jax.experimental.pallas import tpu as pltpu
from jax.sharding import PartitionSpec as P

HD = 256
WINDOW = 512


EPSILON = 1e-06


def from_behind(block, axis, distance):
    devices = range(lax.axis_size(axis))
    route = [(i - distance, i) for i in devices if i - distance in devices]
    return lax.ppermute(block, axis, route)


def rms_norm(values, gain):
    factor = lax.rsqrt(jnp.mean(values * values, axis=-1, keepdims=True) + EPSILON)
    return values * factor * gain


def rotate(tensor, places):
    width_all = tensor.shape[-1]
    half_width = width_all // 2
    freqs = jnp.power(10000.0, -jnp.arange(half_width, dtype=jnp.float32) * 2.0 / width_all)
    angles = places.astype(jnp.float32)[:, None] * freqs[None, :]
    cosine = jnp.cos(angles)[:, None, :]
    sine = jnp.sin(angles)[:, None, :]
    first_half = tensor[..., :half_width]
    second_half = tensor[..., half_width:]
    return jnp.concatenate(
        [first_half * cosine - second_half * sine, second_half * cosine + first_half * sine],
        axis=-1,
    )


def glu(gate_up):
    return jax.nn.gelu(gate_up[:, 0], approximate=True) * gate_up[:, 1]


def contract_last(left_side, right_side):
    return lax.dot_general(
        left_side, right_side, (((1,), (1,)), ((), ())), preferred_element_type=jnp.float32
    )


def contract_first(left_side, right_side):
    return lax.dot_general(
        left_side, right_side, (((0,), (0,)), ((), ())), preferred_element_type=jnp.float32
    )


MESH = pl.DeviceIdType.MESH
F32 = jnp.float32
BF16 = jnp.bfloat16
LANES = 128
SEMAPHORES = 174


def mm(left, right):
    return jnp.dot(left, right, preferred_element_type=F32)


def rms_factor(values):
    return lax.rsqrt(jnp.mean(values * values, axis=-1, keepdims=True) + EPSILON)


def rms_backward(grad, values, factor, gain):
    unit = values * factor
    scaled = grad * gain
    inner = jnp.mean(scaled * unit, axis=-1, keepdims=True)
    return factor * (scaled - unit * inner), jnp.sum(grad * unit, axis=0, keepdims=True)


def turn(values, cosine, sine):
    half = values.shape[-1] // 2
    first, second = values[:, :half], values[:, half:]
    return jnp.concatenate([first * cosine - second * sine, second * cosine + first * sine], axis=1)


def turn_back(values, cosine, sine):
    half = values.shape[-1] // 2
    first, second = values[:, :half], values[:, half:]
    return jnp.concatenate([first * cosine + second * sine, second * cosine - first * sine], axis=1)


def emit_kernel(count, *refs):
    sources, results, held = refs[:count], refs[count : 2 * count], refs[2 * count : 3 * count]
    incoming, outgoing = refs[3 * count :]
    reads = [pltpu.make_async_copy(sources[n], held[n], incoming.at[n]) for n in range(count)]
    writes = [pltpu.make_async_copy(held[n], results[n], outgoing.at[n]) for n in range(count)]
    for moved in reads:
        moved.start()
    for n in range(count):
        reads[n].wait()
        writes[n].start()
    for moved in writes:
        moved.wait()


def fused_kernel(
    sizes,
    act,
    positions,
    seg_ids,
    norm_gains,
    head_gains,
    w_gateup,
    w_down,
    cot_all,
    w_query,
    w_keyval,
    w_out,
    out_block,
    out_input,
    out_norm,
    out_head,
    out_query,
    out_kv,
    out_out,
    out_gateup,
    out_down,
    cosine,
    sine,
    seg_row,
    seg_col,
    gain_pack,
    gain_all,
    w_ff,
    cot,
    wa,
    wf,
    seg_left,
    gain_rows,
    head_rows,
    nrm,
    qraw,
    kv_raw,
    qs,
    kv,
    probs,
    mix,
    p4,
    p4_core,
    p4_sum,
    p4_chip,
    hid,
    bran,
    xg,
    gel,
    upg,
    active,
    p8,
    p8_core,
    p8_sum,
    p8_chip,
    dd,
    dhid,
    db,
    dscore,
    dmix,
    dq,
    kvp,
    kvp_core,
    kvp_sum,
    kvp_chip,
    ret_out,
    ret_in,
    dkv_mine,
    dkv_cols,
    gall_x,
    gall_z,
    ga,
    ga_x,
    ga_z,
    kvg,
    ff_stage,
    gain_mine,
    gain_tensor,
    gain_x,
    gain_z,
    block_all,
    input_all,
    st_out,
    st_query,
    st_norm,
    st_head,
    st_kv,
    ss,
    rs,
    ls,
):
    C = sizes["context"]
    T, D, R, U = sizes["tokens"], sizes["width"], sizes["rows"], sizes["units"]
    units = w_down.shape[1]
    narrow = HD // (2 * C)
    S = T // 4
    f = lax.axis_index("fsdp")
    c = lax.axis_index("context")
    t = lax.axis_index("tensor")
    y, core = t // 2, t % 2
    m = c % 2
    base = c - m
    partner = {"tensor": y * 2 + (1 - core)}
    across = {"fsdp": 1 - f}
    counter = [0]
    sent = []

    def slots(count):
        first = counter[0]
        counter[0] += count
        assert counter[0] <= SEMAPHORES
        return first

    def copy(k, src, dst, device):
        return pltpu.make_async_remote_copy(
            src_ref=src,
            dst_ref=dst,
            send_sem=ss.at[k],
            recv_sem=rs.at[k],
            device_id=device,
            device_id_type=MESH,
        )

    def send(k, src, dst, device):
        moved = copy(k, src, dst, device)
        moved.start()
        sent.append(moved)

    def arrive(k, dst):
        copy(k, dst, dst, partner).wait_recv()

    def settle():
        for moved in sent:
            moved.wait_send()
        sent.clear()

    def along(step):
        return {"context": (c + step) % C}

    def rows_of(ff, cc):
        return pl.ds(pl.multiple_of((ff * C + cc) * R, R), R)

    def chip_of(k, count):
        if count == 2:
            return {"tensor": k * 2 + core}
        return {"context": base + k // 2, "tensor": (k % 2) * 2 + core}

    barrier = pltpu.get_barrier_semaphore()
    greeted = [along(step) for step in range(1, C)] + [across]
    greeted += [{"tensor": (t + step) % 4} for step in range(1, 4)]
    greeted += [{"context": base + 1 - m, "tensor": (1 - y) * 2 + core}]
    for device in greeted:
        pl.semaphore_signal(barrier, inc=1, device_id=device, device_id_type=MESH)
    gain_pack[...] = jnp.zeros(gain_pack.shape, F32)
    gain_pack[0:4, 0:R] = norm_gains[...].astype(F32)
    gain_pack[4:6, 0:narrow] = head_gains[...].astype(F32)
    seg_row[...] = jnp.broadcast_to(seg_ids[...], seg_row.shape)
    pl.semaphore_wait(barrier, len(greeted))

    mine = rows_of(f, c)
    kv_cols = pl.ds(pl.multiple_of(t * LANES, LANES), LANES)
    attn_parts = (
        (w_query, slice(0, HD)),
        (w_keyval.at[:, kv_cols], slice(HD, HD + LANES)),
        (w_out, slice(HD + LANES, 2 * HD + LANES)),
    )
    q_cols, kv_part, o_cols = (cols for _, cols in attn_parts[:3])
    local = []
    for n, (part, cols) in enumerate(attn_parts):
        local.append(pltpu.make_async_copy(part, wa.at[mine, cols], ls.at[6 + n]))
        local[-1].start()
    ka = slots(3 * C)
    kar = slots(C - 1)
    kg = slots(2 * C - 1)
    for step in range(1, C):
        for n, (part, cols) in enumerate(attn_parts):
            send(ka + 3 * step + n, part, wa.at[mine, cols], along(step))
    for n, (part, cols) in enumerate(attn_parts):
        send(ka + n, part, wa.at[mine, cols], across)
    own_gain = gain_all.at[f * C + c]
    gain_all[f * C + c] = gain_pack[...]
    for step in range(1, C):
        send(kg + step, gain_pack, own_gain, along(step))
    send(kg, gain_pack, own_gain, across)
    ks = slots(1)

    @pl.when(c < C - 1)
    def _():
        copy(ks, seg_row, seg_left, {"context": c + 1}).start()

    pieces = ((0, 0, 384), (0, 384, U), (1, 0, 512), (1, 512, U), (2, 0, 512), (2, 512, U))
    kf = slots((2 * C - 1) * len(pieces))

    def piece(p, rows):
        w, low, high = pieces[p]
        return wf.at[w, rows, low:high]

    side = c // 2
    near, far = 2 - side, 3 * (1 - side)

    def send_ff(p):
        k = kf + (2 * C - 1) * p
        w, low, high = pieces[p]
        turns = tuple((c + step) % C for step in range(1, C))
        for to in (base + 1 - m, near, far) if p in (3, 4) else turns:
            send(
                k + (to - c + C) % C,
                w_ff.at[to % 2, w, :, low:high],
                piece(p, mine),
                {"context": to},
            )
        send(k, w_ff.at[m, w, :, low:high], piece(p, mine), across)

    def relay_ff(p):
        k = kf + (2 * C - 1) * p
        for source in (base + 1 - m, near, far):
            step = (c - source + C) % C
            part = piece(p, rows_of(f, source))
            arrive(k + step, part)
            send(k + C - 1 + step, part, part, across)

    def meet_ff(p):
        k = kf + (2 * C - 1) * p
        arrive(k, piece(p, rows_of(1 - f, c)))
        for step in range(1, C):
            arrive(k + C - 1 + step, piece(p, rows_of(1 - f, (c - step + C) % C)))

    for w in range(3):
        whole = w_down[...] if w == 2 else w_gateup[:, w, :]
        w_ff[0, w] = whole[:, 0:U]
        w_ff[1, w, :, 0 : units - U] = whole[:, U:units]
        w_ff[1, w, :, units - U :] = jnp.zeros((R, 2 * U - units), BF16)
    seg_col[...] = jnp.transpose(seg_row[...].astype(F32))[:, 0:1].astype(jnp.int32)
    place = jnp.broadcast_to(positions[...].astype(F32), (8, T))
    index = lax.broadcasted_iota(jnp.int32, (1, HD // 2), 1).astype(F32)
    angle = jnp.transpose(place)[:, 0:1] * jnp.exp(index * (-2.0 * math.log(10000.0) / HD))
    cosine[...] = jnp.cos(angle)
    sine[...] = jnp.sin(angle)
    shard = pl.ds(pl.multiple_of(t * S, S), S)
    own_cot = pltpu.make_async_copy(cot_all.at[shard], cot, ls.at[2])
    own_cot.start()
    own_ff = pltpu.make_async_copy(w_ff.at[m], wf.at[:, mine], ls.at[1])
    own_ff.start()
    for step in range(1, C):
        other = rows_of(f, (c - step + C) % C)
        for n, (_, cols) in enumerate(attn_parts):
            arrive(ka + 3 * step + n, wa.at[other, cols])
        send(kar + step - 1, wa.at[other], wa.at[other], across)
        part = gain_all.at[f * C + (c - step + C) % C]
        arrive(kg + step, part)
        send(kg + C - 1 + step, part, part, across)
    for moved in local:
        moved.wait()
    send_ff(0)
    for n, (_, cols) in enumerate(attn_parts):
        arrive(ka + n, wa.at[rows_of(1 - f, c), cols])
    for step in range(1, C):
        arrive(kar + step - 1, wa.at[rows_of(1 - f, (c - step + C) % C)])

    @pl.when(c > 0)
    def _():
        arrive(ks, seg_left)

    @pl.when(c == 0)
    def _():
        seg_left[...] = jnp.full(seg_left.shape, -1, jnp.int32)
        kv[0:T] = jnp.zeros((T, 2 * HD), BF16)

    arrive(kg, gain_all.at[(1 - f) * C + c])
    for step in range(1, C):
        arrive(kg + C - 1 + step, gain_all.at[(1 - f) * C + (c - step + C) % C])
    wide = jnp.zeros((8, D), F32)
    heads = jnp.zeros((8, HD), F32)
    blank = jnp.zeros((8, D - gain_pack.shape[1]), F32)
    for j in range(2 * C):
        part = gain_all[j]
        wide = wide + pltpu.roll(jnp.concatenate([part, blank], axis=1), j * R, 1)
        heads = heads + pltpu.roll(part[:, 0:HD], j * narrow, 1)
    gain_rows[...] = wide
    head_rows[...] = heads

    def gain(index):
        return gain_rows[index : index + 1]

    def head_gain(index):
        return head_rows[4 + index : 5 + index]

    half = T // 2

    def project(i, _):
        rows = pl.ds(pl.multiple_of(i * half, half), half)
        values = act[rows].astype(F32)
        low = (values * rms_factor(values) * gain(0)).astype(BF16)
        nrm[rows] = low
        kv_raw[t, rows] = mm(low, wa[:, kv_part]).astype(BF16)
        return 0

    lax.fori_loop(0, 2, project, 0)
    ku = slots(4)
    for i in range(1, 4):
        send(ku + i, kv_raw.at[t], kv_raw.at[t], {"tensor": (t + i) % 4})

    def query(i, _):
        rows = pl.ds(pl.multiple_of(i * half, half), half)
        raw_q = mm(nrm[rows], wa[:, q_cols])
        qraw[rows] = raw_q
        qs[rows] = turn(
            raw_q * rms_factor(raw_q) * head_gain(0), cosine[rows], sine[rows]
        ).astype(BF16)
        return 0

    lax.fori_loop(0, 2, query, 0)
    for i in range(1, 4):
        arrive(ku + i, kv_raw.at[(t - i + 4) % 4])

    def key(i, _):
        rows = pl.ds(pl.multiple_of(i * half, half), half)
        raw_k = jnp.concatenate([kv_raw[0, rows], kv_raw[1, rows]], axis=1).astype(F32)
        own = pl.ds(pl.multiple_of(T + i * half, half), half)
        kv[own, 0:HD] = turn(
            raw_k * rms_factor(raw_k) * head_gain(1), cosine[rows], sine[rows]
        ).astype(BF16)
        kv[own, HD : HD + LANES] = kv_raw[2, rows]
        kv[own, HD + LANES :] = kv_raw[3, rows]
        return 0

    lax.fori_loop(0, 2, key, 0)
    kk = slots(2)
    my_half = pl.ds(pl.multiple_of(core * half, half), half)
    other_half = pl.ds(pl.multiple_of((1 - core) * half, half), half)
    own_half = pl.ds(pl.multiple_of(T + core * half, half), half)

    @pl.when(c < C - 1)
    def _():
        copy(kk, kv.at[own_half], kv.at[my_half], {"context": c + 1}).start()

    send_ff(1)
    send_ff(2)
    relay_ff(0)

    @pl.when(c > 0)
    def _():
        arrive(kk, kv.at[my_half])
        moved = copy(kk + 1, kv.at[my_half], kv.at[my_half], partner)
        moved.start()
        arrive(kk + 1, kv.at[other_half])
        moved.wait_send()

    scale = HD**-0.5
    no_left = jnp.where(c > 0, 0, 2 * T)
    k4 = slots(2)

    def attend(i, _):
        rows = pl.ds(pl.multiple_of(i * half, half), half)
        q = qs[rows]
        labels = seg_col[rows]
        row = lax.broadcasted_iota(jnp.int32, (half, T), 0) + i * half
        col = lax.broadcasted_iota(jnp.int32, (half, T), 1)
        left = contract_last(q, kv[0:T, 0:HD]) * scale
        left = jnp.where((labels == seg_left[0:1]) & (col > row + no_left), left, -1e30)
        own = contract_last(q, kv[T:, 0:HD]) * scale
        own = jnp.where((labels == seg_row[0:1]) & (col <= row), own, -1e30)
        top = jnp.maximum(
            jnp.max(left, axis=1, keepdims=True), jnp.max(own, axis=1, keepdims=True)
        )
        left, own = jnp.exp(left - top), jnp.exp(own - top)
        total = jnp.sum(left, axis=1, keepdims=True) + jnp.sum(own, axis=1, keepdims=True)
        left, own = left / total, own / total
        probs[rows, 0:T] = left
        probs[rows, T:] = own
        mixed = mm(left.astype(BF16), kv[0:T, HD:]) + mm(own.astype(BF16), kv[T:, HD:])
        mixed = mixed.astype(BF16)
        mix[rows] = mixed
        part = contract_last(mixed, wa[:, o_cols]).astype(BF16)
        p4[i, 0] = part[0:S]
        p4[i, 1] = part[S:]
        copy(k4 + i, p4.at[i, 1 - core], p4_core.at[i], partner).start()
        return 0

    lax.fori_loop(0, 2, attend, 0)

    def sum4(k):
        kc = slots(1)
        arrive(k + (1 - y), p4_core.at[1 - y])
        p4_sum[...] = (
            p4[1 - y, core].astype(F32) + p4_core[1 - y].astype(F32)
        ).astype(BF16)
        copy(kc, p4_sum, p4_chip, chip_of(1 - y, 2)).start()
        arrive(k + y, p4_core.at[y])
        return kc

    def finish4(kc):
        arrive(kc, p4_chip)
        return (
            p4[y, core].astype(F32)
            + p4_core[y].astype(F32)
            + p4_chip[...].astype(F32)
        )

    kc = sum4(k4)
    relay_ff(1)
    branch = finish4(kc)
    copy(kc, p4_sum, p4_chip, chip_of(1 - y, 2)).wait_send()
    for i in range(2):
        copy(k4 + i, p4.at[i, 1 - core], p4_core.at[i], partner).wait_send()

    bran[...] = branch
    hidden = act[shard].astype(F32) + branch * rms_factor(branch) * gain(1)
    hid[...] = hidden
    low = (hidden * rms_factor(hidden) * gain(2)).astype(BF16)

    me = m * 2 + y

    def gather8(full, value):
        kg = slots(8)
        full[me, core] = value
        send(kg + 4, full.at[me, core], full.at[me, core], partner)
        for i in range(1, 4):
            send(kg + i, full.at[me, core], full.at[me, core], chip_of((me + i) % 4, 4))
        return kg

    def pass8(kg, full, i):
        k = (me - i + 4) % 4
        arrive(kg + i, full.at[k, core])
        copy(kg + 4 + i, full.at[k, core], full.at[k, core], partner).start()

    def meet8(kg, full, i):
        k = (me - i + 4) % 4
        arrive(kg + 4 + i, full.at[k, 1 - core])

    def settle8(kg, full):
        for i in range(1, 4):
            k = (me - i + 4) % 4
            copy(kg + 4 + i, full.at[k, core], full.at[k, core], partner).wait_send()

    def give8(ko, i):
        k = (me - i + 4) % 4
        copy(ko + i, p8.at[k, 1 - core], p8_core.at[i], partner).start()

    def push8(ko, i):
        k = (me - i + 4) % 4
        arrive(ko + i, p8_core.at[i])
        p8_sum[i - 1] = (
            p8[k, core].astype(F32) + p8_core[i].astype(F32)
        ).astype(BF16)
        copy(ko + 4 + i, p8_sum.at[i - 1], p8_chip.at[i - 1], chip_of(k, 4)).start()

    def finish8(ko):
        arrive(ko, p8_core.at[0])
        total = p8[me, core].astype(F32) + p8_core[0].astype(F32)
        for i in range(1, 4):
            arrive(ko + 4 + i, p8_chip.at[i - 1])
            total = total + p8_chip[i - 1].astype(F32)
        for i in range(4):
            copy(ko + i, p8.at[0, 1 - core], p8_core.at[i], partner).wait_send()
        for i in range(1, 4):
            copy(ko + 4 + i, p8_sum.at[0], p8_chip.at[0], partner).wait_send()
        return total

    kx = slots(7)
    beside, beyond = m * 2 + 1 - y, (1 - m) * 2 + y
    corner = (1 - m) * 2 + 1 - y
    xg[me, core] = low
    send(kx + 2, xg.at[me, core], xg.at[me, core], chip_of(beyond, 4))
    send(kx + 1, xg.at[me, core], xg.at[me, core], chip_of(beside, 4))
    send(kx, xg.at[me, core], xg.at[me, core], partner)
    send_ff(3)
    send_ff(4)
    relay_ff(2)
    send_ff(5)
    for i, k in ((1, beside), (2, beyond), (3, corner)):
        part = xg.at[k, core]
        arrive(kx + i, part)
        if i == 2:
            send(kx + 3, part, part, chip_of(beside, 4))
        send(kx + 3 + i, part, part, partner)
    relay_ff(3)
    own_ff.wait()
    own_cot.wait()
    for p in range(4):
        meet_ff(p)
    arrive(kx, xg.at[me, 1 - core])
    for i, k in ((1, beside), (2, beyond), (3, corner)):
        arrive(kx + 3 + i, xg.at[k, 1 - core])
    root = 0.7978845608028654
    ko = slots(8)

    def forward(i, _):
        k = (me - i + 4) % 4
        x = xg[k].reshape(2 * S, D)
        gate = mm(x, wf[0])
        up = mm(x, wf[1])
        square = gate * gate
        bent = jnp.tanh(root * gate * (1.0 + 0.044715 * square))
        ramp = 0.5 * (1.0 + bent)
        gelu = gate * ramp
        slope = ramp + 0.5 * gate * (1.0 - bent * bent) * root * (1.0 + 3 * 0.044715 * square)
        gel[k] = gelu.astype(BF16)
        upg[k] = (up * slope).astype(BF16)
        active[k] = (gelu * up).astype(BF16)
        return 0

    lax.fori_loop(0, 2, forward, 0)
    relay_ff(4)
    lax.fori_loop(2, 4, forward, 0)
    relay_ff(5)
    meet_ff(4)
    meet_ff(5)

    def lower(i, _):
        k = (me - i + 4) % 4
        p8[k] = contract_last(active[k], wf[2]).astype(BF16).reshape(2, S, D)
        give8(ko, i)

        @pl.when(i > 1)
        def _():
            push8(ko, i - 1)

        return 0

    lax.fori_loop(0, 4, lower, 0)
    push8(ko, 3)
    down = finish8(ko)

    factor = rms_factor(down)
    grad = cot[...].astype(F32)
    result = (hid[...] + down * factor * gain(3)).astype(BF16)
    d_down, gain_3 = rms_backward(grad, down, factor, gain(3))
    gain_mine[3:4] = gain_3
    kd = gather8(dd, d_down.astype(BF16))

    def share4(full):
        kb = slots(3)
        send(kb, full.at[y, core], full.at[y, core], chip_of(1 - y, 2))
        send(kb + 1, full.at[y, core], full.at[y, core], partner)
        return kb

    def meet4(kb, full):
        arrive(kb, full.at[1 - y, core])
        send(kb + 2, full.at[1 - y, core], full.at[1 - y, core], partner)
        arrive(kb + 1, full.at[y, 1 - core])
        arrive(kb + 2, full.at[1 - y, 1 - core])

    block_all[y, core] = result
    ko2 = slots(8)

    def backward(i, _):
        k = (me - i + 4) % 4
        meet8(kd, dd, i)
        low = dd[k].reshape(2 * S, D)
        d_active = mm(low, wf[2])

        @pl.when(i < 3)
        def _():
            pass8(kd, dd, i + 1)

        d_gate = (d_active * upg[k].astype(F32)).astype(BF16)
        d_up = (d_active * gel[k].astype(F32)).astype(BF16)
        upg[k] = d_gate
        gel[k] = d_up
        p8[k] = (
            (contract_last(d_gate, wf[0]) + contract_last(d_up, wf[1]))
            .astype(BF16)
            .reshape(2, S, D)
        )
        give8(ko2, i)

        @pl.when(i > 1)
        def _():
            push8(ko2, i - 1)

        return 0

    lax.fori_loop(0, 4, backward, 0)
    push8(ko2, 3)
    settle8(kd, dd)

    settle()
    gall = wf
    mine_x = pl.ds(pl.multiple_of(f * C * R, C * R), C * R)
    theirs_x = pl.ds(pl.multiple_of((1 - f) * C * R, C * R), C * R)
    ff_chunk = lambda w, low, high: (
        gall.at[w, :, low:high],
        gall_x.at[w, :, low:high],
        gall_z.at[:, w, :, low:high],
    )
    attn_chunk = lambda low, high: (
        ga.at[:, low:high],
        ga_x.at[:, low:high],
        ga_z.at[:, :, low:high],
    )
    chunks = (
        ff_chunk(2, 0, 256),
        ff_chunk(2, 256, 512),
        ff_chunk(2, 512, U),
        ff_chunk(0, 0, 512),
        ff_chunk(0, 512, U),
        attn_chunk(0, HD),
        ff_chunk(1, 0, 640),
        attn_chunk(HD, 2 * HD + LANES),
        ff_chunk(1, 640, U),
    )
    kw = slots(len(chunks))
    kz = slots(len(chunks) * (C - 1))

    def weight_grad(w, left, right, early, lead=0):
        def tile(n, low, high):
            cols = pl.ds(pl.multiple_of(n * LANES, LANES), LANES)
            block = left[:, :, :, cols].reshape(8 * S, LANES)
            gall[w, cols, low:high] = contract_first(
                block, right[:, :, low:high].reshape(8 * S, high - low)
            ).astype(BF16)
            return 0

        first = D // LANES // 2
        if lead:
            lax.fori_loop(0, first + 1, lambda n, _: tile(n + first * (1 - f), 0, lead), 0)
            weight_send(early[0])
            early = early[1:]
        lax.fori_loop(0, first + 1, lambda n, _: tile(n + first * (1 - f), lead, U), 0)
        for q in early:
            weight_send(q)
        lax.fori_loop(0, first, lambda n, _: tile(n + (first + 1) * f, 0, U), 0)

    def weight_send(q):
        full, from_x, _ = chunks[q]
        send(kw + q, full.at[theirs_x], from_x, across)

    def weight_push(q):
        full, from_x, from_z = chunks[q]
        arrive(kw + q, from_x)

        def add(n, _):
            rows = pl.ds(pl.multiple_of(f * C * R + n * R, R), R)
            part = pl.ds(pl.multiple_of(n * R, R), R)
            full[rows] = (full[rows].astype(F32) + from_x[part].astype(F32)).astype(BF16)
            return 0

        lax.fori_loop(0, C, add, 0)
        for to in (far, near, base + 1 - m):
            step = (to - c + C) % C
            send(
                kz + q * (C - 1) + step - 1,
                full.at[rows_of(f, to)],
                from_z.at[step - 1],
                {"context": to},
            )

    def weight_meet(*which):
        for q in which:
            for step in range(1, C):
                arrive(kz + q * (C - 1) + step - 1, chunks[q][2].at[step - 1])

    def weight_end(w):
        same = gall[w, rows_of(f, c)].astype(F32)
        other = jnp.zeros((R, U), F32)
        for step in range(1, C):
            if step % 2:
                other = other + gall_z[step - 1, w].astype(F32)
            else:
                same = same + gall_z[step - 1, w].astype(F32)
        ff_stage[:, 0:U] = jnp.where(m == 0, same, other)
        ff_stage[:, U:units] = jnp.where(m == 0, other, same)[:, 0 : units - U]
        into = out_down if w == 2 else out_gateup.at[:, w]
        saved = pltpu.make_async_copy(ff_stage, into, ls.at[5])
        saved.start()
        saved.wait()

    weight_grad(2, dd, active, (0, 1, 2), 256)
    weight_grad(0, xg, upg, (3, 4))
    weight_push(0)
    d_normed = finish8(ko2)
    hidden = hid[...]
    d_hidden, gain_2 = rms_backward(d_normed, hidden, rms_factor(hidden), gain(2))
    d_hidden = cot[...].astype(F32) + d_hidden
    dhid[...] = d_hidden
    gain_mine[2:3] = gain_2
    branch = bran[...]
    d_branch, gain_1 = rms_backward(d_hidden, branch, rms_factor(branch), gain(1))
    gain_mine[1:2] = gain_1
    db[y, core] = d_branch.astype(BF16)
    kb = share4(db)
    weight_push(1)
    weight_grad(1, xg, gel, ())
    weight_push(2)
    meet4(kb, db)

    def out_grad(n, _):
        cols = pl.ds(pl.multiple_of(n * LANES, LANES), LANES)
        ga[cols, 0:HD] = contract_first(
            db[:, :, :, cols].reshape(T, LANES), mix[...]
        ).astype(BF16)
        return 0

    lax.fori_loop(0, D // LANES, out_grad, 0)
    weight_send(5)
    weight_send(6)

    def scores_back(i, gain_q):
        rows = pl.ds(pl.multiple_of(i * half, half), half)
        d_mixed = mm(db[i].reshape(half, D), wa[:, o_cols]).astype(BF16)
        dmix[rows] = d_mixed
        p = probs[rows]
        d_probs = contract_last(d_mixed, kv[:, HD:])
        inner = jnp.sum(p * d_probs, axis=1, keepdims=True)
        low = (p * (d_probs - inner)).astype(BF16)
        dscore[rows] = low
        d_q = mm(low, kv[:, 0:HD]) * scale
        raw = qraw[rows]
        factor = rms_factor(raw)
        d_raw, part = rms_backward(
            turn_back(d_q, cosine[rows], sine[rows]), raw, factor, head_gain(0)
        )
        dq[rows] = d_raw.astype(BF16)
        return gain_q + part

    gain_q = lax.fori_loop(0, 2, scores_back, jnp.zeros((1, HD), F32))
    kp = slots(3)

    def keys_back(n, _):
        cols = pl.ds(pl.multiple_of(n * half, half), half)
        d_k = contract_first(dscore[:, cols], qs[...]) * scale
        d_v = contract_first(probs[:, cols].astype(BF16), dmix[...])
        both = jnp.concatenate([d_k, d_v], axis=1).astype(BF16)
        kvp[n % 2, 0, n // 2] = both[0:S]
        kvp[n % 2, 1, n // 2] = both[S:]
        return 0

    lax.fori_loop(0, 4, keys_back, 0)
    for i in range(2):
        send(kp + i, kvp.at[i, 1 - core], kvp_core.at[i], partner)

    arrive(kp + (1 - y), kvp_core.at[1 - y])
    kvp_sum[...] = (kvp[1 - y, core].astype(F32) + kvp_core[1 - y].astype(F32)).astype(BF16)
    send(kp + 2, kvp_sum, kvp_chip, chip_of(1 - y, 2))
    kr = share4(block_all)
    weight_push(3)
    arrive(kp + y, kvp_core.at[y])
    arrive(kp + 2, kvp_chip)
    d_left = (
        kvp[y, core, 0].astype(F32) + kvp_core[y, 0].astype(F32) + kvp_chip[0].astype(F32)
    )
    kt = slots(1)
    ret_out[...] = d_left.astype(BF16)

    @pl.when(c > 0)
    def _():
        copy(kt, ret_out, ret_in, {"context": c - 1}).start()

    weight_push(4)
    weight_push(5)

    @pl.when(c < C - 1)
    def _():
        arrive(kt, ret_in)

    @pl.when(c == C - 1)
    def _():
        ret_in[...] = jnp.zeros((S, 2 * HD), BF16)

    d_kv = (
        kvp[y, core, 1].astype(F32)
        + kvp_core[y, 1].astype(F32)
        + kvp_chip[1].astype(F32)
        + ret_in[...].astype(F32)
    )
    raw = jnp.concatenate([kv_raw[0, shard], kv_raw[1, shard]], axis=1).astype(F32)
    d_raw, gain_k = rms_backward(
        turn_back(d_kv[:, :HD], cosine[shard], sine[shard]), raw, rms_factor(raw), head_gain(1)
    )
    d_kv = jnp.concatenate([d_raw, d_kv[:, HD:]], axis=1).astype(BF16)
    for i in range(4):
        dkv_mine[i] = d_kv[:, i * LANES : (i + 1) * LANES]
    kq = slots(4)
    for i in range(1, 4):
        k = (t + i) % 4
        send(kq + i, dkv_mine.at[k], dkv_cols.at[t], {"tensor": k})
    dkv_cols[t] = dkv_mine[t]
    for i in range(1, 4):
        arrive(kq + i, dkv_cols.at[(t - i + 4) % 4])

    k4 = slots(2)

    def query_back(i, _):
        rows = pl.ds(pl.multiple_of(i * half, half), half)
        pair = pl.ds(i * 2, 2)
        part = contract_last(dq[rows], wa[:, q_cols])
        part = part + contract_last(dkv_cols[pair].reshape(half, LANES), wa[:, kv_part])
        part = part.astype(BF16)
        p4[i, 0] = part[0:S]
        p4[i, 1] = part[S:]
        copy(k4 + i, p4.at[i, 1 - core], p4_core.at[i], partner).start()
        return 0

    lax.fori_loop(0, 2, query_back, 0)

    def attn_grad(n, _):
        cols = pl.ds(pl.multiple_of(n * LANES, LANES), LANES)
        left = nrm[:, cols]
        ga[cols, HD : 2 * HD] = contract_first(left, dq[...]).astype(BF16)
        ga[cols, 2 * HD :] = contract_first(left, dkv_cols[...].reshape(T, LANES)).astype(BF16)
        return 0

    lax.fori_loop(0, D // LANES, attn_grad, 0)
    weight_send(7)
    weight_send(8)
    weight_push(6)
    kc = sum4(k4)
    meet4(kr, block_all)
    save_block = pltpu.make_async_copy(block_all, out_block, ls.at[3])
    save_block.start()
    d_normed = finish4(kc)
    copy(kc, p4_sum, p4_chip, chip_of(1 - y, 2)).wait_send()
    for i in range(2):
        copy(k4 + i, p4.at[i, 1 - core], p4_core.at[i], partner).wait_send()
    values = act[shard].astype(F32)
    d_input, gain_0 = rms_backward(d_normed, values, rms_factor(values), gain(0))
    input_all[y, core] = (dhid[...] + d_input).astype(BF16)
    gain_mine[0:1] = gain_0
    gain_mine[4:8] = jnp.zeros((4, D), F32)
    gain_mine[4:5, 0:HD] = gain_q
    gain_mine[5:6, 0:HD] = gain_k
    kn = slots(4 + 1 + C)
    for i in range(1, 4):
        send(kn + i, gain_mine, gain_tensor.at[i], {"tensor": (t + i) % 4})
    ki = share4(input_all)
    weight_push(7)
    total = gain_mine[...]
    for i in range(1, 4):
        arrive(kn + i, gain_tensor.at[i])
        total = total + gain_tensor[i]
    gain_tensor[0] = total
    send(kn, gain_tensor.at[0], gain_x.at[0], across)
    weight_push(8)
    arrive(kn, gain_x.at[0])
    gain_x[1] = total + gain_x[0]
    for step in range(1, C):
        send(kn + 4 + step, gain_x.at[1], gain_z.at[step], along(step))
    weight_meet(0, 1, 2)
    weight_end(2)
    meet4(ki, input_all)
    save_input = pltpu.make_async_copy(input_all, out_input, ls.at[4])
    save_input.start()
    weight_meet(3, 4)
    weight_end(0)
    weight_meet(5, 7)
    attn = ga[rows_of(f, c)].astype(F32)
    for step in range(1, C):
        attn = attn + ga_z[step - 1].astype(F32)
    kvg[t] = attn[:, 2 * HD :]
    kh = slots(4)
    for i in range(1, 4):
        send(kh + i, kvg.at[t], kvg.at[t], {"tensor": (t + i) % 4})
    st_out[...] = attn[:, 0:HD]
    st_query[...] = attn[:, HD : 2 * HD]
    staged = []

    def save(n, src, dst):
        staged.append(pltpu.make_async_copy(src, dst, ls.at[10 + n]))
        staged[-1].start()

    save(0, st_out, out_out)
    save(1, st_query, out_query)
    total = gain_x[1]
    for step in range(1, C):
        arrive(kn + 4 + step, gain_z.at[step])
        total = total + gain_z[step]
    owner = f * C + c
    moved = pltpu.roll(total, (D - owner * R) % D, 1)
    st_norm[...] = moved[0:4, 0:R]
    moved = pltpu.roll(total[:, 0:HD], (HD - owner * narrow) % HD, 1)
    st_head[...] = moved[4:6, 0:narrow]
    save(2, st_norm, out_norm)
    save(3, st_head, out_head)
    weight_meet(6, 8)
    weight_end(1)
    for i in range(1, 4):
        arrive(kh + i, kvg.at[(t - i + 4) % 4])
    for k in range(4):
        st_kv[:, k * LANES : (k + 1) * LANES] = kvg[k]
    save(4, st_kv, out_kv)
    save_block.wait()
    save_input.wait()
    for moved in staged:
        moved.wait()
    settle()

    @pl.when(c < C - 1)
    def _():
        copy(ks, seg_row, seg_left, {"context": c + 1}).wait_send()
        copy(kk, kv.at[own_half], kv.at[my_half], {"context": c + 1}).wait_send()

    @pl.when(c > 0)
    def _():
        copy(kt, ret_out, ret_in, {"context": c - 1}).wait_send()
    assert counter[0] == SEMAPHORES, counter


def fused(
    mesh,
    activations,
    positions,
    seg_ids,
    norm_gains,
    head_gains,
    w_query,
    w_keyval,
    w_out,
    w_gateup,
    w_down,
    cotangent,
):
    C = mesh.shape["context"]
    T, D = activations.shape[1:]
    R, units = w_down.shape
    U = -(-units // (2 * LANES)) * LANES
    S = T // 4
    pack = -(-R // LANES) * LANES
    operands = (
        activations[0],
        positions,
        seg_ids,
        norm_gains,
        head_gains,
        w_gateup,
        w_down,
        cotangent[0],
        w_query,
        w_keyval,
        w_out,
    )
    scratch = [
        pltpu.VMEM((T, HD // 2), F32),
        pltpu.VMEM((T, HD // 2), F32),
        pltpu.VMEM((8, T), jnp.int32),
        pltpu.VMEM((T, 1), jnp.int32),
        pltpu.VMEM((8, pack), F32),
        pltpu.VMEM((2 * C, 8, pack), F32),
        pltpu.VMEM((2, 3, R, U), BF16),
        pltpu.VMEM((S, D), BF16),
        pltpu.VMEM((D, 2 * HD + LANES), BF16),
        pltpu.VMEM((3, D, U), BF16),
        pltpu.VMEM((8, T), jnp.int32),
        pltpu.VMEM((8, D), F32),
        pltpu.VMEM((8, HD), F32),
        pltpu.VMEM((T, D), BF16),
        pltpu.VMEM((T, HD), F32),
        pltpu.VMEM((4, T, LANES), BF16),
        pltpu.VMEM((T, HD), BF16),
        pltpu.VMEM((2 * T, 2 * HD), BF16),
        pltpu.VMEM((T, 2 * T), F32),
        pltpu.VMEM((T, HD), BF16),
        pltpu.VMEM((2, 2, S, D), BF16),
        pltpu.VMEM((2, S, D), BF16),
        pltpu.VMEM((S, D), BF16),
        pltpu.VMEM((S, D), BF16),
        pltpu.VMEM((S, D), F32),
        pltpu.VMEM((S, D), F32),
        pltpu.VMEM((4, 2, S, D), BF16),
        pltpu.VMEM((4, 2 * S, U), BF16),
        pltpu.VMEM((4, 2 * S, U), BF16),
        pltpu.VMEM((4, 2 * S, U), BF16),
        pltpu.VMEM((4, 2, S, D), BF16),
        pltpu.VMEM((4, S, D), BF16),
        pltpu.VMEM((3, S, D), BF16),
        pltpu.VMEM((3, S, D), BF16),
        pltpu.VMEM((4, 2, S, D), BF16),
        pltpu.VMEM((S, D), F32),
        pltpu.VMEM((2, 2, S, D), BF16),
        pltpu.VMEM((T, 2 * T), BF16),
        pltpu.VMEM((T, HD), BF16),
        pltpu.VMEM((T, HD), BF16),
        pltpu.VMEM((2, 2, 2, S, 2 * HD), BF16),
        pltpu.VMEM((2, 2, S, 2 * HD), BF16),
        pltpu.VMEM((2, S, 2 * HD), BF16),
        pltpu.VMEM((2, S, 2 * HD), BF16),
        pltpu.VMEM((S, 2 * HD), BF16),
        pltpu.VMEM((S, 2 * HD), BF16),
        pltpu.VMEM((4, S, LANES), BF16),
        pltpu.VMEM((4, S, LANES), BF16),
        pltpu.VMEM((3, C * R, U), BF16),
        pltpu.VMEM((C - 1, 3, R, U), BF16),
        pltpu.VMEM((D, 2 * HD + LANES), BF16),
        pltpu.VMEM((C * R, 2 * HD + LANES), BF16),
        pltpu.VMEM((C - 1, R, 2 * HD + LANES), BF16),
        pltpu.VMEM((4, R, LANES), F32),
        pltpu.VMEM((R, units), F32),
        pltpu.VMEM((8, D), F32),
        pltpu.VMEM((4, 8, D), F32),
        pltpu.VMEM((2, 8, D), F32),
        pltpu.VMEM((C, 8, D), F32),
        pltpu.VMEM((2, 2, S, D), BF16),
        pltpu.VMEM((2, 2, S, D), BF16),
        pltpu.VMEM((R, HD), F32),
        pltpu.VMEM((R, HD), F32),
        pltpu.VMEM(norm_gains.shape, F32),
        pltpu.VMEM(head_gains.shape, F32),
        pltpu.VMEM((R, 2 * HD), F32),
        pltpu.SemaphoreType.DMA((SEMAPHORES,)),
        pltpu.SemaphoreType.DMA((SEMAPHORES,)),
        pltpu.SemaphoreType.DMA((15,)),
    ]
    vmem = pl.BlockSpec(memory_space=pltpu.VMEM)
    anywhere = pl.BlockSpec(memory_space=pl.ANY)
    results = (
        jax.ShapeDtypeStruct((2, 2, S, D), BF16),
        jax.ShapeDtypeStruct((2, 2, S, D), BF16),
        jax.ShapeDtypeStruct(norm_gains.shape, F32),
        jax.ShapeDtypeStruct(head_gains.shape, F32),
        jax.ShapeDtypeStruct(w_query.shape, F32),
        jax.ShapeDtypeStruct(w_keyval.shape, F32),
        jax.ShapeDtypeStruct(w_out.shape, F32),
        jax.ShapeDtypeStruct(w_gateup.shape, F32),
        jax.ShapeDtypeStruct(w_down.shape, F32),
    )
    sizes = {"context": C, "tokens": T, "width": D, "rows": R, "units": U}
    parts = pl.pallas_call(
        functools.partial(fused_kernel, sizes),
        out_shape=results,
        in_specs=[vmem] * 7 + [anywhere] * 4,
        out_specs=[anywhere] * len(results),
        scratch_shapes=scratch,
        compiler_params=pltpu.CompilerParams(
            collective_id=0, has_side_effects=True, vmem_limit_bytes=67043328
        ),
    )(*operands)
    count = len(parts)
    block_out, input_grad, *grads = pl.pallas_call(
        functools.partial(emit_kernel, count),
        out_shape=results,
        in_specs=[anywhere] * count,
        out_specs=[anywhere] * count,
        scratch_shapes=[pltpu.VMEM(part.shape, part.dtype) for part in parts]
        + [pltpu.SemaphoreType.DMA((count,))] * 2,
    )(*parts)
    return block_out.reshape(1, T, D), input_grad.reshape(1, T, D), *grads


def block(mesh, *arrays):
    tokens, rows = arrays[0].shape[1], arrays[9].shape[0]
    fits = (
        mesh.shape["fsdp"] == 2
        and mesh.shape["tensor"] == 4
        and mesh.shape["context"] == 4
        and tokens == WINDOW
        and rows % 16 == 0
        and arrays[5].shape[1] == HD
        and arrays[6].shape[1] == 4 * LANES
    )
    return fused(mesh, *arrays) if fits else shards(*arrays)


def shards(
    activations,
    positions,
    seg_ids,
    norm_gains,
    head_gains,
    w_query,
    w_keyval,
    w_out,
    w_gateup,
    w_down,
    cotangent,
):
    tokens = activations.shape[1]
    local_heads = w_query.shape[1] // HD
    inputs = activations[0].astype(jnp.float32)
    places = positions[0]
    documents = seg_ids[0]
    gains_all, heads_all, query_all, keyval_all, out_all = (
        lax.all_gather(norm_gains, ("fsdp", "context"), axis=1, tiled=True),
        lax.all_gather(head_gains, ("fsdp", "context"), axis=1, tiled=True),
        lax.all_gather(w_query, ("fsdp", "context"), axis=0, tiled=True),
        lax.all_gather(w_keyval, ("fsdp", "context"), axis=0, tiled=True),
        lax.all_gather(w_out, ("fsdp", "context"), axis=0, tiled=True),
    )
    gains_f = gains_all.astype(jnp.float32)
    heads_f = heads_all.astype(jnp.float32)
    normed_f, input_back = jax.vjp(rms_norm, inputs, gains_f[0])
    normed = normed_f.astype(jnp.bfloat16)
    query_raw = jnp.dot(normed, query_all, preferred_element_type=jnp.float32).reshape(
        tokens, local_heads, HD
    )
    keyval_raw = jnp.dot(normed, keyval_all, preferred_element_type=jnp.float32)

    def prepare(raw_heads, head_gain):
        return rotate(rms_norm(raw_heads, head_gain), places)

    query_rot, query_back = jax.vjp(prepare, query_raw, heads_f[0])
    key_rot, key_back = jax.vjp(prepare, keyval_raw[:, None, :HD], heads_f[1])
    queries = query_rot.astype(jnp.bfloat16)
    own_keyval = jnp.concatenate([key_rot[:, 0], keyval_raw[:, HD:]], axis=1).astype(jnp.bfloat16)
    labels = jnp.stack([places, documents])
    keep_from = tokens - tokens
    left_keyval, left_labels = from_behind((own_keyval, labels), "context", 1)
    keys_all = jnp.concatenate([left_keyval, own_keyval], axis=0)
    key_places = jnp.concatenate([left_labels[0], places])
    key_documents = jnp.concatenate([left_labels[1], documents])
    has_left = lax.axis_index("context") > 0
    key_live = jnp.concatenate([jnp.full((tokens,), has_left), jnp.ones((tokens,), dtype=bool)])
    scale_factor = HD ** (-0.5)
    block_rows = 512
    block_starts = jnp.arange(tokens // block_rows) * block_rows

    def block_scores():
        spacing = places[:, None] - key_places[None, :]
        visible = (
            key_live[None, :]
            & (documents[:, None] == key_documents[None, :])
            & (spacing >= 0)
            & (spacing < WINDOW)
        )
        raw_scores = (
            jnp.einsum("qhd,kd->hqk", queries, keys_all[:, :HD], preferred_element_type=jnp.float32)
            * scale_factor
        )
        return (jnp.where(visible[None], raw_scores, -1e30), keys_all, queries)

    def forward_block(start):
        scores, near_keyval, query_block = block_scores()
        row_top = jnp.max(scores, axis=-1, keepdims=True)
        raised = jnp.exp(scores - row_top)
        row_total = jnp.sum(raised, axis=-1, keepdims=True)
        probs = raised / row_total
        mixed_block = jnp.einsum(
            "hqk,kd->qhd",
            probs.astype(jnp.bfloat16),
            near_keyval[:, HD:],
            preferred_element_type=jnp.float32,
        )
        return (mixed_block.astype(jnp.bfloat16), row_top + jnp.log(row_total))

    mixed_blocks, log_blocks = lax.map(forward_block, block_starts)
    mixed_low = mixed_blocks.reshape(tokens, local_heads * HD)
    branch = lax.psum(contract_last(mixed_low, out_all).astype(jnp.bfloat16), "tensor").astype(jnp.float32)
    post_attn, post_attn_back = jax.vjp(rms_norm, branch, gains_f[1])
    hidden = inputs + post_attn
    normed_mlp_f, pre_mlp_back = jax.vjp(rms_norm, hidden, gains_f[2])
    normed_mlp = normed_mlp_f.astype(jnp.bfloat16)
    columns = normed_mlp
    gate_up = jnp.einsum(
        "bn,nkf->bkf",
        columns,
        lax.all_gather(w_gateup, ("fsdp", "context"), axis=0, tiled=True),
        preferred_element_type=jnp.float32,
    )
    active_f, glu_back = jax.vjp(glu, gate_up)
    active = active_f.astype(jnp.bfloat16)
    down = lax.psum(
        contract_last(
            active, lax.all_gather(w_down, ("fsdp", "context"), axis=0, tiled=True)
        ).astype(jnp.bfloat16),
        "tensor",
    ).astype(jnp.float32)
    post_mlp, post_mlp_back = jax.vjp(rms_norm, down, gains_f[3])
    result = hidden + post_mlp
    grad_out = cotangent[0].astype(jnp.float32)
    d_down, gain_post_mlp = post_mlp_back(grad_out)
    down_low = d_down.astype(jnp.bfloat16)
    columns = down_low
    d_active = jnp.dot(
        columns,
        lax.all_gather(w_down, ("fsdp", "context"), axis=0, tiled=True),
        preferred_element_type=jnp.float32,
    )
    d_gate_up = glu_back(d_active)[0].astype(jnp.bfloat16)
    d_normed_part = jnp.einsum(
        "bkf,nkf->bn",
        d_gate_up,
        lax.all_gather(w_gateup, ("fsdp", "context"), axis=0, tiled=True),
        preferred_element_type=jnp.float32,
    )
    d_normed_mlp = lax.psum(d_normed_part.astype(jnp.bfloat16), "tensor").astype(jnp.float32)
    d_hidden_norm, gain_pre_mlp = pre_mlp_back(d_normed_mlp)
    d_hidden = grad_out + d_hidden_norm
    features = normed_mlp
    grad_cols = down_low
    gate_up_term = jnp.einsum(
        "bn,bkf->nkf", features, d_gate_up, preferred_element_type=jnp.float32
    )
    down_term = contract_first(grad_cols, active)
    scatter = lambda part: lax.psum_scatter(
        part.astype(jnp.bfloat16), ("fsdp", "context"), scatter_dimension=0, tiled=True
    ).astype(jnp.float32)
    gate_grad = scatter(gate_up_term[:, 0])
    up_grad = scatter(gate_up_term[:, 1])
    down_grad = scatter(down_term)
    d_branch, gain_post_attn = post_attn_back(d_hidden)
    branch_low = d_branch.astype(jnp.bfloat16)
    d_mixed = jnp.dot(branch_low, out_all, preferred_element_type=jnp.float32)
    d_mixed_low = d_mixed.astype(jnp.bfloat16).reshape(tokens, local_heads, HD)

    def backward_block(carry, item):
        start, log_block = item
        scores, near_keyval, query_block = block_scores()
        probs_again = jnp.exp(scores - log_block)
        d_probs = jnp.einsum(
            "qhd,kd->hqk", d_mixed_low, near_keyval[:, HD:], preferred_element_type=jnp.float32
        )
        row_inner = jnp.sum(probs_again * d_probs, axis=-1, keepdims=True)
        d_scores = (probs_again * (d_probs - row_inner)).astype(jnp.bfloat16)
        d_query_block = (
            jnp.einsum(
                "hqk,kd->qhd", d_scores, near_keyval[:, :HD], preferred_element_type=jnp.float32
            )
            * scale_factor
        )
        d_keys = (
            jnp.einsum("hqk,qhd->kd", d_scores, query_block, preferred_element_type=jnp.float32)
            * scale_factor
        )
        d_values = jnp.einsum(
            "hqk,qhd->kd",
            probs_again.astype(jnp.bfloat16),
            d_mixed_low,
            preferred_element_type=jnp.float32,
        )
        updated = carry + jnp.concatenate([d_keys, d_values], axis=1)
        return (updated, d_query_block)

    d_keyval, d_query_blocks = lax.scan(
        backward_block,
        jnp.zeros((tokens + tokens, 2 * HD), jnp.float32),
        (block_starts, log_blocks),
    )
    d_queries = d_query_blocks.reshape(tokens, local_heads, HD)
    returned = from_behind(d_keyval[:tokens].astype(jnp.bfloat16), "context", -1).astype(
        jnp.float32
    )
    own_grad = d_keyval[tokens:].at[keep_from:].add(returned)
    d_query_raw, gain_query = query_back(d_queries)
    d_query_low = d_query_raw.reshape(tokens, local_heads * HD).astype(jnp.bfloat16)
    d_normed_query, keyval_grad, gain_query_all = (
        lax.psum(contract_last(d_query_low, query_all).astype(jnp.bfloat16), "tensor").astype(
            jnp.float32
        ),
        lax.psum(own_grad.astype(jnp.bfloat16), "tensor").astype(jnp.float32),
        lax.psum(gain_query.astype(jnp.bfloat16), "tensor").astype(jnp.float32),
    )
    d_key_raw, gain_key = key_back(keyval_grad[:, None, :HD])
    d_keyval_low = jnp.concatenate([d_key_raw[:, 0], keyval_grad[:, HD:]], axis=1).astype(
        jnp.bfloat16
    )
    d_normed = d_normed_query + contract_last(d_keyval_low, keyval_all)
    d_input_norm, gain_input = input_back(d_normed)
    input_total = d_hidden + d_input_norm
    features = normed
    grad_cols = branch_low
    attn_grads = lax.psum_scatter(
        jnp.stack(
            [contract_first(features, d_query_low), contract_first(grad_cols, mixed_low)], axis=1
        ).astype(jnp.bfloat16),
        ("fsdp", "context"),
        scatter_dimension=0,
        tiled=True,
    ).astype(jnp.float32)
    keyval_term = contract_first(normed, d_keyval_low)
    gain_terms = jnp.stack([gain_input, gain_post_attn, gain_pre_mlp, gain_post_mlp])
    head_terms = jnp.stack([gain_query_all, gain_key])
    gain_grad, head_grad, keyval_weight_grad = (
        lax.psum_scatter(
            gain_terms.astype(jnp.bfloat16), ("fsdp", "context"), scatter_dimension=1, tiled=True
        ).astype(jnp.float32),
        lax.psum_scatter(
            head_terms.astype(jnp.bfloat16), ("fsdp", "context"), scatter_dimension=1, tiled=True
        ).astype(jnp.float32),
        lax.psum_scatter(
            keyval_term.astype(jnp.bfloat16), ("fsdp", "context"), scatter_dimension=0, tiled=True
        ).astype(jnp.float32),
    )
    return (
        result[None].astype(jnp.bfloat16),
        input_total[None].astype(jnp.bfloat16),
        gain_grad,
        head_grad,
        attn_grads[:, 0],
        keyval_weight_grad,
        attn_grads[:, 1],
        jnp.stack([gate_grad, up_grad], axis=1),
        down_grad,
    )


def solution(mesh):
    return jax.shard_map(
        functools.partial(block, mesh),
        mesh=mesh,
        in_specs=(
            P("fsdp", "context", None),
            P("fsdp", "context"),
            P("fsdp", "context"),
            P(None, ("fsdp", "context")),
            P(None, ("fsdp", "context")),
            P(("fsdp", "context"), "tensor"),
            P(("fsdp", "context"), None),
            P(("fsdp", "context"), "tensor"),
            P(("fsdp", "context"), None, "tensor"),
            P(("fsdp", "context"), "tensor"),
            P("fsdp", "context", None),
        ),
        out_specs=(
            P("fsdp", "context", None),
            P("fsdp", "context", None),
            P(None, ("fsdp", "context")),
            P(None, ("fsdp", "context")),
            P(("fsdp", "context"), "tensor"),
            P(("fsdp", "context"), None),
            P(("fsdp", "context"), "tensor"),
            P(("fsdp", "context"), None, "tensor"),
            P(("fsdp", "context"), "tensor"),
        ),
        check_vma=False,
    )
```

```python
import functools
import math

import jax
import jax.numpy as jnp
from jax import lax
from jax.experimental import pallas as pl
from jax.experimental.pallas import tpu as pltpu
from jax.sharding import PartitionSpec as P

HD = 256
WINDOW = 512


EPSILON = 1e-06


def from_behind(block, axis, distance):
    devices = range(lax.axis_size(axis))
    route = [(i - distance, i) for i in devices if i - distance in devices]
    return lax.ppermute(block, axis, route)


def rms_norm(values, gain):
    factor = lax.rsqrt(jnp.mean(values * values, axis=-1, keepdims=True) + EPSILON)
    return values * factor * gain


def rotate(tensor, places):
    width_all = tensor.shape[-1]
    half_width = width_all // 2
    freqs = jnp.power(10000.0, -jnp.arange(half_width, dtype=jnp.float32) * 2.0 / width_all)
    angles = places.astype(jnp.float32)[:, None] * freqs[None, :]
    cosine = jnp.cos(angles)[:, None, :]
    sine = jnp.sin(angles)[:, None, :]
    first_half = tensor[..., :half_width]
    second_half = tensor[..., half_width:]
    return jnp.concatenate(
        [first_half * cosine - second_half * sine, second_half * cosine + first_half * sine],
        axis=-1,
    )


def glu(gate_up):
    return jax.nn.gelu(gate_up[:, 0], approximate=True) * gate_up[:, 1]


def contract_last(left_side, right_side):
    return lax.dot_general(
        left_side, right_side, (((1,), (1,)), ((), ())), preferred_element_type=jnp.float32
    )


def contract_first(left_side, right_side):
    return lax.dot_general(
        left_side, right_side, (((0,), (0,)), ((), ())), preferred_element_type=jnp.float32
    )


MESH = pl.DeviceIdType.MESH
F32 = jnp.float32
BF16 = jnp.bfloat16
LANES = 128
SEMAPHORES = 178


def mm(left, right):
    return jnp.dot(left, right, preferred_element_type=F32)


def rms_factor(values):
    return lax.rsqrt(jnp.mean(values * values, axis=-1, keepdims=True) + EPSILON)


def rms_backward(grad, values, factor, gain):
    unit = values * factor
    scaled = grad * gain
    inner = jnp.mean(scaled * unit, axis=-1, keepdims=True)
    return factor * (scaled - unit * inner), jnp.sum(grad * unit, axis=0, keepdims=True)


def turn(values, cosine, sine):
    half = values.shape[-1] // 2
    first, second = values[:, :half], values[:, half:]
    return jnp.concatenate([first * cosine - second * sine, second * cosine + first * sine], axis=1)


def turn_back(values, cosine, sine):
    half = values.shape[-1] // 2
    first, second = values[:, :half], values[:, half:]
    return jnp.concatenate([first * cosine + second * sine, second * cosine - first * sine], axis=1)


def emit_kernel(count, *refs):
    sources, results, held = refs[:count], refs[count : 2 * count], refs[2 * count : 3 * count]
    incoming, outgoing = refs[3 * count :]
    reads = [pltpu.make_async_copy(sources[n], held[n], incoming.at[n]) for n in range(count)]
    writes = [pltpu.make_async_copy(held[n], results[n], outgoing.at[n]) for n in range(count)]
    for moved in reads:
        moved.start()
    for n in range(count):
        reads[n].wait()
        writes[n].start()
    for moved in writes:
        moved.wait()


def fused_kernel(
    sizes,
    act,
    positions,
    seg_ids,
    norm_gains,
    head_gains,
    w_gateup,
    w_down,
    cot_all,
    w_query,
    w_keyval,
    w_out,
    out_block,
    out_input,
    out_norm,
    out_head,
    out_query,
    out_kv,
    out_out,
    out_gateup,
    out_down,
    cosine,
    sine,
    seg_row,
    seg_col,
    gain_pack,
    gain_all,
    w_ff,
    cot,
    wa,
    wf,
    seg_left,
    gain_rows,
    head_rows,
    nrm,
    qraw,
    kv_raw,
    qs,
    kv,
    probs,
    mix,
    p4,
    p4_core,
    p4_sum,
    p4_chip,
    hid,
    bran,
    xg,
    gel,
    upg,
    active,
    p8,
    p8_core,
    p8_sum,
    p8_chip,
    dd,
    dhid,
    db,
    dscore,
    dmix,
    dq,
    kvp,
    kvp_core,
    kvp_sum,
    kvp_chip,
    ret_out,
    ret_in,
    dkv_mine,
    dkv_cols,
    gall_x,
    gall_z,
    ga,
    ga_x,
    ga_z,
    kvg,
    ff_stage,
    gain_mine,
    gain_tensor,
    gain_x,
    gain_z,
    block_all,
    input_all,
    st_out,
    st_query,
    st_norm,
    st_head,
    st_kv,
    ss,
    rs,
    ls,
):
    C = sizes["context"]
    T, D, R, U = sizes["tokens"], sizes["width"], sizes["rows"], sizes["units"]
    units = w_down.shape[1]
    narrow = HD // (2 * C)
    S = T // 4
    f = lax.axis_index("fsdp")
    c = lax.axis_index("context")
    t = lax.axis_index("tensor")
    y, core = t // 2, t % 2
    m = c % 2
    base = c - m
    partner = {"tensor": y * 2 + (1 - core)}
    across = {"fsdp": 1 - f}
    counter = [0]
    sent = []

    def slots(count):
        first = counter[0]
        counter[0] += count
        assert counter[0] <= SEMAPHORES
        return first

    def copy(k, src, dst, device):
        return pltpu.make_async_remote_copy(
            src_ref=src,
            dst_ref=dst,
            send_sem=ss.at[k],
            recv_sem=rs.at[k],
            device_id=device,
            device_id_type=MESH,
        )

    def send(k, src, dst, device):
        moved = copy(k, src, dst, device)
        moved.start()
        sent.append(moved)

    def arrive(k, dst):
        copy(k, dst, dst, partner).wait_recv()

    def settle():
        for moved in sent:
            moved.wait_send()
        sent.clear()

    def along(step):
        return {"context": (c + step) % C}

    def rows_of(ff, cc):
        return pl.ds(pl.multiple_of((ff * C + cc) * R, R), R)

    def chip_of(k, count):
        if count == 2:
            return {"tensor": k * 2 + core}
        return {"context": base + k // 2, "tensor": (k % 2) * 2 + core}

    barrier = pltpu.get_barrier_semaphore()
    greeted = [along(step) for step in range(1, C)] + [across]
    greeted += [{"tensor": (t + step) % 4} for step in range(1, 4)]
    greeted += [{"context": base + 1 - m, "tensor": (1 - y) * 2 + core}]
    for device in greeted:
        pl.semaphore_signal(barrier, inc=1, device_id=device, device_id_type=MESH)
    gain_pack[...] = jnp.zeros(gain_pack.shape, F32)
    gain_pack[0:4, 0:R] = norm_gains[...].astype(F32)
    gain_pack[4:6, 0:narrow] = head_gains[...].astype(F32)
    seg_row[...] = jnp.broadcast_to(seg_ids[...], seg_row.shape)
    pl.semaphore_wait(barrier, len(greeted))

    mine = rows_of(f, c)
    kv_cols = pl.ds(pl.multiple_of(t * LANES, LANES), LANES)
    attn_parts = (
        (w_query, slice(0, HD)),
        (w_keyval.at[:, kv_cols], slice(HD, HD + LANES)),
        (w_out, slice(HD + LANES, 2 * HD + LANES)),
    )
    q_cols, kv_part, o_cols = (cols for _, cols in attn_parts[:3])
    local = []
    for n, (part, cols) in enumerate(attn_parts):
        local.append(pltpu.make_async_copy(part, wa.at[mine, cols], ls.at[6 + n]))
        local[-1].start()
    ka = slots(3 * C)
    kar = slots(C - 1)
    kg = slots(2 * C - 1)
    for step in range(1, C):
        for n, (part, cols) in enumerate(attn_parts):
            send(ka + 3 * step + n, part, wa.at[mine, cols], along(step))
    for n, (part, cols) in enumerate(attn_parts):
        send(ka + n, part, wa.at[mine, cols], across)
    own_gain = gain_all.at[f * C + c]
    gain_all[f * C + c] = gain_pack[...]
    for step in range(1, C):
        send(kg + step, gain_pack, own_gain, along(step))
    send(kg, gain_pack, own_gain, across)
    ks = slots(1)

    @pl.when(c < C - 1)
    def _():
        copy(ks, seg_row, seg_left, {"context": c + 1}).start()

    pieces = ((0, 0, 384), (0, 384, U), (1, 0, 512), (1, 512, U), (2, 0, 512), (2, 512, U))
    kf = slots((2 * C - 1) * len(pieces))

    def piece(p, rows):
        w, low, high = pieces[p]
        return wf.at[w, rows, low:high]

    side = c // 2
    near, far = 2 - side, 3 * (1 - side)

    def send_ff(p):
        k = kf + (2 * C - 1) * p
        w, low, high = pieces[p]
        turns = tuple((c + step) % C for step in range(1, C))
        for to in (base + 1 - m, near, far) if p in (3, 4) else turns:
            send(
                k + (to - c + C) % C,
                w_ff.at[to % 2, w, :, low:high],
                piece(p, mine),
                {"context": to},
            )
        send(k, w_ff.at[m, w, :, low:high], piece(p, mine), across)

    def relay_ff(p):
        k = kf + (2 * C - 1) * p
        for source in (base + 1 - m, near, far):
            step = (c - source + C) % C
            part = piece(p, rows_of(f, source))
            arrive(k + step, part)
            send(k + C - 1 + step, part, part, across)

    def meet_ff(p):
        k = kf + (2 * C - 1) * p
        arrive(k, piece(p, rows_of(1 - f, c)))
        for step in range(1, C):
            arrive(k + C - 1 + step, piece(p, rows_of(1 - f, (c - step + C) % C)))

    for w in range(3):
        whole = w_down[...] if w == 2 else w_gateup[:, w, :]
        w_ff[0, w] = whole[:, 0:U]
        w_ff[1, w, :, 0 : units - U] = whole[:, U:units]
        w_ff[1, w, :, units - U :] = jnp.zeros((R, 2 * U - units), BF16)
    seg_col[...] = jnp.transpose(seg_row[...].astype(F32))[:, 0:1].astype(jnp.int32)
    place = jnp.broadcast_to(positions[...].astype(F32), (8, T))
    index = lax.broadcasted_iota(jnp.int32, (1, HD // 2), 1).astype(F32)
    angle = jnp.transpose(place)[:, 0:1] * jnp.exp(index * (-2.0 * math.log(10000.0) / HD))
    cosine[...] = jnp.cos(angle)
    sine[...] = jnp.sin(angle)
    shard = pl.ds(pl.multiple_of(t * S, S), S)
    own_cot = pltpu.make_async_copy(cot_all.at[shard], cot, ls.at[2])
    own_cot.start()
    own_ff = pltpu.make_async_copy(w_ff.at[m], wf.at[:, mine], ls.at[1])
    own_ff.start()
    for step in range(1, C):
        other = rows_of(f, (c - step + C) % C)
        for n, (_, cols) in enumerate(attn_parts):
            arrive(ka + 3 * step + n, wa.at[other, cols])
        send(kar + step - 1, wa.at[other], wa.at[other], across)
        part = gain_all.at[f * C + (c - step + C) % C]
        arrive(kg + step, part)
        send(kg + C - 1 + step, part, part, across)
    for moved in local:
        moved.wait()
    send_ff(0)
    for n, (_, cols) in enumerate(attn_parts):
        arrive(ka + n, wa.at[rows_of(1 - f, c), cols])
    for step in range(1, C):
        arrive(kar + step - 1, wa.at[rows_of(1 - f, (c - step + C) % C)])

    @pl.when(c > 0)
    def _():
        arrive(ks, seg_left)

    @pl.when(c == 0)
    def _():
        seg_left[...] = jnp.full(seg_left.shape, -1, jnp.int32)
        kv[0:T] = jnp.zeros((T, 2 * HD), BF16)

    arrive(kg, gain_all.at[(1 - f) * C + c])
    for step in range(1, C):
        arrive(kg + C - 1 + step, gain_all.at[(1 - f) * C + (c - step + C) % C])
    wide = jnp.zeros((8, D), F32)
    heads = jnp.zeros((8, HD), F32)
    blank = jnp.zeros((8, D - gain_pack.shape[1]), F32)
    for j in range(2 * C):
        part = gain_all[j]
        wide = wide + pltpu.roll(jnp.concatenate([part, blank], axis=1), j * R, 1)
        heads = heads + pltpu.roll(part[:, 0:HD], j * narrow, 1)
    gain_rows[...] = wide
    head_rows[...] = heads

    def gain(index):
        return gain_rows[index : index + 1]

    def head_gain(index):
        return head_rows[4 + index : 5 + index]

    half = T // 2

    def project(i, _):
        rows = pl.ds(pl.multiple_of(i * half, half), half)
        values = act[rows].astype(F32)
        low = (values * rms_factor(values) * gain(0)).astype(BF16)
        nrm[rows] = low
        kv_raw[t, rows] = mm(low, wa[:, kv_part]).astype(BF16)
        return 0

    lax.fori_loop(0, 2, project, 0)
    ku = slots(4)
    for i in range(1, 4):
        send(ku + i, kv_raw.at[t], kv_raw.at[t], {"tensor": (t + i) % 4})

    def query(i, _):
        rows = pl.ds(pl.multiple_of(i * half, half), half)
        raw_q = mm(nrm[rows], wa[:, q_cols])
        qraw[rows] = raw_q
        qs[rows] = turn(
            raw_q * rms_factor(raw_q) * head_gain(0), cosine[rows], sine[rows]
        ).astype(BF16)
        return 0

    lax.fori_loop(0, 2, query, 0)
    for i in range(1, 4):
        arrive(ku + i, kv_raw.at[(t - i + 4) % 4])

    def key(i, _):
        rows = pl.ds(pl.multiple_of(i * half, half), half)
        raw_k = jnp.concatenate([kv_raw[0, rows], kv_raw[1, rows]], axis=1).astype(F32)
        own = pl.ds(pl.multiple_of(T + i * half, half), half)
        kv[own, 0:HD] = turn(
            raw_k * rms_factor(raw_k) * head_gain(1), cosine[rows], sine[rows]
        ).astype(BF16)
        kv[own, HD : HD + LANES] = kv_raw[2, rows]
        kv[own, HD + LANES :] = kv_raw[3, rows]
        return 0

    lax.fori_loop(0, 2, key, 0)
    kk = slots(2)
    my_half = pl.ds(pl.multiple_of(core * half, half), half)
    other_half = pl.ds(pl.multiple_of((1 - core) * half, half), half)
    own_half = pl.ds(pl.multiple_of(T + core * half, half), half)

    @pl.when(c < C - 1)
    def _():
        copy(kk, kv.at[own_half], kv.at[my_half], {"context": c + 1}).start()

    send_ff(1)
    send_ff(2)
    relay_ff(0)

    @pl.when(c > 0)
    def _():
        arrive(kk, kv.at[my_half])
        moved = copy(kk + 1, kv.at[my_half], kv.at[my_half], partner)
        moved.start()
        arrive(kk + 1, kv.at[other_half])
        moved.wait_send()

    scale = HD**-0.5
    no_left = jnp.where(c > 0, 0, 2 * T)
    k4 = slots(2)

    def attend(i, _):
        rows = pl.ds(pl.multiple_of(i * half, half), half)
        q = qs[rows]
        labels = seg_col[rows]
        row = lax.broadcasted_iota(jnp.int32, (half, T), 0) + i * half
        col = lax.broadcasted_iota(jnp.int32, (half, T), 1)
        left = contract_last(q, kv[0:T, 0:HD]) * scale
        left = jnp.where((labels == seg_left[0:1]) & (col > row + no_left), left, -1e30)
        own = contract_last(q, kv[T:, 0:HD]) * scale
        own = jnp.where((labels == seg_row[0:1]) & (col <= row), own, -1e30)
        top = jnp.maximum(
            jnp.max(left, axis=1, keepdims=True), jnp.max(own, axis=1, keepdims=True)
        )
        left, own = jnp.exp(left - top), jnp.exp(own - top)
        total = jnp.sum(left, axis=1, keepdims=True) + jnp.sum(own, axis=1, keepdims=True)
        left, own = left / total, own / total
        probs[rows, 0:T] = left
        probs[rows, T:] = own
        mixed = mm(left.astype(BF16), kv[0:T, HD:]) + mm(own.astype(BF16), kv[T:, HD:])
        mixed = mixed.astype(BF16)
        mix[rows] = mixed
        part = contract_last(mixed, wa[:, o_cols]).astype(BF16)
        p4[i, 0] = part[0:S]
        p4[i, 1] = part[S:]
        copy(k4 + i, p4.at[i, 1 - core], p4_core.at[i], partner).start()
        return 0

    lax.fori_loop(0, 2, attend, 0)

    def sum4(k):
        kc = slots(1)
        arrive(k + (1 - y), p4_core.at[1 - y])
        p4_sum[...] = (
            p4[1 - y, core].astype(F32) + p4_core[1 - y].astype(F32)
        ).astype(BF16)
        copy(kc, p4_sum, p4_chip, chip_of(1 - y, 2)).start()
        arrive(k + y, p4_core.at[y])
        return kc

    def finish4(kc):
        arrive(kc, p4_chip)
        return (
            p4[y, core].astype(F32)
            + p4_core[y].astype(F32)
            + p4_chip[...].astype(F32)
        )

    kc = sum4(k4)
    relay_ff(1)
    branch = finish4(kc)
    copy(kc, p4_sum, p4_chip, chip_of(1 - y, 2)).wait_send()
    for i in range(2):
        copy(k4 + i, p4.at[i, 1 - core], p4_core.at[i], partner).wait_send()

    bran[...] = branch
    hidden = act[shard].astype(F32) + branch * rms_factor(branch) * gain(1)
    hid[...] = hidden
    low = (hidden * rms_factor(hidden) * gain(2)).astype(BF16)

    me = m * 2 + y

    def gather8(full, value):
        kg = slots(8)
        full[me, core] = value
        send(kg + 4, full.at[me, core], full.at[me, core], partner)
        for i in range(1, 4):
            send(kg + i, full.at[me, core], full.at[me, core], chip_of((me + i) % 4, 4))
        return kg

    def pass8(kg, full, i):
        k = (me - i + 4) % 4
        arrive(kg + i, full.at[k, core])
        copy(kg + 4 + i, full.at[k, core], full.at[k, core], partner).start()

    def meet8(kg, full, i):
        k = (me - i + 4) % 4
        arrive(kg + 4 + i, full.at[k, 1 - core])

    def settle8(kg, full):
        for i in range(1, 4):
            k = (me - i + 4) % 4
            copy(kg + 4 + i, full.at[k, core], full.at[k, core], partner).wait_send()

    def give8(ko, i):
        k = (me - i + 4) % 4
        copy(ko + i, p8.at[k, 1 - core], p8_core.at[i], partner).start()

    def push8(ko, i):
        k = (me - i + 4) % 4
        arrive(ko + i, p8_core.at[i])
        p8_sum[i - 1] = (
            p8[k, core].astype(F32) + p8_core[i].astype(F32)
        ).astype(BF16)
        copy(ko + 4 + i, p8_sum.at[i - 1], p8_chip.at[i - 1], chip_of(k, 4)).start()

    def finish8(ko):
        arrive(ko, p8_core.at[0])
        total = p8[me, core].astype(F32) + p8_core[0].astype(F32)
        for i in range(1, 4):
            arrive(ko + 4 + i, p8_chip.at[i - 1])
            total = total + p8_chip[i - 1].astype(F32)
        for i in range(4):
            copy(ko + i, p8.at[0, 1 - core], p8_core.at[i], partner).wait_send()
        for i in range(1, 4):
            copy(ko + 4 + i, p8_sum.at[0], p8_chip.at[0], partner).wait_send()
        return total

    kx = slots(7)
    beside, beyond = m * 2 + 1 - y, (1 - m) * 2 + y
    corner = (1 - m) * 2 + 1 - y
    xg[me, core] = low
    send(kx + 2, xg.at[me, core], xg.at[me, core], chip_of(beyond, 4))
    send(kx + 1, xg.at[me, core], xg.at[me, core], chip_of(beside, 4))
    send(kx, xg.at[me, core], xg.at[me, core], partner)
    send_ff(3)
    send_ff(4)
    relay_ff(2)
    send_ff(5)
    relay_ff(3)
    for i, k in ((1, beside), (2, beyond), (3, corner)):
        part = xg.at[k, core]
        arrive(kx + i, part)
        if i == 2:
            send(kx + 3, part, part, chip_of(beside, 4))
        send(kx + 3 + i, part, part, partner)
    relay_ff(4)
    own_ff.wait()
    own_cot.wait()
    for p in range(4):
        meet_ff(p)
    arrive(kx, xg.at[me, 1 - core])
    for i, k in ((1, beside), (2, beyond), (3, corner)):
        arrive(kx + 3 + i, xg.at[k, 1 - core])
    root = 0.7978845608028654
    ko = slots(8)

    def forward(i, _):
        k = (me - i + 4) % 4
        x = xg[k].reshape(2 * S, D)
        gate = mm(x, wf[0])
        up = mm(x, wf[1])
        square = gate * gate
        bent = jnp.tanh(root * gate * (1.0 + 0.044715 * square))
        ramp = 0.5 * (1.0 + bent)
        gelu = gate * ramp
        slope = ramp + 0.5 * gate * (1.0 - bent * bent) * root * (1.0 + 3 * 0.044715 * square)
        gel[k] = gelu.astype(BF16)
        upg[k] = (up * slope).astype(BF16)
        active[k] = (gelu * up).astype(BF16)
        return 0

    lax.fori_loop(0, 3, forward, 0)
    relay_ff(5)
    lax.fori_loop(3, 4, forward, 0)
    meet_ff(4)
    meet_ff(5)

    def lower(i, _):
        k = (me - i + 4) % 4
        p8[k] = contract_last(active[k], wf[2]).astype(BF16).reshape(2, S, D)
        give8(ko, i)

        @pl.when(i > 1)
        def _():
            push8(ko, i - 1)

        return 0

    lax.fori_loop(0, 4, lower, 0)
    push8(ko, 3)
    down = finish8(ko)

    factor = rms_factor(down)
    grad = cot[...].astype(F32)
    result = (hid[...] + down * factor * gain(3)).astype(BF16)
    d_down, gain_3 = rms_backward(grad, down, factor, gain(3))
    gain_mine[3:4] = gain_3
    kd = gather8(dd, d_down.astype(BF16))

    def share4(full):
        kb = slots(3)
        send(kb, full.at[y, core], full.at[y, core], chip_of(1 - y, 2))
        send(kb + 1, full.at[y, core], full.at[y, core], partner)
        return kb

    def meet4(kb, full):
        arrive(kb, full.at[1 - y, core])
        send(kb + 2, full.at[1 - y, core], full.at[1 - y, core], partner)
        arrive(kb + 1, full.at[y, 1 - core])
        arrive(kb + 2, full.at[1 - y, 1 - core])

    block_all[y, core] = result
    ko2 = slots(8)

    def backward(i, _):
        k = (me - i + 4) % 4
        meet8(kd, dd, i)
        low = dd[k].reshape(2 * S, D)
        d_active = mm(low, wf[2])

        @pl.when(i < 3)
        def _():
            pass8(kd, dd, i + 1)

        d_gate = (d_active * upg[k].astype(F32)).astype(BF16)
        d_up = (d_active * gel[k].astype(F32)).astype(BF16)
        upg[k] = d_gate
        gel[k] = d_up
        p8[k] = (
            (contract_last(d_gate, wf[0]) + contract_last(d_up, wf[1]))
            .astype(BF16)
            .reshape(2, S, D)
        )
        give8(ko2, i)

        @pl.when(i > 1)
        def _():
            push8(ko2, i - 1)

        return 0

    lax.fori_loop(0, 4, backward, 0)
    push8(ko2, 3)
    settle8(kd, dd)

    settle()
    gall = wf
    mine_x = pl.ds(pl.multiple_of(f * C * R, C * R), C * R)
    theirs_x = pl.ds(pl.multiple_of((1 - f) * C * R, C * R), C * R)
    ff_chunk = lambda w, low, high: (
        gall.at[w, :, low:high],
        gall_x.at[w, :, low:high],
        gall_z.at[:, w, :, low:high],
    )
    attn_chunk = lambda low, high: (
        ga.at[:, low:high],
        ga_x.at[:, low:high],
        ga_z.at[:, :, low:high],
    )
    chunks = (
        ff_chunk(2, 0, 128),
        ff_chunk(2, 128, 384),
        ff_chunk(2, 384, U),
        ff_chunk(0, 0, 512),
        ff_chunk(0, 512, U),
        attn_chunk(0, HD),
        ff_chunk(1, 0, 256),
        ff_chunk(1, 256, 640),
        attn_chunk(HD, 2 * HD + LANES),
        ff_chunk(1, 640, U),
    )
    kw = slots(len(chunks))
    kz = slots(len(chunks) * (C - 1))

    def weight_grad(w, left, right, early, lead=0):
        def tile(n, low, high):
            cols = pl.ds(pl.multiple_of(n * LANES, LANES), LANES)
            block = left[:, :, :, cols].reshape(8 * S, LANES)
            gall[w, cols, low:high] = contract_first(
                block, right[:, :, low:high].reshape(8 * S, high - low)
            ).astype(BF16)
            return 0

        first = D // LANES // 2
        if lead:
            lax.fori_loop(0, first + 1, lambda n, _: tile(n + first * (1 - f), 0, lead), 0)
            weight_send(early[0])
            early = early[1:]
        lax.fori_loop(0, first + 1, lambda n, _: tile(n + first * (1 - f), lead, U), 0)
        for q in early:
            weight_send(q)
        lax.fori_loop(0, first, lambda n, _: tile(n + (first + 1) * f, 0, U), 0)

    def weight_send(q):
        full, from_x, _ = chunks[q]
        send(kw + q, full.at[theirs_x], from_x, across)

    def weight_push(q):
        full, from_x, from_z = chunks[q]
        arrive(kw + q, from_x)

        def add(n, _):
            rows = pl.ds(pl.multiple_of(f * C * R + n * R, R), R)
            part = pl.ds(pl.multiple_of(n * R, R), R)
            full[rows] = (full[rows].astype(F32) + from_x[part].astype(F32)).astype(BF16)
            return 0

        lax.fori_loop(0, C, add, 0)
        for to in (far, near, base + 1 - m):
            step = (to - c + C) % C
            send(
                kz + q * (C - 1) + step - 1,
                full.at[rows_of(f, to)],
                from_z.at[step - 1],
                {"context": to},
            )

    def weight_meet(*which):
        for q in which:
            for step in range(1, C):
                arrive(kz + q * (C - 1) + step - 1, chunks[q][2].at[step - 1])

    def weight_end(w):
        same = gall[w, rows_of(f, c)].astype(F32)
        other = jnp.zeros((R, U), F32)
        for step in range(1, C):
            if step % 2:
                other = other + gall_z[step - 1, w].astype(F32)
            else:
                same = same + gall_z[step - 1, w].astype(F32)
        ff_stage[:, 0:U] = jnp.where(m == 0, same, other)
        ff_stage[:, U:units] = jnp.where(m == 0, other, same)[:, 0 : units - U]
        into = out_down if w == 2 else out_gateup.at[:, w]
        saved = pltpu.make_async_copy(ff_stage, into, ls.at[5])
        saved.start()
        saved.wait()

    weight_grad(2, dd, active, (0, 1, 2), 128)
    weight_push(0)
    weight_grad(0, xg, upg, (3, 4))
    weight_push(1)
    d_normed = finish8(ko2)
    hidden = hid[...]
    d_hidden, gain_2 = rms_backward(d_normed, hidden, rms_factor(hidden), gain(2))
    d_hidden = cot[...].astype(F32) + d_hidden
    dhid[...] = d_hidden
    gain_mine[2:3] = gain_2
    branch = bran[...]
    d_branch, gain_1 = rms_backward(d_hidden, branch, rms_factor(branch), gain(1))
    gain_mine[1:2] = gain_1
    db[y, core] = d_branch.astype(BF16)
    kb = share4(db)
    weight_grad(1, xg, gel, ())
    weight_push(2)
    meet4(kb, db)

    def out_grad(n, _):
        cols = pl.ds(pl.multiple_of(n * LANES, LANES), LANES)
        ga[cols, 0:HD] = contract_first(
            db[:, :, :, cols].reshape(T, LANES), mix[...]
        ).astype(BF16)
        return 0

    lax.fori_loop(0, D // LANES, out_grad, 0)
    weight_send(5)
    weight_send(6)
    weight_send(7)

    def scores_back(i, gain_q):
        rows = pl.ds(pl.multiple_of(i * half, half), half)
        d_mixed = mm(db[i].reshape(half, D), wa[:, o_cols]).astype(BF16)
        dmix[rows] = d_mixed
        p = probs[rows]
        d_probs = contract_last(d_mixed, kv[:, HD:])
        inner = jnp.sum(p * d_probs, axis=1, keepdims=True)
        low = (p * (d_probs - inner)).astype(BF16)
        dscore[rows] = low
        d_q = mm(low, kv[:, 0:HD]) * scale
        raw = qraw[rows]
        factor = rms_factor(raw)
        d_raw, part = rms_backward(
            turn_back(d_q, cosine[rows], sine[rows]), raw, factor, head_gain(0)
        )
        dq[rows] = d_raw.astype(BF16)
        return gain_q + part

    gain_q = lax.fori_loop(0, 2, scores_back, jnp.zeros((1, HD), F32))
    kp = slots(3)

    def keys_back(n, _):
        cols = pl.ds(pl.multiple_of(n * half, half), half)
        d_k = contract_first(dscore[:, cols], qs[...]) * scale
        d_v = contract_first(probs[:, cols].astype(BF16), dmix[...])
        both = jnp.concatenate([d_k, d_v], axis=1).astype(BF16)
        kvp[n % 2, 0, n // 2] = both[0:S]
        kvp[n % 2, 1, n // 2] = both[S:]
        return 0

    lax.fori_loop(0, 4, keys_back, 0)
    for i in range(2):
        send(kp + i, kvp.at[i, 1 - core], kvp_core.at[i], partner)

    arrive(kp + (1 - y), kvp_core.at[1 - y])
    kvp_sum[...] = (kvp[1 - y, core].astype(F32) + kvp_core[1 - y].astype(F32)).astype(BF16)
    send(kp + 2, kvp_sum, kvp_chip, chip_of(1 - y, 2))
    kr = share4(block_all)
    weight_push(3)
    arrive(kp + y, kvp_core.at[y])
    arrive(kp + 2, kvp_chip)
    d_left = (
        kvp[y, core, 0].astype(F32) + kvp_core[y, 0].astype(F32) + kvp_chip[0].astype(F32)
    )
    kt = slots(1)
    ret_out[...] = d_left.astype(BF16)

    @pl.when(c > 0)
    def _():
        copy(kt, ret_out, ret_in, {"context": c - 1}).start()

    weight_push(4)
    weight_push(5)
    weight_push(6)

    @pl.when(c < C - 1)
    def _():
        arrive(kt, ret_in)

    @pl.when(c == C - 1)
    def _():
        ret_in[...] = jnp.zeros((S, 2 * HD), BF16)

    d_kv = (
        kvp[y, core, 1].astype(F32)
        + kvp_core[y, 1].astype(F32)
        + kvp_chip[1].astype(F32)
        + ret_in[...].astype(F32)
    )
    raw = jnp.concatenate([kv_raw[0, shard], kv_raw[1, shard]], axis=1).astype(F32)
    d_raw, gain_k = rms_backward(
        turn_back(d_kv[:, :HD], cosine[shard], sine[shard]), raw, rms_factor(raw), head_gain(1)
    )
    d_kv = jnp.concatenate([d_raw, d_kv[:, HD:]], axis=1).astype(BF16)
    for i in range(4):
        dkv_mine[i] = d_kv[:, i * LANES : (i + 1) * LANES]
    kq = slots(4)
    for i in range(1, 4):
        k = (t + i) % 4
        send(kq + i, dkv_mine.at[k], dkv_cols.at[t], {"tensor": k})
    dkv_cols[t] = dkv_mine[t]
    for i in range(1, 4):
        arrive(kq + i, dkv_cols.at[(t - i + 4) % 4])

    k4 = slots(2)

    def query_back(i, _):
        rows = pl.ds(pl.multiple_of(i * half, half), half)
        pair = pl.ds(i * 2, 2)
        part = contract_last(dq[rows], wa[:, q_cols])
        part = part + contract_last(dkv_cols[pair].reshape(half, LANES), wa[:, kv_part])
        part = part.astype(BF16)
        p4[i, 0] = part[0:S]
        p4[i, 1] = part[S:]
        copy(k4 + i, p4.at[i, 1 - core], p4_core.at[i], partner).start()
        return 0

    lax.fori_loop(0, 2, query_back, 0)

    def attn_grad(n, _):
        cols = pl.ds(pl.multiple_of(n * LANES, LANES), LANES)
        left = nrm[:, cols]
        ga[cols, HD : 2 * HD] = contract_first(left, dq[...]).astype(BF16)
        ga[cols, 2 * HD :] = contract_first(left, dkv_cols[...].reshape(T, LANES)).astype(BF16)
        return 0

    lax.fori_loop(0, D // LANES, attn_grad, 0)
    weight_send(8)
    weight_send(9)
    weight_push(7)
    kc = sum4(k4)
    meet4(kr, block_all)
    save_block = pltpu.make_async_copy(block_all, out_block, ls.at[3])
    save_block.start()
    d_normed = finish4(kc)
    copy(kc, p4_sum, p4_chip, chip_of(1 - y, 2)).wait_send()
    for i in range(2):
        copy(k4 + i, p4.at[i, 1 - core], p4_core.at[i], partner).wait_send()
    values = act[shard].astype(F32)
    d_input, gain_0 = rms_backward(d_normed, values, rms_factor(values), gain(0))
    input_all[y, core] = (dhid[...] + d_input).astype(BF16)
    gain_mine[0:1] = gain_0
    gain_mine[4:8] = jnp.zeros((4, D), F32)
    gain_mine[4:5, 0:HD] = gain_q
    gain_mine[5:6, 0:HD] = gain_k
    kn = slots(4 + 1 + C)
    for i in range(1, 4):
        send(kn + i, gain_mine, gain_tensor.at[i], {"tensor": (t + i) % 4})
    ki = share4(input_all)
    weight_push(8)
    total = gain_mine[...]
    for i in range(1, 4):
        arrive(kn + i, gain_tensor.at[i])
        total = total + gain_tensor[i]
    gain_tensor[0] = total
    send(kn, gain_tensor.at[0], gain_x.at[0], across)
    arrive(kn, gain_x.at[0])
    gain_x[1] = total + gain_x[0]
    for step in range(1, C):
        send(kn + 4 + step, gain_x.at[1], gain_z.at[step], along(step))
    weight_push(9)
    weight_meet(0, 1, 2)
    weight_end(2)
    meet4(ki, input_all)
    save_input = pltpu.make_async_copy(input_all, out_input, ls.at[4])
    save_input.start()
    weight_meet(3, 4)
    weight_end(0)
    weight_meet(5, 8)
    attn = ga[rows_of(f, c)].astype(F32)
    for step in range(1, C):
        attn = attn + ga_z[step - 1].astype(F32)
    kvg[t] = attn[:, 2 * HD :]
    kh = slots(4)
    for i in range(1, 4):
        send(kh + i, kvg.at[t], kvg.at[t], {"tensor": (t + i) % 4})
    st_out[...] = attn[:, 0:HD]
    st_query[...] = attn[:, HD : 2 * HD]
    staged = []

    def save(n, src, dst):
        staged.append(pltpu.make_async_copy(src, dst, ls.at[10 + n]))
        staged[-1].start()

    save(0, st_out, out_out)
    save(1, st_query, out_query)
    total = gain_x[1]
    for step in range(1, C):
        arrive(kn + 4 + step, gain_z.at[step])
        total = total + gain_z[step]
    owner = f * C + c
    moved = pltpu.roll(total, (D - owner * R) % D, 1)
    st_norm[...] = moved[0:4, 0:R]
    moved = pltpu.roll(total[:, 0:HD], (HD - owner * narrow) % HD, 1)
    st_head[...] = moved[4:6, 0:narrow]
    save(2, st_norm, out_norm)
    save(3, st_head, out_head)
    weight_meet(6, 7, 9)
    weight_end(1)
    for i in range(1, 4):
        arrive(kh + i, kvg.at[(t - i + 4) % 4])
    for k in range(4):
        st_kv[:, k * LANES : (k + 1) * LANES] = kvg[k]
    save(4, st_kv, out_kv)
    save_block.wait()
    save_input.wait()
    for moved in staged:
        moved.wait()
    settle()

    @pl.when(c < C - 1)
    def _():
        copy(ks, seg_row, seg_left, {"context": c + 1}).wait_send()
        copy(kk, kv.at[own_half], kv.at[my_half], {"context": c + 1}).wait_send()

    @pl.when(c > 0)
    def _():
        copy(kt, ret_out, ret_in, {"context": c - 1}).wait_send()
    assert counter[0] == SEMAPHORES, counter


def fused(
    mesh,
    activations,
    positions,
    seg_ids,
    norm_gains,
    head_gains,
    w_query,
    w_keyval,
    w_out,
    w_gateup,
    w_down,
    cotangent,
):
    C = mesh.shape["context"]
    T, D = activations.shape[1:]
    R, units = w_down.shape
    U = -(-units // (2 * LANES)) * LANES
    S = T // 4
    pack = -(-R // LANES) * LANES
    operands = (
        activations[0],
        positions,
        seg_ids,
        norm_gains,
        head_gains,
        w_gateup,
        w_down,
        cotangent[0],
        w_query,
        w_keyval,
        w_out,
    )
    scratch = [
        pltpu.VMEM((T, HD // 2), F32),
        pltpu.VMEM((T, HD // 2), F32),
        pltpu.VMEM((8, T), jnp.int32),
        pltpu.VMEM((T, 1), jnp.int32),
        pltpu.VMEM((8, pack), F32),
        pltpu.VMEM((2 * C, 8, pack), F32),
        pltpu.VMEM((2, 3, R, U), BF16),
        pltpu.VMEM((S, D), BF16),
        pltpu.VMEM((D, 2 * HD + LANES), BF16),
        pltpu.VMEM((3, D, U), BF16),
        pltpu.VMEM((8, T), jnp.int32),
        pltpu.VMEM((8, D), F32),
        pltpu.VMEM((8, HD), F32),
        pltpu.VMEM((T, D), BF16),
        pltpu.VMEM((T, HD), F32),
        pltpu.VMEM((4, T, LANES), BF16),
        pltpu.VMEM((T, HD), BF16),
        pltpu.VMEM((2 * T, 2 * HD), BF16),
        pltpu.VMEM((T, 2 * T), F32),
        pltpu.VMEM((T, HD), BF16),
        pltpu.VMEM((2, 2, S, D), BF16),
        pltpu.VMEM((2, S, D), BF16),
        pltpu.VMEM((S, D), BF16),
        pltpu.VMEM((S, D), BF16),
        pltpu.VMEM((S, D), F32),
        pltpu.VMEM((S, D), F32),
        pltpu.VMEM((4, 2, S, D), BF16),
        pltpu.VMEM((4, 2 * S, U), BF16),
        pltpu.VMEM((4, 2 * S, U), BF16),
        pltpu.VMEM((4, 2 * S, U), BF16),
        pltpu.VMEM((4, 2, S, D), BF16),
        pltpu.VMEM((4, S, D), BF16),
        pltpu.VMEM((3, S, D), BF16),
        pltpu.VMEM((3, S, D), BF16),
        pltpu.VMEM((4, 2, S, D), BF16),
        pltpu.VMEM((S, D), F32),
        pltpu.VMEM((2, 2, S, D), BF16),
        pltpu.VMEM((T, 2 * T), BF16),
        pltpu.VMEM((T, HD), BF16),
        pltpu.VMEM((T, HD), BF16),
        pltpu.VMEM((2, 2, 2, S, 2 * HD), BF16),
        pltpu.VMEM((2, 2, S, 2 * HD), BF16),
        pltpu.VMEM((2, S, 2 * HD), BF16),
        pltpu.VMEM((2, S, 2 * HD), BF16),
        pltpu.VMEM((S, 2 * HD), BF16),
        pltpu.VMEM((S, 2 * HD), BF16),
        pltpu.VMEM((4, S, LANES), BF16),
        pltpu.VMEM((4, S, LANES), BF16),
        pltpu.VMEM((3, C * R, U), BF16),
        pltpu.VMEM((C - 1, 3, R, U), BF16),
        pltpu.VMEM((D, 2 * HD + LANES), BF16),
        pltpu.VMEM((C * R, 2 * HD + LANES), BF16),
        pltpu.VMEM((C - 1, R, 2 * HD + LANES), BF16),
        pltpu.VMEM((4, R, LANES), F32),
        pltpu.VMEM((R, units), F32),
        pltpu.VMEM((8, D), F32),
        pltpu.VMEM((4, 8, D), F32),
        pltpu.VMEM((2, 8, D), F32),
        pltpu.VMEM((C, 8, D), F32),
        pltpu.VMEM((2, 2, S, D), BF16),
        pltpu.VMEM((2, 2, S, D), BF16),
        pltpu.VMEM((R, HD), F32),
        pltpu.VMEM((R, HD), F32),
        pltpu.VMEM(norm_gains.shape, F32),
        pltpu.VMEM(head_gains.shape, F32),
        pltpu.VMEM((R, 2 * HD), F32),
        pltpu.SemaphoreType.DMA((SEMAPHORES,)),
        pltpu.SemaphoreType.DMA((SEMAPHORES,)),
        pltpu.SemaphoreType.DMA((15,)),
    ]
    vmem = pl.BlockSpec(memory_space=pltpu.VMEM)
    anywhere = pl.BlockSpec(memory_space=pl.ANY)
    results = (
        jax.ShapeDtypeStruct((2, 2, S, D), BF16),
        jax.ShapeDtypeStruct((2, 2, S, D), BF16),
        jax.ShapeDtypeStruct(norm_gains.shape, F32),
        jax.ShapeDtypeStruct(head_gains.shape, F32),
        jax.ShapeDtypeStruct(w_query.shape, F32),
        jax.ShapeDtypeStruct(w_keyval.shape, F32),
        jax.ShapeDtypeStruct(w_out.shape, F32),
        jax.ShapeDtypeStruct(w_gateup.shape, F32),
        jax.ShapeDtypeStruct(w_down.shape, F32),
    )
    sizes = {"context": C, "tokens": T, "width": D, "rows": R, "units": U}
    parts = pl.pallas_call(
        functools.partial(fused_kernel, sizes),
        out_shape=results,
        in_specs=[vmem] * 7 + [anywhere] * 4,
        out_specs=[anywhere] * len(results),
        scratch_shapes=scratch,
        compiler_params=pltpu.CompilerParams(
            collective_id=0, has_side_effects=True, vmem_limit_bytes=67043328
        ),
    )(*operands)
    count = len(parts)
    block_out, input_grad, *grads = pl.pallas_call(
        functools.partial(emit_kernel, count),
        out_shape=results,
        in_specs=[anywhere] * count,
        out_specs=[anywhere] * count,
        scratch_shapes=[pltpu.VMEM(part.shape, part.dtype) for part in parts]
        + [pltpu.SemaphoreType.DMA((count,))] * 2,
    )(*parts)
    return block_out.reshape(1, T, D), input_grad.reshape(1, T, D), *grads


def block(mesh, *arrays):
    tokens, rows = arrays[0].shape[1], arrays[9].shape[0]
    fits = (
        mesh.shape["fsdp"] == 2
        and mesh.shape["tensor"] == 4
        and mesh.shape["context"] == 4
        and tokens == WINDOW
        and rows % 16 == 0
        and arrays[5].shape[1] == HD
        and arrays[6].shape[1] == 4 * LANES
    )
    return fused(mesh, *arrays) if fits else shards(*arrays)


def shards(
    activations,
    positions,
    seg_ids,
    norm_gains,
    head_gains,
    w_query,
    w_keyval,
    w_out,
    w_gateup,
    w_down,
    cotangent,
):
    tokens = activations.shape[1]
    local_heads = w_query.shape[1] // HD
    inputs = activations[0].astype(jnp.float32)
    places = positions[0]
    documents = seg_ids[0]
    gains_all, heads_all, query_all, keyval_all, out_all = (
        lax.all_gather(norm_gains, ("fsdp", "context"), axis=1, tiled=True),
        lax.all_gather(head_gains, ("fsdp", "context"), axis=1, tiled=True),
        lax.all_gather(w_query, ("fsdp", "context"), axis=0, tiled=True),
        lax.all_gather(w_keyval, ("fsdp", "context"), axis=0, tiled=True),
        lax.all_gather(w_out, ("fsdp", "context"), axis=0, tiled=True),
    )
    gains_f = gains_all.astype(jnp.float32)
    heads_f = heads_all.astype(jnp.float32)
    normed_f, input_back = jax.vjp(rms_norm, inputs, gains_f[0])
    normed = normed_f.astype(jnp.bfloat16)
    query_raw = jnp.dot(normed, query_all, preferred_element_type=jnp.float32).reshape(
        tokens, local_heads, HD
    )
    keyval_raw = jnp.dot(normed, keyval_all, preferred_element_type=jnp.float32)

    def prepare(raw_heads, head_gain):
        return rotate(rms_norm(raw_heads, head_gain), places)

    query_rot, query_back = jax.vjp(prepare, query_raw, heads_f[0])
    key_rot, key_back = jax.vjp(prepare, keyval_raw[:, None, :HD], heads_f[1])
    queries = query_rot.astype(jnp.bfloat16)
    own_keyval = jnp.concatenate([key_rot[:, 0], keyval_raw[:, HD:]], axis=1).astype(jnp.bfloat16)
    labels = jnp.stack([places, documents])
    keep_from = tokens - tokens
    left_keyval, left_labels = from_behind((own_keyval, labels), "context", 1)
    keys_all = jnp.concatenate([left_keyval, own_keyval], axis=0)
    key_places = jnp.concatenate([left_labels[0], places])
    key_documents = jnp.concatenate([left_labels[1], documents])
    has_left = lax.axis_index("context") > 0
    key_live = jnp.concatenate([jnp.full((tokens,), has_left), jnp.ones((tokens,), dtype=bool)])
    scale_factor = HD ** (-0.5)
    block_rows = 512
    block_starts = jnp.arange(tokens // block_rows) * block_rows

    def block_scores():
        spacing = places[:, None] - key_places[None, :]
        visible = (
            key_live[None, :]
            & (documents[:, None] == key_documents[None, :])
            & (spacing >= 0)
            & (spacing < WINDOW)
        )
        raw_scores = (
            jnp.einsum("qhd,kd->hqk", queries, keys_all[:, :HD], preferred_element_type=jnp.float32)
            * scale_factor
        )
        return (jnp.where(visible[None], raw_scores, -1e30), keys_all, queries)

    def forward_block(start):
        scores, near_keyval, query_block = block_scores()
        row_top = jnp.max(scores, axis=-1, keepdims=True)
        raised = jnp.exp(scores - row_top)
        row_total = jnp.sum(raised, axis=-1, keepdims=True)
        probs = raised / row_total
        mixed_block = jnp.einsum(
            "hqk,kd->qhd",
            probs.astype(jnp.bfloat16),
            near_keyval[:, HD:],
            preferred_element_type=jnp.float32,
        )
        return (mixed_block.astype(jnp.bfloat16), row_top + jnp.log(row_total))

    mixed_blocks, log_blocks = lax.map(forward_block, block_starts)
    mixed_low = mixed_blocks.reshape(tokens, local_heads * HD)
    branch = lax.psum(contract_last(mixed_low, out_all).astype(jnp.bfloat16), "tensor").astype(jnp.float32)
    post_attn, post_attn_back = jax.vjp(rms_norm, branch, gains_f[1])
    hidden = inputs + post_attn
    normed_mlp_f, pre_mlp_back = jax.vjp(rms_norm, hidden, gains_f[2])
    normed_mlp = normed_mlp_f.astype(jnp.bfloat16)
    columns = normed_mlp
    gate_up = jnp.einsum(
        "bn,nkf->bkf",
        columns,
        lax.all_gather(w_gateup, ("fsdp", "context"), axis=0, tiled=True),
        preferred_element_type=jnp.float32,
    )
    active_f, glu_back = jax.vjp(glu, gate_up)
    active = active_f.astype(jnp.bfloat16)
    down = lax.psum(
        contract_last(
            active, lax.all_gather(w_down, ("fsdp", "context"), axis=0, tiled=True)
        ).astype(jnp.bfloat16),
        "tensor",
    ).astype(jnp.float32)
    post_mlp, post_mlp_back = jax.vjp(rms_norm, down, gains_f[3])
    result = hidden + post_mlp
    grad_out = cotangent[0].astype(jnp.float32)
    d_down, gain_post_mlp = post_mlp_back(grad_out)
    down_low = d_down.astype(jnp.bfloat16)
    columns = down_low
    d_active = jnp.dot(
        columns,
        lax.all_gather(w_down, ("fsdp", "context"), axis=0, tiled=True),
        preferred_element_type=jnp.float32,
    )
    d_gate_up = glu_back(d_active)[0].astype(jnp.bfloat16)
    d_normed_part = jnp.einsum(
        "bkf,nkf->bn",
        d_gate_up,
        lax.all_gather(w_gateup, ("fsdp", "context"), axis=0, tiled=True),
        preferred_element_type=jnp.float32,
    )
    d_normed_mlp = lax.psum(d_normed_part.astype(jnp.bfloat16), "tensor").astype(jnp.float32)
    d_hidden_norm, gain_pre_mlp = pre_mlp_back(d_normed_mlp)
    d_hidden = grad_out + d_hidden_norm
    features = normed_mlp
    grad_cols = down_low
    gate_up_term = jnp.einsum(
        "bn,bkf->nkf", features, d_gate_up, preferred_element_type=jnp.float32
    )
    down_term = contract_first(grad_cols, active)
    scatter = lambda part: lax.psum_scatter(
        part.astype(jnp.bfloat16), ("fsdp", "context"), scatter_dimension=0, tiled=True
    ).astype(jnp.float32)
    gate_grad = scatter(gate_up_term[:, 0])
    up_grad = scatter(gate_up_term[:, 1])
    down_grad = scatter(down_term)
    d_branch, gain_post_attn = post_attn_back(d_hidden)
    branch_low = d_branch.astype(jnp.bfloat16)
    d_mixed = jnp.dot(branch_low, out_all, preferred_element_type=jnp.float32)
    d_mixed_low = d_mixed.astype(jnp.bfloat16).reshape(tokens, local_heads, HD)

    def backward_block(carry, item):
        start, log_block = item
        scores, near_keyval, query_block = block_scores()
        probs_again = jnp.exp(scores - log_block)
        d_probs = jnp.einsum(
            "qhd,kd->hqk", d_mixed_low, near_keyval[:, HD:], preferred_element_type=jnp.float32
        )
        row_inner = jnp.sum(probs_again * d_probs, axis=-1, keepdims=True)
        d_scores = (probs_again * (d_probs - row_inner)).astype(jnp.bfloat16)
        d_query_block = (
            jnp.einsum(
                "hqk,kd->qhd", d_scores, near_keyval[:, :HD], preferred_element_type=jnp.float32
            )
            * scale_factor
        )
        d_keys = (
            jnp.einsum("hqk,qhd->kd", d_scores, query_block, preferred_element_type=jnp.float32)
            * scale_factor
        )
        d_values = jnp.einsum(
            "hqk,qhd->kd",
            probs_again.astype(jnp.bfloat16),
            d_mixed_low,
            preferred_element_type=jnp.float32,
        )
        updated = carry + jnp.concatenate([d_keys, d_values], axis=1)
        return (updated, d_query_block)

    d_keyval, d_query_blocks = lax.scan(
        backward_block,
        jnp.zeros((tokens + tokens, 2 * HD), jnp.float32),
        (block_starts, log_blocks),
    )
    d_queries = d_query_blocks.reshape(tokens, local_heads, HD)
    returned = from_behind(d_keyval[:tokens].astype(jnp.bfloat16), "context", -1).astype(
        jnp.float32
    )
    own_grad = d_keyval[tokens:].at[keep_from:].add(returned)
    d_query_raw, gain_query = query_back(d_queries)
    d_query_low = d_query_raw.reshape(tokens, local_heads * HD).astype(jnp.bfloat16)
    d_normed_query, keyval_grad, gain_query_all = (
        lax.psum(contract_last(d_query_low, query_all).astype(jnp.bfloat16), "tensor").astype(
            jnp.float32
        ),
        lax.psum(own_grad.astype(jnp.bfloat16), "tensor").astype(jnp.float32),
        lax.psum(gain_query.astype(jnp.bfloat16), "tensor").astype(jnp.float32),
    )
    d_key_raw, gain_key = key_back(keyval_grad[:, None, :HD])
    d_keyval_low = jnp.concatenate([d_key_raw[:, 0], keyval_grad[:, HD:]], axis=1).astype(
        jnp.bfloat16
    )
    d_normed = d_normed_query + contract_last(d_keyval_low, keyval_all)
    d_input_norm, gain_input = input_back(d_normed)
    input_total = d_hidden + d_input_norm
    features = normed
    grad_cols = branch_low
    attn_grads = lax.psum_scatter(
        jnp.stack(
            [contract_first(features, d_query_low), contract_first(grad_cols, mixed_low)], axis=1
        ).astype(jnp.bfloat16),
        ("fsdp", "context"),
        scatter_dimension=0,
        tiled=True,
    ).astype(jnp.float32)
    keyval_term = contract_first(normed, d_keyval_low)
    gain_terms = jnp.stack([gain_input, gain_post_attn, gain_pre_mlp, gain_post_mlp])
    head_terms = jnp.stack([gain_query_all, gain_key])
    gain_grad, head_grad, keyval_weight_grad = (
        lax.psum_scatter(
            gain_terms.astype(jnp.bfloat16), ("fsdp", "context"), scatter_dimension=1, tiled=True
        ).astype(jnp.float32),
        lax.psum_scatter(
            head_terms.astype(jnp.bfloat16), ("fsdp", "context"), scatter_dimension=1, tiled=True
        ).astype(jnp.float32),
        lax.psum_scatter(
            keyval_term.astype(jnp.bfloat16), ("fsdp", "context"), scatter_dimension=0, tiled=True
        ).astype(jnp.float32),
    )
    return (
        result[None].astype(jnp.bfloat16),
        input_total[None].astype(jnp.bfloat16),
        gain_grad,
        head_grad,
        attn_grads[:, 0],
        keyval_weight_grad,
        attn_grads[:, 1],
        jnp.stack([gate_grad, up_grad], axis=1),
        down_grad,
    )


def solution(mesh):
    return jax.shard_map(
        functools.partial(block, mesh),
        mesh=mesh,
        in_specs=(
            P("fsdp", "context", None),
            P("fsdp", "context"),
            P("fsdp", "context"),
            P(None, ("fsdp", "context")),
            P(None, ("fsdp", "context")),
            P(("fsdp", "context"), "tensor"),
            P(("fsdp", "context"), None),
            P(("fsdp", "context"), "tensor"),
            P(("fsdp", "context"), None, "tensor"),
            P(("fsdp", "context"), "tensor"),
            P("fsdp", "context", None),
        ),
        out_specs=(
            P("fsdp", "context", None),
            P("fsdp", "context", None),
            P(None, ("fsdp", "context")),
            P(None, ("fsdp", "context")),
            P(("fsdp", "context"), "tensor"),
            P(("fsdp", "context"), None),
            P(("fsdp", "context"), "tensor"),
            P(("fsdp", "context"), None, "tensor"),
            P(("fsdp", "context"), "tensor"),
        ),
        check_vma=False,
    )
```

```python
import functools
import math

import jax
import jax.numpy as jnp
from jax import lax
from jax.experimental import pallas as pl
from jax.experimental.pallas import tpu as pltpu
from jax.sharding import PartitionSpec as P

HD = 256
WINDOW = 512


EPSILON = 1e-06


def from_behind(block, axis, distance):
    devices = range(lax.axis_size(axis))
    route = [(i - distance, i) for i in devices if i - distance in devices]
    return lax.ppermute(block, axis, route)


def rms_norm(values, gain):
    factor = lax.rsqrt(jnp.mean(values * values, axis=-1, keepdims=True) + EPSILON)
    return values * factor * gain


def rotate(tensor, places):
    width_all = tensor.shape[-1]
    half_width = width_all // 2
    freqs = jnp.power(10000.0, -jnp.arange(half_width, dtype=jnp.float32) * 2.0 / width_all)
    angles = places.astype(jnp.float32)[:, None] * freqs[None, :]
    cosine = jnp.cos(angles)[:, None, :]
    sine = jnp.sin(angles)[:, None, :]
    first_half = tensor[..., :half_width]
    second_half = tensor[..., half_width:]
    return jnp.concatenate(
        [first_half * cosine - second_half * sine, second_half * cosine + first_half * sine],
        axis=-1,
    )


def glu(gate_up):
    return jax.nn.gelu(gate_up[:, 0], approximate=True) * gate_up[:, 1]


def contract_last(left_side, right_side):
    return lax.dot_general(
        left_side, right_side, (((1,), (1,)), ((), ())), preferred_element_type=jnp.float32
    )


def contract_first(left_side, right_side):
    return lax.dot_general(
        left_side, right_side, (((0,), (0,)), ((), ())), preferred_element_type=jnp.float32
    )


MESH = pl.DeviceIdType.MESH
F32 = jnp.float32
BF16 = jnp.bfloat16
LANES = 128
SEMAPHORES = 178


def mm(left, right):
    return jnp.dot(left, right, preferred_element_type=F32)


def rms_factor(values):
    return lax.rsqrt(jnp.mean(values * values, axis=-1, keepdims=True) + EPSILON)


def rms_backward(grad, values, factor, gain):
    unit = values * factor
    scaled = grad * gain
    inner = jnp.mean(scaled * unit, axis=-1, keepdims=True)
    return factor * (scaled - unit * inner), jnp.sum(grad * unit, axis=0, keepdims=True)


def turn(values, cosine, sine):
    half = values.shape[-1] // 2
    first, second = values[:, :half], values[:, half:]
    return jnp.concatenate([first * cosine - second * sine, second * cosine + first * sine], axis=1)


def turn_back(values, cosine, sine):
    half = values.shape[-1] // 2
    first, second = values[:, :half], values[:, half:]
    return jnp.concatenate([first * cosine + second * sine, second * cosine - first * sine], axis=1)


def emit_kernel(count, *refs):
    sources, results, held = refs[:count], refs[count : 2 * count], refs[2 * count : 3 * count]
    incoming, outgoing = refs[3 * count :]
    reads = [pltpu.make_async_copy(sources[n], held[n], incoming.at[n]) for n in range(count)]
    writes = [pltpu.make_async_copy(held[n], results[n], outgoing.at[n]) for n in range(count)]
    for moved in reads:
        moved.start()
    for n in range(count):
        reads[n].wait()
        writes[n].start()
    for moved in writes:
        moved.wait()


def fused_kernel(
    sizes,
    act_all,
    positions,
    seg_ids,
    norm_gains,
    head_gains,
    gateup_all,
    down_all,
    cot_all,
    w_query,
    w_keyval,
    w_out,
    out_block,
    out_input,
    out_norm,
    out_head,
    out_query,
    out_kv,
    out_out,
    out_gateup,
    out_down,
    act,
    w_gateup,
    w_down,
    cosine,
    sine,
    seg_row,
    seg_col,
    gain_pack,
    gain_all,
    w_ff,
    cot,
    wa,
    wf,
    seg_left,
    gain_rows,
    head_rows,
    nrm,
    qraw,
    kv_raw,
    qs,
    kv,
    probs,
    mix,
    p4,
    p4_core,
    p4_sum,
    p4_chip,
    hid,
    bran,
    xg,
    gel,
    upg,
    active,
    p8,
    p8_core,
    p8_sum,
    p8_chip,
    dd,
    dhid,
    db,
    dscore,
    dmix,
    dq,
    kvp,
    kvp_core,
    kvp_sum,
    kvp_chip,
    ret_out,
    ret_in,
    dkv_mine,
    dkv_cols,
    gall_x,
    gall_z,
    ga,
    ga_x,
    ga_z,
    kvg,
    ff_stage,
    gain_mine,
    gain_tensor,
    gain_x,
    gain_z,
    block_all,
    input_all,
    st_out,
    st_query,
    st_norm,
    st_head,
    st_kv,
    ss,
    rs,
    ls,
):
    C = sizes["context"]
    T, D, R, U = sizes["tokens"], sizes["width"], sizes["rows"], sizes["units"]
    units = w_down.shape[1]
    narrow = HD // (2 * C)
    S = T // 4
    f = lax.axis_index("fsdp")
    c = lax.axis_index("context")
    t = lax.axis_index("tensor")
    y, core = t // 2, t % 2
    m = c % 2
    base = c - m
    partner = {"tensor": y * 2 + (1 - core)}
    across = {"fsdp": 1 - f}
    counter = [0]
    sent = []

    def slots(count):
        first = counter[0]
        counter[0] += count
        assert counter[0] <= SEMAPHORES
        return first

    def copy(k, src, dst, device):
        return pltpu.make_async_remote_copy(
            src_ref=src,
            dst_ref=dst,
            send_sem=ss.at[k],
            recv_sem=rs.at[k],
            device_id=device,
            device_id_type=MESH,
        )

    def send(k, src, dst, device):
        moved = copy(k, src, dst, device)
        moved.start()
        sent.append(moved)

    def arrive(k, dst):
        copy(k, dst, dst, partner).wait_recv()

    def settle():
        for moved in sent:
            moved.wait_send()
        sent.clear()

    def along(step):
        return {"context": (c + step) % C}

    def rows_of(ff, cc):
        return pl.ds(pl.multiple_of((ff * C + cc) * R, R), R)

    def chip_of(k, count):
        if count == 2:
            return {"tensor": k * 2 + core}
        return {"context": base + k // 2, "tensor": (k % 2) * 2 + core}

    loads = [
        pltpu.make_async_copy(src, dst, ls.at[15 + n])
        for n, (src, dst) in enumerate(
            ((gateup_all, w_gateup), (down_all, w_down), (act_all, act))
        )
    ]
    for moved in loads:
        moved.start()

    barrier = pltpu.get_barrier_semaphore()
    greeted = [along(step) for step in range(1, C)] + [across]
    greeted += [{"tensor": (t + step) % 4} for step in range(1, 4)]
    greeted += [{"context": base + 1 - m, "tensor": (1 - y) * 2 + core}]
    for device in greeted:
        pl.semaphore_signal(barrier, inc=1, device_id=device, device_id_type=MESH)
    gain_pack[...] = jnp.zeros(gain_pack.shape, F32)
    gain_pack[0:4, 0:R] = norm_gains[...].astype(F32)
    gain_pack[4:6, 0:narrow] = head_gains[...].astype(F32)
    seg_row[...] = jnp.broadcast_to(seg_ids[...], seg_row.shape)
    pl.semaphore_wait(barrier, len(greeted))

    mine = rows_of(f, c)
    kv_cols = pl.ds(pl.multiple_of(t * LANES, LANES), LANES)
    attn_parts = (
        (w_query, slice(0, HD)),
        (w_keyval.at[:, kv_cols], slice(HD, HD + LANES)),
        (w_out, slice(HD + LANES, 2 * HD + LANES)),
    )
    q_cols, kv_part, o_cols = (cols for _, cols in attn_parts[:3])
    local = []
    for n, (part, cols) in enumerate(attn_parts):
        local.append(pltpu.make_async_copy(part, wa.at[mine, cols], ls.at[6 + n]))
        local[-1].start()
    ka = slots(3 * C)
    kar = slots(C - 1)
    kg = slots(2 * C - 1)
    for step in range(1, C):
        for n, (part, cols) in enumerate(attn_parts):
            send(ka + 3 * step + n, part, wa.at[mine, cols], along(step))
    for n, (part, cols) in enumerate(attn_parts):
        send(ka + n, part, wa.at[mine, cols], across)
    own_gain = gain_all.at[f * C + c]
    gain_all[f * C + c] = gain_pack[...]
    for step in range(1, C):
        send(kg + step, gain_pack, own_gain, along(step))
    send(kg, gain_pack, own_gain, across)
    ks = slots(1)

    @pl.when(c < C - 1)
    def _():
        copy(ks, seg_row, seg_left, {"context": c + 1}).start()

    pieces = ((0, 0, 384), (0, 384, U), (1, 0, 512), (1, 512, U), (2, 0, 512), (2, 512, U))
    kf = slots((2 * C - 1) * len(pieces))

    def piece(p, rows):
        w, low, high = pieces[p]
        return wf.at[w, rows, low:high]

    side = c // 2
    near, far = 2 - side, 3 * (1 - side)

    def send_ff(p):
        k = kf + (2 * C - 1) * p
        w, low, high = pieces[p]
        turns = tuple((c + step) % C for step in range(1, C))
        for to in (base + 1 - m, near, far) if p in (3, 4) else turns:
            send(
                k + (to - c + C) % C,
                w_ff.at[to % 2, w, :, low:high],
                piece(p, mine),
                {"context": to},
            )
        send(k, w_ff.at[m, w, :, low:high], piece(p, mine), across)

    def relay_ff(p):
        k = kf + (2 * C - 1) * p
        for source in (base + 1 - m, near, far):
            step = (c - source + C) % C
            part = piece(p, rows_of(f, source))
            arrive(k + step, part)
            send(k + C - 1 + step, part, part, across)

    def meet_ff(p):
        k = kf + (2 * C - 1) * p
        arrive(k, piece(p, rows_of(1 - f, c)))
        for step in range(1, C):
            arrive(k + C - 1 + step, piece(p, rows_of(1 - f, (c - step + C) % C)))

    for moved in loads:
        moved.wait()
    for w in range(3):
        whole = w_down[...] if w == 2 else w_gateup[:, w, :]
        w_ff[0, w] = whole[:, 0:U]
        w_ff[1, w, :, 0 : units - U] = whole[:, U:units]
        w_ff[1, w, :, units - U :] = jnp.zeros((R, 2 * U - units), BF16)
    seg_col[...] = jnp.transpose(seg_row[...].astype(F32))[:, 0:1].astype(jnp.int32)
    place = jnp.broadcast_to(positions[...].astype(F32), (8, T))
    index = lax.broadcasted_iota(jnp.int32, (1, HD // 2), 1).astype(F32)
    angle = jnp.transpose(place)[:, 0:1] * jnp.exp(index * (-2.0 * math.log(10000.0) / HD))
    cosine[...] = jnp.cos(angle)
    sine[...] = jnp.sin(angle)
    shard = pl.ds(pl.multiple_of(t * S, S), S)
    own_cot = pltpu.make_async_copy(cot_all.at[shard], cot, ls.at[2])
    own_cot.start()
    own_ff = pltpu.make_async_copy(w_ff.at[m], wf.at[:, mine], ls.at[1])
    own_ff.start()
    for step in range(1, C):
        other = rows_of(f, (c - step + C) % C)
        for n, (_, cols) in enumerate(attn_parts):
            arrive(ka + 3 * step + n, wa.at[other, cols])
        send(kar + step - 1, wa.at[other], wa.at[other], across)
        part = gain_all.at[f * C + (c - step + C) % C]
        arrive(kg + step, part)
        send(kg + C - 1 + step, part, part, across)
    for moved in local:
        moved.wait()
    send_ff(0)
    for n, (_, cols) in enumerate(attn_parts):
        arrive(ka + n, wa.at[rows_of(1 - f, c), cols])
    for step in range(1, C):
        arrive(kar + step - 1, wa.at[rows_of(1 - f, (c - step + C) % C)])

    @pl.when(c > 0)
    def _():
        arrive(ks, seg_left)

    @pl.when(c == 0)
    def _():
        seg_left[...] = jnp.full(seg_left.shape, -1, jnp.int32)
        kv[0:T] = jnp.zeros((T, 2 * HD), BF16)

    arrive(kg, gain_all.at[(1 - f) * C + c])
    for step in range(1, C):
        arrive(kg + C - 1 + step, gain_all.at[(1 - f) * C + (c - step + C) % C])
    wide = jnp.zeros((8, D), F32)
    heads = jnp.zeros((8, HD), F32)
    blank = jnp.zeros((8, D - gain_pack.shape[1]), F32)
    for j in range(2 * C):
        part = gain_all[j]
        wide = wide + pltpu.roll(jnp.concatenate([part, blank], axis=1), j * R, 1)
        heads = heads + pltpu.roll(part[:, 0:HD], j * narrow, 1)
    gain_rows[...] = wide
    head_rows[...] = heads

    def gain(index):
        return gain_rows[index : index + 1]

    def head_gain(index):
        return head_rows[4 + index : 5 + index]

    half = T // 2

    def project(i, _):
        rows = pl.ds(pl.multiple_of(i * half, half), half)
        values = act[rows].astype(F32)
        low = (values * rms_factor(values) * gain(0)).astype(BF16)
        nrm[rows] = low
        kv_raw[t, rows] = mm(low, wa[:, kv_part]).astype(BF16)
        return 0

    lax.fori_loop(0, 2, project, 0)
    ku = slots(4)
    for i in range(1, 4):
        send(ku + i, kv_raw.at[t], kv_raw.at[t], {"tensor": (t + i) % 4})

    def query(i, _):
        rows = pl.ds(pl.multiple_of(i * half, half), half)
        raw_q = mm(nrm[rows], wa[:, q_cols])
        qraw[rows] = raw_q
        qs[rows] = turn(
            raw_q * rms_factor(raw_q) * head_gain(0), cosine[rows], sine[rows]
        ).astype(BF16)
        return 0

    lax.fori_loop(0, 2, query, 0)
    for i in range(1, 4):
        arrive(ku + i, kv_raw.at[(t - i + 4) % 4])

    def key(i, _):
        rows = pl.ds(pl.multiple_of(i * half, half), half)
        raw_k = jnp.concatenate([kv_raw[0, rows], kv_raw[1, rows]], axis=1).astype(F32)
        own = pl.ds(pl.multiple_of(T + i * half, half), half)
        kv[own, 0:HD] = turn(
            raw_k * rms_factor(raw_k) * head_gain(1), cosine[rows], sine[rows]
        ).astype(BF16)
        kv[own, HD : HD + LANES] = kv_raw[2, rows]
        kv[own, HD + LANES :] = kv_raw[3, rows]
        return 0

    lax.fori_loop(0, 2, key, 0)
    kk = slots(2)
    my_half = pl.ds(pl.multiple_of(core * half, half), half)
    other_half = pl.ds(pl.multiple_of((1 - core) * half, half), half)
    own_half = pl.ds(pl.multiple_of(T + core * half, half), half)

    @pl.when(c < C - 1)
    def _():
        copy(kk, kv.at[own_half], kv.at[my_half], {"context": c + 1}).start()

    send_ff(1)
    send_ff(2)
    relay_ff(0)

    @pl.when(c > 0)
    def _():
        arrive(kk, kv.at[my_half])
        moved = copy(kk + 1, kv.at[my_half], kv.at[my_half], partner)
        moved.start()
        arrive(kk + 1, kv.at[other_half])
        moved.wait_send()

    scale = HD**-0.5
    no_left = jnp.where(c > 0, 0, 2 * T)
    k4 = slots(2)

    def attend(i, _):
        rows = pl.ds(pl.multiple_of(i * half, half), half)
        q = qs[rows]
        labels = seg_col[rows]
        row = lax.broadcasted_iota(jnp.int32, (half, T), 0) + i * half
        col = lax.broadcasted_iota(jnp.int32, (half, T), 1)
        left = contract_last(q, kv[0:T, 0:HD]) * scale
        left = jnp.where((labels == seg_left[0:1]) & (col > row + no_left), left, -1e30)
        own = contract_last(q, kv[T:, 0:HD]) * scale
        own = jnp.where((labels == seg_row[0:1]) & (col <= row), own, -1e30)
        top = jnp.maximum(
            jnp.max(left, axis=1, keepdims=True), jnp.max(own, axis=1, keepdims=True)
        )
        left, own = jnp.exp(left - top), jnp.exp(own - top)
        total = jnp.sum(left, axis=1, keepdims=True) + jnp.sum(own, axis=1, keepdims=True)
        left, own = left / total, own / total
        probs[rows, 0:T] = left
        probs[rows, T:] = own
        mixed = mm(left.astype(BF16), kv[0:T, HD:]) + mm(own.astype(BF16), kv[T:, HD:])
        mixed = mixed.astype(BF16)
        mix[rows] = mixed
        part = contract_last(mixed, wa[:, o_cols]).astype(BF16)
        p4[i, 0] = part[0:S]
        p4[i, 1] = part[S:]
        copy(k4 + i, p4.at[i, 1 - core], p4_core.at[i], partner).start()
        return 0

    lax.fori_loop(0, 2, attend, 0)

    def sum4(k):
        kc = slots(1)
        arrive(k + (1 - y), p4_core.at[1 - y])
        p4_sum[...] = (
            p4[1 - y, core].astype(F32) + p4_core[1 - y].astype(F32)
        ).astype(BF16)
        copy(kc, p4_sum, p4_chip, chip_of(1 - y, 2)).start()
        arrive(k + y, p4_core.at[y])
        return kc

    def finish4(kc):
        arrive(kc, p4_chip)
        return (
            p4[y, core].astype(F32)
            + p4_core[y].astype(F32)
            + p4_chip[...].astype(F32)
        )

    kc = sum4(k4)
    relay_ff(1)
    branch = finish4(kc)
    copy(kc, p4_sum, p4_chip, chip_of(1 - y, 2)).wait_send()
    for i in range(2):
        copy(k4 + i, p4.at[i, 1 - core], p4_core.at[i], partner).wait_send()

    bran[...] = branch
    hidden = act[shard].astype(F32) + branch * rms_factor(branch) * gain(1)
    hid[...] = hidden
    low = (hidden * rms_factor(hidden) * gain(2)).astype(BF16)

    me = m * 2 + y

    def gather8(full, value):
        kg = slots(8)
        full[me, core] = value
        send(kg + 4, full.at[me, core], full.at[me, core], partner)
        for i in range(1, 4):
            send(kg + i, full.at[me, core], full.at[me, core], chip_of((me + i) % 4, 4))
        return kg

    def pass8(kg, full, i):
        k = (me - i + 4) % 4
        arrive(kg + i, full.at[k, core])
        copy(kg + 4 + i, full.at[k, core], full.at[k, core], partner).start()

    def meet8(kg, full, i):
        k = (me - i + 4) % 4
        arrive(kg + 4 + i, full.at[k, 1 - core])

    def settle8(kg, full):
        for i in range(1, 4):
            k = (me - i + 4) % 4
            copy(kg + 4 + i, full.at[k, core], full.at[k, core], partner).wait_send()

    def give8(ko, i):
        k = (me - i + 4) % 4
        copy(ko + i, p8.at[k, 1 - core], p8_core.at[i], partner).start()

    def push8(ko, i):
        k = (me - i + 4) % 4
        arrive(ko + i, p8_core.at[i])
        p8_sum[i - 1] = (
            p8[k, core].astype(F32) + p8_core[i].astype(F32)
        ).astype(BF16)
        copy(ko + 4 + i, p8_sum.at[i - 1], p8_chip.at[i - 1], chip_of(k, 4)).start()

    def finish8(ko):
        arrive(ko, p8_core.at[0])
        total = p8[me, core].astype(F32) + p8_core[0].astype(F32)
        for i in range(1, 4):
            arrive(ko + 4 + i, p8_chip.at[i - 1])
            total = total + p8_chip[i - 1].astype(F32)
        for i in range(4):
            copy(ko + i, p8.at[0, 1 - core], p8_core.at[i], partner).wait_send()
        for i in range(1, 4):
            copy(ko + 4 + i, p8_sum.at[0], p8_chip.at[0], partner).wait_send()
        return total

    kx = slots(7)
    beside, beyond = m * 2 + 1 - y, (1 - m) * 2 + y
    corner = (1 - m) * 2 + 1 - y
    xg[me, core] = low
    send(kx + 2, xg.at[me, core], xg.at[me, core], chip_of(beyond, 4))
    send(kx + 1, xg.at[me, core], xg.at[me, core], chip_of(beside, 4))
    send(kx, xg.at[me, core], xg.at[me, core], partner)
    send_ff(3)
    send_ff(4)
    relay_ff(2)
    send_ff(5)
    relay_ff(3)
    for i, k in ((1, beside), (2, beyond), (3, corner)):
        part = xg.at[k, core]
        arrive(kx + i, part)
        if i == 2:
            send(kx + 3, part, part, chip_of(beside, 4))
        send(kx + 3 + i, part, part, partner)
    relay_ff(4)
    own_ff.wait()
    own_cot.wait()
    for p in range(4):
        meet_ff(p)
    arrive(kx, xg.at[me, 1 - core])
    for i, k in ((1, beside), (2, beyond), (3, corner)):
        arrive(kx + 3 + i, xg.at[k, 1 - core])
    root = 0.7978845608028654
    ko = slots(8)

    def forward(i, _):
        k = (me - i + 4) % 4
        x = xg[k].reshape(2 * S, D)
        gate = mm(x, wf[0])
        up = mm(x, wf[1])
        square = gate * gate
        bent = jnp.tanh(root * gate * (1.0 + 0.044715 * square))
        ramp = 0.5 * (1.0 + bent)
        gelu = gate * ramp
        slope = ramp + 0.5 * gate * (1.0 - bent * bent) * root * (1.0 + 3 * 0.044715 * square)
        gel[k] = gelu.astype(BF16)
        upg[k] = (up * slope).astype(BF16)
        active[k] = (gelu * up).astype(BF16)
        return 0

    lax.fori_loop(0, 3, forward, 0)
    relay_ff(5)
    lax.fori_loop(3, 4, forward, 0)
    meet_ff(4)
    meet_ff(5)

    def lower(i, _):
        k = (me - i + 4) % 4
        p8[k] = contract_last(active[k], wf[2]).astype(BF16).reshape(2, S, D)
        give8(ko, i)

        @pl.when(i > 1)
        def _():
            push8(ko, i - 1)

        return 0

    lax.fori_loop(0, 4, lower, 0)
    push8(ko, 3)
    down = finish8(ko)

    factor = rms_factor(down)
    grad = cot[...].astype(F32)
    result = (hid[...] + down * factor * gain(3)).astype(BF16)
    d_down, gain_3 = rms_backward(grad, down, factor, gain(3))
    gain_mine[3:4] = gain_3
    kd = gather8(dd, d_down.astype(BF16))

    def share4(full):
        kb = slots(3)
        send(kb, full.at[y, core], full.at[y, core], chip_of(1 - y, 2))
        send(kb + 1, full.at[y, core], full.at[y, core], partner)
        return kb

    def meet4(kb, full):
        arrive(kb, full.at[1 - y, core])
        send(kb + 2, full.at[1 - y, core], full.at[1 - y, core], partner)
        arrive(kb + 1, full.at[y, 1 - core])
        arrive(kb + 2, full.at[1 - y, 1 - core])

    block_all[y, core] = result
    ko2 = slots(8)

    def backward(i, _):
        k = (me - i + 4) % 4
        meet8(kd, dd, i)
        low = dd[k].reshape(2 * S, D)
        d_active = mm(low, wf[2])

        @pl.when(i < 3)
        def _():
            pass8(kd, dd, i + 1)

        d_gate = (d_active * upg[k].astype(F32)).astype(BF16)
        d_up = (d_active * gel[k].astype(F32)).astype(BF16)
        upg[k] = d_gate
        gel[k] = d_up
        p8[k] = (
            (contract_last(d_gate, wf[0]) + contract_last(d_up, wf[1]))
            .astype(BF16)
            .reshape(2, S, D)
        )
        give8(ko2, i)

        @pl.when(i > 1)
        def _():
            push8(ko2, i - 1)

        return 0

    lax.fori_loop(0, 4, backward, 0)
    push8(ko2, 3)
    settle8(kd, dd)

    settle()
    gall = wf
    mine_x = pl.ds(pl.multiple_of(f * C * R, C * R), C * R)
    theirs_x = pl.ds(pl.multiple_of((1 - f) * C * R, C * R), C * R)
    ff_chunk = lambda w, low, high: (
        gall.at[w, :, low:high],
        gall_x.at[w, :, low:high],
        gall_z.at[:, w, :, low:high],
    )
    attn_chunk = lambda low, high: (
        ga.at[:, low:high],
        ga_x.at[:, low:high],
        ga_z.at[:, :, low:high],
    )
    chunks = (
        ff_chunk(2, 0, 128),
        ff_chunk(2, 128, 384),
        ff_chunk(2, 384, U),
        ff_chunk(0, 0, 512),
        ff_chunk(0, 512, U),
        attn_chunk(0, HD),
        ff_chunk(1, 0, 256),
        ff_chunk(1, 256, 640),
        attn_chunk(HD, 2 * HD + LANES),
        ff_chunk(1, 640, U),
    )
    kw = slots(len(chunks))
    kz = slots(len(chunks) * (C - 1))

    def weight_grad(w, left, right, early, lead=0):
        def tile(n, low, high):
            cols = pl.ds(pl.multiple_of(n * LANES, LANES), LANES)
            block = left[:, :, :, cols].reshape(8 * S, LANES)
            gall[w, cols, low:high] = contract_first(
                block, right[:, :, low:high].reshape(8 * S, high - low)
            ).astype(BF16)
            return 0

        first = D // LANES // 2
        if lead:
            lax.fori_loop(0, first + 1, lambda n, _: tile(n + first * (1 - f), 0, lead), 0)
            weight_send(early[0])
            early = early[1:]
        lax.fori_loop(0, first + 1, lambda n, _: tile(n + first * (1 - f), lead, U), 0)
        for q in early:
            weight_send(q)
        lax.fori_loop(0, first, lambda n, _: tile(n + (first + 1) * f, 0, U), 0)

    def weight_send(q):
        full, from_x, _ = chunks[q]
        send(kw + q, full.at[theirs_x], from_x, across)

    def weight_push(q):
        full, from_x, from_z = chunks[q]
        arrive(kw + q, from_x)

        def add(n, _):
            rows = pl.ds(pl.multiple_of(f * C * R + n * R, R), R)
            part = pl.ds(pl.multiple_of(n * R, R), R)
            full[rows] = (full[rows].astype(F32) + from_x[part].astype(F32)).astype(BF16)
            return 0

        lax.fori_loop(0, C, add, 0)
        for to in (far, near, base + 1 - m):
            step = (to - c + C) % C
            send(
                kz + q * (C - 1) + step - 1,
                full.at[rows_of(f, to)],
                from_z.at[step - 1],
                {"context": to},
            )

    def weight_meet(*which):
        for q in which:
            for step in range(1, C):
                arrive(kz + q * (C - 1) + step - 1, chunks[q][2].at[step - 1])

    def weight_end(w):
        same = gall[w, rows_of(f, c)].astype(F32)
        other = jnp.zeros((R, U), F32)
        for step in range(1, C):
            if step % 2:
                other = other + gall_z[step - 1, w].astype(F32)
            else:
                same = same + gall_z[step - 1, w].astype(F32)
        ff_stage[:, 0:U] = jnp.where(m == 0, same, other)
        ff_stage[:, U:units] = jnp.where(m == 0, other, same)[:, 0 : units - U]
        into = out_down if w == 2 else out_gateup.at[:, w]
        saved = pltpu.make_async_copy(ff_stage, into, ls.at[5])
        saved.start()
        saved.wait()

    weight_grad(2, dd, active, (0, 1, 2), 128)
    weight_push(0)
    weight_grad(0, xg, upg, (3, 4))
    weight_push(1)
    d_normed = finish8(ko2)
    hidden = hid[...]
    d_hidden, gain_2 = rms_backward(d_normed, hidden, rms_factor(hidden), gain(2))
    d_hidden = cot[...].astype(F32) + d_hidden
    dhid[...] = d_hidden
    gain_mine[2:3] = gain_2
    branch = bran[...]
    d_branch, gain_1 = rms_backward(d_hidden, branch, rms_factor(branch), gain(1))
    gain_mine[1:2] = gain_1
    db[y, core] = d_branch.astype(BF16)
    kb = share4(db)
    weight_grad(1, xg, gel, ())
    weight_push(2)
    meet4(kb, db)

    def out_grad(n, _):
        cols = pl.ds(pl.multiple_of(n * LANES, LANES), LANES)
        ga[cols, 0:HD] = contract_first(
            db[:, :, :, cols].reshape(T, LANES), mix[...]
        ).astype(BF16)
        return 0

    lax.fori_loop(0, D // LANES, out_grad, 0)
    weight_send(5)
    weight_send(6)
    weight_send(7)

    def scores_back(i, gain_q):
        rows = pl.ds(pl.multiple_of(i * half, half), half)
        d_mixed = mm(db[i].reshape(half, D), wa[:, o_cols]).astype(BF16)
        dmix[rows] = d_mixed
        p = probs[rows]
        d_probs = contract_last(d_mixed, kv[:, HD:])
        inner = jnp.sum(p * d_probs, axis=1, keepdims=True)
        low = (p * (d_probs - inner)).astype(BF16)
        dscore[rows] = low
        d_q = mm(low, kv[:, 0:HD]) * scale
        raw = qraw[rows]
        factor = rms_factor(raw)
        d_raw, part = rms_backward(
            turn_back(d_q, cosine[rows], sine[rows]), raw, factor, head_gain(0)
        )
        dq[rows] = d_raw.astype(BF16)
        return gain_q + part

    gain_q = lax.fori_loop(0, 2, scores_back, jnp.zeros((1, HD), F32))
    kp = slots(3)

    def keys_back(n, _):
        cols = pl.ds(pl.multiple_of(n * half, half), half)
        d_k = contract_first(dscore[:, cols], qs[...]) * scale
        d_v = contract_first(probs[:, cols].astype(BF16), dmix[...])
        both = jnp.concatenate([d_k, d_v], axis=1).astype(BF16)
        kvp[n % 2, 0, n // 2] = both[0:S]
        kvp[n % 2, 1, n // 2] = both[S:]
        return 0

    lax.fori_loop(0, 4, keys_back, 0)
    for i in range(2):
        send(kp + i, kvp.at[i, 1 - core], kvp_core.at[i], partner)

    arrive(kp + (1 - y), kvp_core.at[1 - y])
    kvp_sum[...] = (kvp[1 - y, core].astype(F32) + kvp_core[1 - y].astype(F32)).astype(BF16)
    send(kp + 2, kvp_sum, kvp_chip, chip_of(1 - y, 2))
    kr = share4(block_all)
    weight_push(3)
    arrive(kp + y, kvp_core.at[y])
    arrive(kp + 2, kvp_chip)
    d_left = (
        kvp[y, core, 0].astype(F32) + kvp_core[y, 0].astype(F32) + kvp_chip[0].astype(F32)
    )
    kt = slots(1)
    ret_out[...] = d_left.astype(BF16)

    @pl.when(c > 0)
    def _():
        copy(kt, ret_out, ret_in, {"context": c - 1}).start()

    weight_push(4)
    weight_push(5)
    weight_push(6)

    @pl.when(c < C - 1)
    def _():
        arrive(kt, ret_in)

    @pl.when(c == C - 1)
    def _():
        ret_in[...] = jnp.zeros((S, 2 * HD), BF16)

    d_kv = (
        kvp[y, core, 1].astype(F32)
        + kvp_core[y, 1].astype(F32)
        + kvp_chip[1].astype(F32)
        + ret_in[...].astype(F32)
    )
    raw = jnp.concatenate([kv_raw[0, shard], kv_raw[1, shard]], axis=1).astype(F32)
    d_raw, gain_k = rms_backward(
        turn_back(d_kv[:, :HD], cosine[shard], sine[shard]), raw, rms_factor(raw), head_gain(1)
    )
    d_kv = jnp.concatenate([d_raw, d_kv[:, HD:]], axis=1).astype(BF16)
    for i in range(4):
        dkv_mine[i] = d_kv[:, i * LANES : (i + 1) * LANES]
    kq = slots(4)
    for i in range(1, 4):
        k = (t + i) % 4
        send(kq + i, dkv_mine.at[k], dkv_cols.at[t], {"tensor": k})
    dkv_cols[t] = dkv_mine[t]
    for i in range(1, 4):
        arrive(kq + i, dkv_cols.at[(t - i + 4) % 4])

    k4 = slots(2)

    def query_back(i, _):
        rows = pl.ds(pl.multiple_of(i * half, half), half)
        pair = pl.ds(i * 2, 2)
        part = contract_last(dq[rows], wa[:, q_cols])
        part = part + contract_last(dkv_cols[pair].reshape(half, LANES), wa[:, kv_part])
        part = part.astype(BF16)
        p4[i, 0] = part[0:S]
        p4[i, 1] = part[S:]
        copy(k4 + i, p4.at[i, 1 - core], p4_core.at[i], partner).start()
        return 0

    lax.fori_loop(0, 2, query_back, 0)

    def attn_grad(n, _):
        cols = pl.ds(pl.multiple_of(n * LANES, LANES), LANES)
        left = nrm[:, cols]
        ga[cols, HD : 2 * HD] = contract_first(left, dq[...]).astype(BF16)
        ga[cols, 2 * HD :] = contract_first(left, dkv_cols[...].reshape(T, LANES)).astype(BF16)
        return 0

    lax.fori_loop(0, D // LANES, attn_grad, 0)
    weight_send(8)
    weight_send(9)
    weight_push(7)
    kc = sum4(k4)
    meet4(kr, block_all)
    save_block = pltpu.make_async_copy(block_all, out_block, ls.at[3])
    save_block.start()
    d_normed = finish4(kc)
    copy(kc, p4_sum, p4_chip, chip_of(1 - y, 2)).wait_send()
    for i in range(2):
        copy(k4 + i, p4.at[i, 1 - core], p4_core.at[i], partner).wait_send()
    values = act[shard].astype(F32)
    d_input, gain_0 = rms_backward(d_normed, values, rms_factor(values), gain(0))
    input_all[y, core] = (dhid[...] + d_input).astype(BF16)
    gain_mine[0:1] = gain_0
    gain_mine[4:8] = jnp.zeros((4, D), F32)
    gain_mine[4:5, 0:HD] = gain_q
    gain_mine[5:6, 0:HD] = gain_k
    kn = slots(4 + 1 + C)
    for i in range(1, 4):
        send(kn + i, gain_mine, gain_tensor.at[i], {"tensor": (t + i) % 4})
    ki = share4(input_all)
    weight_push(8)
    total = gain_mine[...]
    for i in range(1, 4):
        arrive(kn + i, gain_tensor.at[i])
        total = total + gain_tensor[i]
    gain_tensor[0] = total
    send(kn, gain_tensor.at[0], gain_x.at[0], across)
    arrive(kn, gain_x.at[0])
    gain_x[1] = total + gain_x[0]
    for step in range(1, C):
        send(kn + 4 + step, gain_x.at[1], gain_z.at[step], along(step))
    weight_push(9)
    weight_meet(0, 1, 2)
    weight_end(2)
    meet4(ki, input_all)
    save_input = pltpu.make_async_copy(input_all, out_input, ls.at[4])
    save_input.start()
    weight_meet(3, 4)
    weight_end(0)
    weight_meet(5, 8)
    attn = ga[rows_of(f, c)].astype(F32)
    for step in range(1, C):
        attn = attn + ga_z[step - 1].astype(F32)
    kvg[t] = attn[:, 2 * HD :]
    kh = slots(4)
    for i in range(1, 4):
        send(kh + i, kvg.at[t], kvg.at[t], {"tensor": (t + i) % 4})
    st_out[...] = attn[:, 0:HD]
    st_query[...] = attn[:, HD : 2 * HD]
    staged = []

    def save(n, src, dst):
        staged.append(pltpu.make_async_copy(src, dst, ls.at[10 + n]))
        staged[-1].start()

    save(0, st_out, out_out)
    save(1, st_query, out_query)
    total = gain_x[1]
    for step in range(1, C):
        arrive(kn + 4 + step, gain_z.at[step])
        total = total + gain_z[step]
    owner = f * C + c
    moved = pltpu.roll(total, (D - owner * R) % D, 1)
    st_norm[...] = moved[0:4, 0:R]
    moved = pltpu.roll(total[:, 0:HD], (HD - owner * narrow) % HD, 1)
    st_head[...] = moved[4:6, 0:narrow]
    save(2, st_norm, out_norm)
    save(3, st_head, out_head)
    weight_meet(6, 7, 9)
    weight_end(1)
    for i in range(1, 4):
        arrive(kh + i, kvg.at[(t - i + 4) % 4])
    for k in range(4):
        st_kv[:, k * LANES : (k + 1) * LANES] = kvg[k]
    save(4, st_kv, out_kv)
    save_block.wait()
    save_input.wait()
    for moved in staged:
        moved.wait()
    settle()

    @pl.when(c < C - 1)
    def _():
        copy(ks, seg_row, seg_left, {"context": c + 1}).wait_send()
        copy(kk, kv.at[own_half], kv.at[my_half], {"context": c + 1}).wait_send()

    @pl.when(c > 0)
    def _():
        copy(kt, ret_out, ret_in, {"context": c - 1}).wait_send()
    assert counter[0] == SEMAPHORES, counter


def fused(
    mesh,
    activations,
    positions,
    seg_ids,
    norm_gains,
    head_gains,
    w_query,
    w_keyval,
    w_out,
    w_gateup,
    w_down,
    cotangent,
):
    C = mesh.shape["context"]
    T, D = activations.shape[1:]
    R, units = w_down.shape
    U = -(-units // (2 * LANES)) * LANES
    S = T // 4
    pack = -(-R // LANES) * LANES
    operands = (
        activations[0],
        positions,
        seg_ids,
        norm_gains,
        head_gains,
        w_gateup,
        w_down,
        cotangent[0],
        w_query,
        w_keyval,
        w_out,
    )
    scratch = [
        pltpu.VMEM((T, D), BF16),
        pltpu.VMEM(w_gateup.shape, BF16),
        pltpu.VMEM(w_down.shape, BF16),
        pltpu.VMEM((T, HD // 2), F32),
        pltpu.VMEM((T, HD // 2), F32),
        pltpu.VMEM((8, T), jnp.int32),
        pltpu.VMEM((T, 1), jnp.int32),
        pltpu.VMEM((8, pack), F32),
        pltpu.VMEM((2 * C, 8, pack), F32),
        pltpu.VMEM((2, 3, R, U), BF16),
        pltpu.VMEM((S, D), BF16),
        pltpu.VMEM((D, 2 * HD + LANES), BF16),
        pltpu.VMEM((3, D, U), BF16),
        pltpu.VMEM((8, T), jnp.int32),
        pltpu.VMEM((8, D), F32),
        pltpu.VMEM((8, HD), F32),
        pltpu.VMEM((T, D), BF16),
        pltpu.VMEM((T, HD), F32),
        pltpu.VMEM((4, T, LANES), BF16),
        pltpu.VMEM((T, HD), BF16),
        pltpu.VMEM((2 * T, 2 * HD), BF16),
        pltpu.VMEM((T, 2 * T), F32),
        pltpu.VMEM((T, HD), BF16),
        pltpu.VMEM((2, 2, S, D), BF16),
        pltpu.VMEM((2, S, D), BF16),
        pltpu.VMEM((S, D), BF16),
        pltpu.VMEM((S, D), BF16),
        pltpu.VMEM((S, D), F32),
        pltpu.VMEM((S, D), F32),
        pltpu.VMEM((4, 2, S, D), BF16),
        pltpu.VMEM((4, 2 * S, U), BF16),
        pltpu.VMEM((4, 2 * S, U), BF16),
        pltpu.VMEM((4, 2 * S, U), BF16),
        pltpu.VMEM((4, 2, S, D), BF16),
        pltpu.VMEM((4, S, D), BF16),
        pltpu.VMEM((3, S, D), BF16),
        pltpu.VMEM((3, S, D), BF16),
        pltpu.VMEM((4, 2, S, D), BF16),
        pltpu.VMEM((S, D), F32),
        pltpu.VMEM((2, 2, S, D), BF16),
        pltpu.VMEM((T, 2 * T), BF16),
        pltpu.VMEM((T, HD), BF16),
        pltpu.VMEM((T, HD), BF16),
        pltpu.VMEM((2, 2, 2, S, 2 * HD), BF16),
        pltpu.VMEM((2, 2, S, 2 * HD), BF16),
        pltpu.VMEM((2, S, 2 * HD), BF16),
        pltpu.VMEM((2, S, 2 * HD), BF16),
        pltpu.VMEM((S, 2 * HD), BF16),
        pltpu.VMEM((S, 2 * HD), BF16),
        pltpu.VMEM((4, S, LANES), BF16),
        pltpu.VMEM((4, S, LANES), BF16),
        pltpu.VMEM((3, C * R, U), BF16),
        pltpu.VMEM((C - 1, 3, R, U), BF16),
        pltpu.VMEM((D, 2 * HD + LANES), BF16),
        pltpu.VMEM((C * R, 2 * HD + LANES), BF16),
        pltpu.VMEM((C - 1, R, 2 * HD + LANES), BF16),
        pltpu.VMEM((4, R, LANES), F32),
        pltpu.VMEM((R, units), F32),
        pltpu.VMEM((8, D), F32),
        pltpu.VMEM((4, 8, D), F32),
        pltpu.VMEM((2, 8, D), F32),
        pltpu.VMEM((C, 8, D), F32),
        pltpu.VMEM((2, 2, S, D), BF16),
        pltpu.VMEM((2, 2, S, D), BF16),
        pltpu.VMEM((R, HD), F32),
        pltpu.VMEM((R, HD), F32),
        pltpu.VMEM(norm_gains.shape, F32),
        pltpu.VMEM(head_gains.shape, F32),
        pltpu.VMEM((R, 2 * HD), F32),
        pltpu.SemaphoreType.DMA((SEMAPHORES,)),
        pltpu.SemaphoreType.DMA((SEMAPHORES,)),
        pltpu.SemaphoreType.DMA((18,)),
    ]
    vmem = pl.BlockSpec(memory_space=pltpu.VMEM)
    anywhere = pl.BlockSpec(memory_space=pl.ANY)
    results = (
        jax.ShapeDtypeStruct((2, 2, S, D), BF16),
        jax.ShapeDtypeStruct((2, 2, S, D), BF16),
        jax.ShapeDtypeStruct(norm_gains.shape, F32),
        jax.ShapeDtypeStruct(head_gains.shape, F32),
        jax.ShapeDtypeStruct(w_query.shape, F32),
        jax.ShapeDtypeStruct(w_keyval.shape, F32),
        jax.ShapeDtypeStruct(w_out.shape, F32),
        jax.ShapeDtypeStruct(w_gateup.shape, F32),
        jax.ShapeDtypeStruct(w_down.shape, F32),
    )
    sizes = {"context": C, "tokens": T, "width": D, "rows": R, "units": U}
    parts = pl.pallas_call(
        functools.partial(fused_kernel, sizes),
        out_shape=results,
        in_specs=[anywhere] + [vmem] * 4 + [anywhere] * 6,
        out_specs=[anywhere] * len(results),
        scratch_shapes=scratch,
        compiler_params=pltpu.CompilerParams(
            collective_id=0, has_side_effects=True, vmem_limit_bytes=67043328
        ),
    )(*operands)
    count = len(parts)
    block_out, input_grad, *grads = pl.pallas_call(
        functools.partial(emit_kernel, count),
        out_shape=results,
        in_specs=[anywhere] * count,
        out_specs=[anywhere] * count,
        scratch_shapes=[pltpu.VMEM(part.shape, part.dtype) for part in parts]
        + [pltpu.SemaphoreType.DMA((count,))] * 2,
    )(*parts)
    return block_out.reshape(1, T, D), input_grad.reshape(1, T, D), *grads


def block(mesh, *arrays):
    tokens, rows = arrays[0].shape[1], arrays[9].shape[0]
    fits = (
        mesh.shape["fsdp"] == 2
        and mesh.shape["tensor"] == 4
        and mesh.shape["context"] == 4
        and tokens == WINDOW
        and rows % 16 == 0
        and arrays[5].shape[1] == HD
        and arrays[6].shape[1] == 4 * LANES
    )
    return fused(mesh, *arrays) if fits else shards(*arrays)


def shards(
    activations,
    positions,
    seg_ids,
    norm_gains,
    head_gains,
    w_query,
    w_keyval,
    w_out,
    w_gateup,
    w_down,
    cotangent,
):
    tokens = activations.shape[1]
    local_heads = w_query.shape[1] // HD
    inputs = activations[0].astype(jnp.float32)
    places = positions[0]
    documents = seg_ids[0]
    gains_all, heads_all, query_all, keyval_all, out_all = (
        lax.all_gather(norm_gains, ("fsdp", "context"), axis=1, tiled=True),
        lax.all_gather(head_gains, ("fsdp", "context"), axis=1, tiled=True),
        lax.all_gather(w_query, ("fsdp", "context"), axis=0, tiled=True),
        lax.all_gather(w_keyval, ("fsdp", "context"), axis=0, tiled=True),
        lax.all_gather(w_out, ("fsdp", "context"), axis=0, tiled=True),
    )
    gains_f = gains_all.astype(jnp.float32)
    heads_f = heads_all.astype(jnp.float32)
    normed_f, input_back = jax.vjp(rms_norm, inputs, gains_f[0])
    normed = normed_f.astype(jnp.bfloat16)
    query_raw = jnp.dot(normed, query_all, preferred_element_type=jnp.float32).reshape(
        tokens, local_heads, HD
    )
    keyval_raw = jnp.dot(normed, keyval_all, preferred_element_type=jnp.float32)

    def prepare(raw_heads, head_gain):
        return rotate(rms_norm(raw_heads, head_gain), places)

    query_rot, query_back = jax.vjp(prepare, query_raw, heads_f[0])
    key_rot, key_back = jax.vjp(prepare, keyval_raw[:, None, :HD], heads_f[1])
    queries = query_rot.astype(jnp.bfloat16)
    own_keyval = jnp.concatenate([key_rot[:, 0], keyval_raw[:, HD:]], axis=1).astype(jnp.bfloat16)
    labels = jnp.stack([places, documents])
    keep_from = tokens - tokens
    left_keyval, left_labels = from_behind((own_keyval, labels), "context", 1)
    keys_all = jnp.concatenate([left_keyval, own_keyval], axis=0)
    key_places = jnp.concatenate([left_labels[0], places])
    key_documents = jnp.concatenate([left_labels[1], documents])
    has_left = lax.axis_index("context") > 0
    key_live = jnp.concatenate([jnp.full((tokens,), has_left), jnp.ones((tokens,), dtype=bool)])
    scale_factor = HD ** (-0.5)
    block_rows = 512
    block_starts = jnp.arange(tokens // block_rows) * block_rows

    def block_scores():
        spacing = places[:, None] - key_places[None, :]
        visible = (
            key_live[None, :]
            & (documents[:, None] == key_documents[None, :])
            & (spacing >= 0)
            & (spacing < WINDOW)
        )
        raw_scores = (
            jnp.einsum("qhd,kd->hqk", queries, keys_all[:, :HD], preferred_element_type=jnp.float32)
            * scale_factor
        )
        return (jnp.where(visible[None], raw_scores, -1e30), keys_all, queries)

    def forward_block(start):
        scores, near_keyval, query_block = block_scores()
        row_top = jnp.max(scores, axis=-1, keepdims=True)
        raised = jnp.exp(scores - row_top)
        row_total = jnp.sum(raised, axis=-1, keepdims=True)
        probs = raised / row_total
        mixed_block = jnp.einsum(
            "hqk,kd->qhd",
            probs.astype(jnp.bfloat16),
            near_keyval[:, HD:],
            preferred_element_type=jnp.float32,
        )
        return (mixed_block.astype(jnp.bfloat16), row_top + jnp.log(row_total))

    mixed_blocks, log_blocks = lax.map(forward_block, block_starts)
    mixed_low = mixed_blocks.reshape(tokens, local_heads * HD)
    branch = lax.psum(contract_last(mixed_low, out_all).astype(jnp.bfloat16), "tensor").astype(jnp.float32)
    post_attn, post_attn_back = jax.vjp(rms_norm, branch, gains_f[1])
    hidden = inputs + post_attn
    normed_mlp_f, pre_mlp_back = jax.vjp(rms_norm, hidden, gains_f[2])
    normed_mlp = normed_mlp_f.astype(jnp.bfloat16)
    columns = normed_mlp
    gate_up = jnp.einsum(
        "bn,nkf->bkf",
        columns,
        lax.all_gather(w_gateup, ("fsdp", "context"), axis=0, tiled=True),
        preferred_element_type=jnp.float32,
    )
    active_f, glu_back = jax.vjp(glu, gate_up)
    active = active_f.astype(jnp.bfloat16)
    down = lax.psum(
        contract_last(
            active, lax.all_gather(w_down, ("fsdp", "context"), axis=0, tiled=True)
        ).astype(jnp.bfloat16),
        "tensor",
    ).astype(jnp.float32)
    post_mlp, post_mlp_back = jax.vjp(rms_norm, down, gains_f[3])
    result = hidden + post_mlp
    grad_out = cotangent[0].astype(jnp.float32)
    d_down, gain_post_mlp = post_mlp_back(grad_out)
    down_low = d_down.astype(jnp.bfloat16)
    columns = down_low
    d_active = jnp.dot(
        columns,
        lax.all_gather(w_down, ("fsdp", "context"), axis=0, tiled=True),
        preferred_element_type=jnp.float32,
    )
    d_gate_up = glu_back(d_active)[0].astype(jnp.bfloat16)
    d_normed_part = jnp.einsum(
        "bkf,nkf->bn",
        d_gate_up,
        lax.all_gather(w_gateup, ("fsdp", "context"), axis=0, tiled=True),
        preferred_element_type=jnp.float32,
    )
    d_normed_mlp = lax.psum(d_normed_part.astype(jnp.bfloat16), "tensor").astype(jnp.float32)
    d_hidden_norm, gain_pre_mlp = pre_mlp_back(d_normed_mlp)
    d_hidden = grad_out + d_hidden_norm
    features = normed_mlp
    grad_cols = down_low
    gate_up_term = jnp.einsum(
        "bn,bkf->nkf", features, d_gate_up, preferred_element_type=jnp.float32
    )
    down_term = contract_first(grad_cols, active)
    scatter = lambda part: lax.psum_scatter(
        part.astype(jnp.bfloat16), ("fsdp", "context"), scatter_dimension=0, tiled=True
    ).astype(jnp.float32)
    gate_grad = scatter(gate_up_term[:, 0])
    up_grad = scatter(gate_up_term[:, 1])
    down_grad = scatter(down_term)
    d_branch, gain_post_attn = post_attn_back(d_hidden)
    branch_low = d_branch.astype(jnp.bfloat16)
    d_mixed = jnp.dot(branch_low, out_all, preferred_element_type=jnp.float32)
    d_mixed_low = d_mixed.astype(jnp.bfloat16).reshape(tokens, local_heads, HD)

    def backward_block(carry, item):
        start, log_block = item
        scores, near_keyval, query_block = block_scores()
        probs_again = jnp.exp(scores - log_block)
        d_probs = jnp.einsum(
            "qhd,kd->hqk", d_mixed_low, near_keyval[:, HD:], preferred_element_type=jnp.float32
        )
        row_inner = jnp.sum(probs_again * d_probs, axis=-1, keepdims=True)
        d_scores = (probs_again * (d_probs - row_inner)).astype(jnp.bfloat16)
        d_query_block = (
            jnp.einsum(
                "hqk,kd->qhd", d_scores, near_keyval[:, :HD], preferred_element_type=jnp.float32
            )
            * scale_factor
        )
        d_keys = (
            jnp.einsum("hqk,qhd->kd", d_scores, query_block, preferred_element_type=jnp.float32)
            * scale_factor
        )
        d_values = jnp.einsum(
            "hqk,qhd->kd",
            probs_again.astype(jnp.bfloat16),
            d_mixed_low,
            preferred_element_type=jnp.float32,
        )
        updated = carry + jnp.concatenate([d_keys, d_values], axis=1)
        return (updated, d_query_block)

    d_keyval, d_query_blocks = lax.scan(
        backward_block,
        jnp.zeros((tokens + tokens, 2 * HD), jnp.float32),
        (block_starts, log_blocks),
    )
    d_queries = d_query_blocks.reshape(tokens, local_heads, HD)
    returned = from_behind(d_keyval[:tokens].astype(jnp.bfloat16), "context", -1).astype(
        jnp.float32
    )
    own_grad = d_keyval[tokens:].at[keep_from:].add(returned)
    d_query_raw, gain_query = query_back(d_queries)
    d_query_low = d_query_raw.reshape(tokens, local_heads * HD).astype(jnp.bfloat16)
    d_normed_query, keyval_grad, gain_query_all = (
        lax.psum(contract_last(d_query_low, query_all).astype(jnp.bfloat16), "tensor").astype(
            jnp.float32
        ),
        lax.psum(own_grad.astype(jnp.bfloat16), "tensor").astype(jnp.float32),
        lax.psum(gain_query.astype(jnp.bfloat16), "tensor").astype(jnp.float32),
    )
    d_key_raw, gain_key = key_back(keyval_grad[:, None, :HD])
    d_keyval_low = jnp.concatenate([d_key_raw[:, 0], keyval_grad[:, HD:]], axis=1).astype(
        jnp.bfloat16
    )
    d_normed = d_normed_query + contract_last(d_keyval_low, keyval_all)
    d_input_norm, gain_input = input_back(d_normed)
    input_total = d_hidden + d_input_norm
    features = normed
    grad_cols = branch_low
    attn_grads = lax.psum_scatter(
        jnp.stack(
            [contract_first(features, d_query_low), contract_first(grad_cols, mixed_low)], axis=1
        ).astype(jnp.bfloat16),
        ("fsdp", "context"),
        scatter_dimension=0,
        tiled=True,
    ).astype(jnp.float32)
    keyval_term = contract_first(normed, d_keyval_low)
    gain_terms = jnp.stack([gain_input, gain_post_attn, gain_pre_mlp, gain_post_mlp])
    head_terms = jnp.stack([gain_query_all, gain_key])
    gain_grad, head_grad, keyval_weight_grad = (
        lax.psum_scatter(
            gain_terms.astype(jnp.bfloat16), ("fsdp", "context"), scatter_dimension=1, tiled=True
        ).astype(jnp.float32),
        lax.psum_scatter(
            head_terms.astype(jnp.bfloat16), ("fsdp", "context"), scatter_dimension=1, tiled=True
        ).astype(jnp.float32),
        lax.psum_scatter(
            keyval_term.astype(jnp.bfloat16), ("fsdp", "context"), scatter_dimension=0, tiled=True
        ).astype(jnp.float32),
    )
    return (
        result[None].astype(jnp.bfloat16),
        input_total[None].astype(jnp.bfloat16),
        gain_grad,
        head_grad,
        attn_grads[:, 0],
        keyval_weight_grad,
        attn_grads[:, 1],
        jnp.stack([gate_grad, up_grad], axis=1),
        down_grad,
    )


def solution(mesh):
    return jax.shard_map(
        functools.partial(block, mesh),
        mesh=mesh,
        in_specs=(
            P("fsdp", "context", None),
            P("fsdp", "context"),
            P("fsdp", "context"),
            P(None, ("fsdp", "context")),
            P(None, ("fsdp", "context")),
            P(("fsdp", "context"), "tensor"),
            P(("fsdp", "context"), None),
            P(("fsdp", "context"), "tensor"),
            P(("fsdp", "context"), None, "tensor"),
            P(("fsdp", "context"), "tensor"),
            P("fsdp", "context", None),
        ),
        out_specs=(
            P("fsdp", "context", None),
            P("fsdp", "context", None),
            P(None, ("fsdp", "context")),
            P(None, ("fsdp", "context")),
            P(("fsdp", "context"), "tensor"),
            P(("fsdp", "context"), None),
            P(("fsdp", "context"), "tensor"),
            P(("fsdp", "context"), None, "tensor"),
            P(("fsdp", "context"), "tensor"),
        ),
        check_vma=False,
    )
```

```python
import functools
import math

import jax
import jax.numpy as jnp
from jax import lax
from jax.experimental import pallas as pl
from jax.experimental.pallas import tpu as pltpu
from jax.sharding import PartitionSpec as P

HD = 256
WINDOW = 512


EPSILON = 1e-06


def from_behind(block, axis, distance):
    devices = range(lax.axis_size(axis))
    route = [(i - distance, i) for i in devices if i - distance in devices]
    return lax.ppermute(block, axis, route)


def rms_norm(values, gain):
    factor = lax.rsqrt(jnp.mean(values * values, axis=-1, keepdims=True) + EPSILON)
    return values * factor * gain


def rotate(tensor, places):
    width_all = tensor.shape[-1]
    half_width = width_all // 2
    freqs = jnp.power(10000.0, -jnp.arange(half_width, dtype=jnp.float32) * 2.0 / width_all)
    angles = places.astype(jnp.float32)[:, None] * freqs[None, :]
    cosine = jnp.cos(angles)[:, None, :]
    sine = jnp.sin(angles)[:, None, :]
    first_half = tensor[..., :half_width]
    second_half = tensor[..., half_width:]
    return jnp.concatenate(
        [first_half * cosine - second_half * sine, second_half * cosine + first_half * sine],
        axis=-1,
    )


def glu(gate_up):
    return jax.nn.gelu(gate_up[:, 0], approximate=True) * gate_up[:, 1]


def contract_last(left_side, right_side):
    return lax.dot_general(
        left_side, right_side, (((1,), (1,)), ((), ())), preferred_element_type=jnp.float32
    )


def contract_first(left_side, right_side):
    return lax.dot_general(
        left_side, right_side, (((0,), (0,)), ((), ())), preferred_element_type=jnp.float32
    )


MESH = pl.DeviceIdType.MESH
F32 = jnp.float32
BF16 = jnp.bfloat16
LANES = 128
SEMAPHORES = 178


def mm(left, right):
    return jnp.dot(left, right, preferred_element_type=F32)


def rms_factor(values):
    return lax.rsqrt(jnp.mean(values * values, axis=-1, keepdims=True) + EPSILON)


def rms_backward(grad, values, factor, gain):
    unit = values * factor
    scaled = grad * gain
    inner = jnp.mean(scaled * unit, axis=-1, keepdims=True)
    return factor * (scaled - unit * inner), jnp.sum(grad * unit, axis=0, keepdims=True)


def turn(values, cosine, sine):
    half = values.shape[-1] // 2
    first, second = values[:, :half], values[:, half:]
    return jnp.concatenate([first * cosine - second * sine, second * cosine + first * sine], axis=1)


def turn_back(values, cosine, sine):
    half = values.shape[-1] // 2
    first, second = values[:, :half], values[:, half:]
    return jnp.concatenate([first * cosine + second * sine, second * cosine - first * sine], axis=1)


def emit_kernel(count, *refs):
    sources, results, held = refs[:count], refs[count : 2 * count], refs[2 * count : 3 * count]
    incoming, outgoing = refs[3 * count :]
    reads = [pltpu.make_async_copy(sources[n], held[n], incoming.at[n]) for n in range(count)]
    writes = [pltpu.make_async_copy(held[n], results[n], outgoing.at[n]) for n in range(count)]
    for moved in reads:
        moved.start()
    for n in range(count):
        reads[n].wait()
        writes[n].start()
    for moved in writes:
        moved.wait()


def fused_kernel(
    sizes,
    act_all,
    positions,
    seg_ids,
    norm_gains,
    head_gains,
    gateup_all,
    down_all,
    cot_all,
    w_query,
    w_keyval,
    w_out,
    out_block,
    out_input,
    out_norm,
    out_head,
    out_query,
    out_kv,
    out_out,
    out_gateup,
    out_down,
    act,
    w_gateup,
    w_down,
    cosine,
    sine,
    seg_row,
    seg_col,
    gain_pack,
    gain_all,
    w_ff,
    cot,
    wa,
    wf,
    seg_left,
    gain_rows,
    head_rows,
    nrm,
    qraw,
    kv_raw,
    qs,
    kv,
    probs,
    mix,
    p4,
    p4_core,
    p4_sum,
    p4_chip,
    hid,
    bran,
    xg,
    gel,
    upg,
    active,
    p8,
    p8_core,
    p8_sum,
    p8_chip,
    dd,
    dhid,
    db,
    dscore,
    dmix,
    dq,
    kvp,
    kvp_core,
    kvp_sum,
    kvp_chip,
    ret_out,
    ret_in,
    dkv_mine,
    dkv_cols,
    gall_x,
    gall_z,
    ga,
    ga_x,
    ga_z,
    kvg,
    ff_stage,
    gain_mine,
    gain_tensor,
    gain_x,
    gain_z,
    block_all,
    input_all,
    st_out,
    st_query,
    st_norm,
    st_head,
    st_kv,
    ss,
    rs,
    ls,
):
    C = sizes["context"]
    T, D, R, U = sizes["tokens"], sizes["width"], sizes["rows"], sizes["units"]
    units = w_down.shape[1]
    narrow = HD // (2 * C)
    S = T // 4
    f = lax.axis_index("fsdp")
    c = lax.axis_index("context")
    t = lax.axis_index("tensor")
    y, core = t // 2, t % 2
    m = c % 2
    base = c - m
    partner = {"tensor": y * 2 + (1 - core)}
    across = {"fsdp": 1 - f}
    counter = [0]
    sent = []

    def slots(count):
        first = counter[0]
        counter[0] += count
        assert counter[0] <= SEMAPHORES
        return first

    def copy(k, src, dst, device):
        return pltpu.make_async_remote_copy(
            src_ref=src,
            dst_ref=dst,
            send_sem=ss.at[k],
            recv_sem=rs.at[k],
            device_id=device,
            device_id_type=MESH,
        )

    def send(k, src, dst, device):
        moved = copy(k, src, dst, device)
        moved.start()
        sent.append(moved)

    def arrive(k, dst):
        copy(k, dst, dst, partner).wait_recv()

    def settle():
        for moved in sent:
            moved.wait_send()
        sent.clear()

    def along(step):
        return {"context": (c + step) % C}

    def rows_of(ff, cc):
        return pl.ds(pl.multiple_of((ff * C + cc) * R, R), R)

    def chip_of(k, count):
        if count == 2:
            return {"tensor": k * 2 + core}
        return {"context": base + k // 2, "tensor": (k % 2) * 2 + core}

    loads = [
        pltpu.make_async_copy(src, dst, ls.at[15 + n])
        for n, (src, dst) in enumerate(
            ((gateup_all, w_gateup), (down_all, w_down), (act_all, act))
        )
    ]
    for moved in loads:
        moved.start()

    barrier = pltpu.get_barrier_semaphore()
    greeted = [along(step) for step in range(1, C)] + [across]
    greeted += [{"tensor": (t + step) % 4} for step in range(1, 4)]
    greeted += [{"context": base + 1 - m, "tensor": (1 - y) * 2 + core}]
    for device in greeted:
        pl.semaphore_signal(barrier, inc=1, device_id=device, device_id_type=MESH)
    gain_pack[...] = jnp.zeros(gain_pack.shape, F32)
    gain_pack[0:4, 0:R] = norm_gains[...].astype(F32)
    gain_pack[4:6, 0:narrow] = head_gains[...].astype(F32)
    seg_row[...] = jnp.broadcast_to(seg_ids[...], seg_row.shape)
    pl.semaphore_wait(barrier, len(greeted))

    mine = rows_of(f, c)
    kv_cols = pl.ds(pl.multiple_of(t * LANES, LANES), LANES)
    attn_parts = (
        (w_query, slice(0, HD)),
        (w_keyval.at[:, kv_cols], slice(HD, HD + LANES)),
        (w_out, slice(HD + LANES, 2 * HD + LANES)),
    )
    q_cols, kv_part, o_cols = (cols for _, cols in attn_parts[:3])
    local = []
    for n, (part, cols) in enumerate(attn_parts):
        local.append(pltpu.make_async_copy(part, wa.at[mine, cols], ls.at[6 + n]))
        local[-1].start()
    ka = slots(3 * C)
    kar = slots(C - 1)
    kg = slots(2 * C - 1)
    for step in range(1, C):
        for n, (part, cols) in enumerate(attn_parts):
            send(ka + 3 * step + n, part, wa.at[mine, cols], along(step))
    for n, (part, cols) in enumerate(attn_parts):
        send(ka + n, part, wa.at[mine, cols], across)
    own_gain = gain_all.at[f * C + c]
    gain_all[f * C + c] = gain_pack[...]
    for step in range(1, C):
        send(kg + step, gain_pack, own_gain, along(step))
    send(kg, gain_pack, own_gain, across)
    ks = slots(1)

    @pl.when(c < C - 1)
    def _():
        copy(ks, seg_row, seg_left, {"context": c + 1}).start()

    pieces = ((0, 0, 384), (0, 384, U), (1, 0, 512), (1, 512, U), (2, 0, 512), (2, 512, U))
    kf = slots((2 * C - 1) * len(pieces))

    def piece(p, rows):
        w, low, high = pieces[p]
        return wf.at[w, rows, low:high]

    side = c // 2
    near, far = 2 - side, 3 * (1 - side)

    def send_ff(p):
        k = kf + (2 * C - 1) * p
        w, low, high = pieces[p]
        turns = tuple((c + step) % C for step in range(1, C))
        for to in (base + 1 - m, near, far) if p in (3, 4) else turns:
            send(
                k + (to - c + C) % C,
                w_ff.at[to % 2, w, :, low:high],
                piece(p, mine),
                {"context": to},
            )
        send(k, w_ff.at[m, w, :, low:high], piece(p, mine), across)

    def relay_ff(p):
        k = kf + (2 * C - 1) * p
        for source in (base + 1 - m, near, far):
            step = (c - source + C) % C
            part = piece(p, rows_of(f, source))
            arrive(k + step, part)
            send(k + C - 1 + step, part, part, across)

    def meet_ff(p):
        k = kf + (2 * C - 1) * p
        arrive(k, piece(p, rows_of(1 - f, c)))
        for step in range(1, C):
            arrive(k + C - 1 + step, piece(p, rows_of(1 - f, (c - step + C) % C)))

    for moved in loads:
        moved.wait()
    for w in range(3):
        whole = w_down[...] if w == 2 else w_gateup[:, w, :]
        w_ff[0, w] = whole[:, 0:U]
        w_ff[1, w, :, 0 : units - U] = whole[:, U:units]
        w_ff[1, w, :, units - U :] = jnp.zeros((R, 2 * U - units), BF16)
    seg_col[...] = jnp.transpose(seg_row[...].astype(F32))[:, 0:1].astype(jnp.int32)
    place = jnp.broadcast_to(positions[...].astype(F32), (8, T))
    index = lax.broadcasted_iota(jnp.int32, (1, HD // 2), 1).astype(F32)
    angle = jnp.transpose(place)[:, 0:1] * jnp.exp(index * (-2.0 * math.log(10000.0) / HD))
    cosine[...] = jnp.cos(angle)
    sine[...] = jnp.sin(angle)
    shard = pl.ds(pl.multiple_of(t * S, S), S)
    own_cot = pltpu.make_async_copy(cot_all.at[shard], cot, ls.at[2])
    own_cot.start()
    own_ff = pltpu.make_async_copy(w_ff.at[m], wf.at[:, mine], ls.at[1])
    own_ff.start()
    for step in range(1, C):
        other = rows_of(f, (c - step + C) % C)
        for n, (_, cols) in enumerate(attn_parts):
            arrive(ka + 3 * step + n, wa.at[other, cols])
        send(kar + step - 1, wa.at[other], wa.at[other], across)
        part = gain_all.at[f * C + (c - step + C) % C]
        arrive(kg + step, part)
        send(kg + C - 1 + step, part, part, across)
    for moved in local:
        moved.wait()
    send_ff(0)
    for n, (_, cols) in enumerate(attn_parts):
        arrive(ka + n, wa.at[rows_of(1 - f, c), cols])
    for step in range(1, C):
        arrive(kar + step - 1, wa.at[rows_of(1 - f, (c - step + C) % C)])

    @pl.when(c > 0)
    def _():
        arrive(ks, seg_left)

    @pl.when(c == 0)
    def _():
        seg_left[...] = jnp.full(seg_left.shape, -1, jnp.int32)
        kv[0:T] = jnp.zeros((T, 2 * HD), BF16)

    arrive(kg, gain_all.at[(1 - f) * C + c])
    for step in range(1, C):
        arrive(kg + C - 1 + step, gain_all.at[(1 - f) * C + (c - step + C) % C])
    wide = jnp.zeros((8, D), F32)
    heads = jnp.zeros((8, HD), F32)
    blank = jnp.zeros((8, D - gain_pack.shape[1]), F32)
    for j in range(2 * C):
        part = gain_all[j]
        wide = wide + pltpu.roll(jnp.concatenate([part, blank], axis=1), j * R, 1)
        heads = heads + pltpu.roll(part[:, 0:HD], j * narrow, 1)
    gain_rows[...] = wide
    head_rows[...] = heads

    def gain(index):
        return gain_rows[index : index + 1]

    def head_gain(index):
        return head_rows[4 + index : 5 + index]

    half = T // 2

    def project(i, _):
        rows = pl.ds(pl.multiple_of(i * half, half), half)
        values = act[rows].astype(F32)
        low = (values * rms_factor(values) * gain(0)).astype(BF16)
        nrm[rows] = low
        kv_raw[t, rows] = mm(low, wa[:, kv_part]).astype(BF16)
        return 0

    lax.fori_loop(0, 2, project, 0)
    ku = slots(4)
    for i in range(1, 4):
        send(ku + i, kv_raw.at[t], kv_raw.at[t], {"tensor": (t + i) % 4})

    def query(i, _):
        rows = pl.ds(pl.multiple_of(i * half, half), half)
        raw_q = mm(nrm[rows], wa[:, q_cols])
        qraw[rows] = raw_q
        qs[rows] = turn(
            raw_q * rms_factor(raw_q) * head_gain(0), cosine[rows], sine[rows]
        ).astype(BF16)
        return 0

    lax.fori_loop(0, 2, query, 0)
    for i in range(1, 4):
        arrive(ku + i, kv_raw.at[(t - i + 4) % 4])

    def key(i, _):
        rows = pl.ds(pl.multiple_of(i * half, half), half)
        raw_k = jnp.concatenate([kv_raw[0, rows], kv_raw[1, rows]], axis=1).astype(F32)
        own = pl.ds(pl.multiple_of(T + i * half, half), half)
        kv[own, 0:HD] = turn(
            raw_k * rms_factor(raw_k) * head_gain(1), cosine[rows], sine[rows]
        ).astype(BF16)
        kv[own, HD : HD + LANES] = kv_raw[2, rows]
        kv[own, HD + LANES :] = kv_raw[3, rows]
        return 0

    lax.fori_loop(0, 2, key, 0)
    kk = slots(2)
    my_half = pl.ds(pl.multiple_of(core * half, half), half)
    other_half = pl.ds(pl.multiple_of((1 - core) * half, half), half)
    own_half = pl.ds(pl.multiple_of(T + core * half, half), half)

    @pl.when(c < C - 1)
    def _():
        copy(kk, kv.at[own_half], kv.at[my_half], {"context": c + 1}).start()

    send_ff(1)
    send_ff(2)
    relay_ff(0)

    @pl.when(c > 0)
    def _():
        arrive(kk, kv.at[my_half])
        moved = copy(kk + 1, kv.at[my_half], kv.at[my_half], partner)
        moved.start()
        arrive(kk + 1, kv.at[other_half])
        moved.wait_send()

    scale = HD**-0.5
    no_left = jnp.where(c > 0, 0, 2 * T)
    k4 = slots(2)

    def attend(i, _):
        rows = pl.ds(pl.multiple_of(i * half, half), half)
        q = qs[rows]
        labels = seg_col[rows]
        row = lax.broadcasted_iota(jnp.int32, (half, T), 0) + i * half
        col = lax.broadcasted_iota(jnp.int32, (half, T), 1)
        left = contract_last(q, kv[0:T, 0:HD]) * scale
        left = jnp.where((labels == seg_left[0:1]) & (col > row + no_left), left, -1e30)
        own = contract_last(q, kv[T:, 0:HD]) * scale
        own = jnp.where((labels == seg_row[0:1]) & (col <= row), own, -1e30)
        top = jnp.maximum(
            jnp.max(left, axis=1, keepdims=True), jnp.max(own, axis=1, keepdims=True)
        )
        left, own = jnp.exp(left - top), jnp.exp(own - top)
        total = jnp.sum(left, axis=1, keepdims=True) + jnp.sum(own, axis=1, keepdims=True)
        left, own = left / total, own / total
        probs[rows, 0:T] = left
        probs[rows, T:] = own
        mixed = mm(left.astype(BF16), kv[0:T, HD:]) + mm(own.astype(BF16), kv[T:, HD:])
        mixed = mixed.astype(BF16)
        mix[rows] = mixed
        part = contract_last(mixed, wa[:, o_cols]).astype(BF16)
        p4[i, 0] = part[0:S]
        p4[i, 1] = part[S:]
        copy(k4 + i, p4.at[i, 1 - core], p4_core.at[i], partner).start()
        return 0

    lax.fori_loop(0, 2, attend, 0)

    def sum4(k):
        kc = slots(1)
        arrive(k + (1 - y), p4_core.at[1 - y])
        p4_sum[...] = (
            p4[1 - y, core].astype(F32) + p4_core[1 - y].astype(F32)
        ).astype(BF16)
        copy(kc, p4_sum, p4_chip, chip_of(1 - y, 2)).start()
        arrive(k + y, p4_core.at[y])
        return kc

    def finish4(kc):
        arrive(kc, p4_chip)
        return (
            p4[y, core].astype(F32)
            + p4_core[y].astype(F32)
            + p4_chip[...].astype(F32)
        )

    kc = sum4(k4)
    relay_ff(1)
    branch = finish4(kc)
    copy(kc, p4_sum, p4_chip, chip_of(1 - y, 2)).wait_send()
    for i in range(2):
        copy(k4 + i, p4.at[i, 1 - core], p4_core.at[i], partner).wait_send()

    bran[...] = branch
    hidden = act[shard].astype(F32) + branch * rms_factor(branch) * gain(1)
    hid[...] = hidden
    low = (hidden * rms_factor(hidden) * gain(2)).astype(BF16)

    me = m * 2 + y

    def gather8(full, value):
        kg = slots(8)
        full[me, core] = value
        send(kg + 4, full.at[me, core], full.at[me, core], partner)
        for i in range(1, 4):
            send(kg + i, full.at[me, core], full.at[me, core], chip_of((me + i) % 4, 4))
        return kg

    def pass8(kg, full, i):
        k = (me - i + 4) % 4
        arrive(kg + i, full.at[k, core])
        copy(kg + 4 + i, full.at[k, core], full.at[k, core], partner).start()

    def meet8(kg, full, i):
        k = (me - i + 4) % 4
        arrive(kg + 4 + i, full.at[k, 1 - core])

    def settle8(kg, full):
        for i in range(1, 4):
            k = (me - i + 4) % 4
            copy(kg + 4 + i, full.at[k, core], full.at[k, core], partner).wait_send()

    def give8(ko, i):
        k = (me - i + 4) % 4
        copy(ko + i, p8.at[k, 1 - core], p8_core.at[i], partner).start()

    def push8(ko, i):
        k = (me - i + 4) % 4
        arrive(ko + i, p8_core.at[i])
        p8_sum[i - 1] = (
            p8[k, core].astype(F32) + p8_core[i].astype(F32)
        ).astype(BF16)
        copy(ko + 4 + i, p8_sum.at[i - 1], p8_chip.at[i - 1], chip_of(k, 4)).start()

    def finish8(ko):
        arrive(ko, p8_core.at[0])
        total = p8[me, core].astype(F32) + p8_core[0].astype(F32)
        for i in range(1, 4):
            arrive(ko + 4 + i, p8_chip.at[i - 1])
            total = total + p8_chip[i - 1].astype(F32)
        for i in range(4):
            copy(ko + i, p8.at[0, 1 - core], p8_core.at[i], partner).wait_send()
        for i in range(1, 4):
            copy(ko + 4 + i, p8_sum.at[0], p8_chip.at[0], partner).wait_send()
        return total

    kx = slots(7)
    beside, beyond = m * 2 + 1 - y, (1 - m) * 2 + y
    corner = (1 - m) * 2 + 1 - y
    xg[me, core] = low
    send(kx + 2, xg.at[me, core], xg.at[me, core], chip_of(beyond, 4))
    send(kx + 1, xg.at[me, core], xg.at[me, core], chip_of(beside, 4))
    send(kx, xg.at[me, core], xg.at[me, core], partner)
    send_ff(3)
    send_ff(4)
    relay_ff(2)
    send_ff(5)
    relay_ff(3)
    for i, k in ((1, beside), (2, beyond), (3, corner)):
        part = xg.at[k, core]
        arrive(kx + i, part)
        if i == 2:
            send(kx + 3, part, part, chip_of(beside, 4))
        send(kx + 3 + i, part, part, partner)
    relay_ff(4)
    own_ff.wait()
    own_cot.wait()
    for p in range(4):
        meet_ff(p)
    arrive(kx, xg.at[me, 1 - core])
    for i, k in ((1, beside), (2, beyond), (3, corner)):
        arrive(kx + 3 + i, xg.at[k, 1 - core])
    root = 0.7978845608028654
    ko = slots(8)

    def forward(i, _):
        k = (me - i + 4) % 4
        x = xg[k].reshape(2 * S, D)
        gate = mm(x, wf[0])
        up = mm(x, wf[1])
        square = gate * gate
        bent = jnp.tanh(root * gate * (1.0 + 0.044715 * square))
        ramp = 0.5 * (1.0 + bent)
        gelu = gate * ramp
        slope = ramp + 0.5 * gate * (1.0 - bent * bent) * root * (1.0 + 3 * 0.044715 * square)
        gel[k] = gelu.astype(BF16)
        upg[k] = (up * slope).astype(BF16)
        active[k] = (gelu * up).astype(BF16)
        return 0

    lax.fori_loop(0, 3, forward, 0)
    relay_ff(5)
    lax.fori_loop(3, 4, forward, 0)
    meet_ff(4)
    meet_ff(5)

    def lower(i, _):
        k = (me - i + 4) % 4
        p8[k] = contract_last(active[k], wf[2]).astype(BF16).reshape(2, S, D)
        give8(ko, i)

        @pl.when(i > 1)
        def _():
            push8(ko, i - 1)

        return 0

    lax.fori_loop(0, 4, lower, 0)
    push8(ko, 3)
    down = finish8(ko)

    factor = rms_factor(down)
    grad = cot[...].astype(F32)
    result = (hid[...] + down * factor * gain(3)).astype(BF16)
    d_down, gain_3 = rms_backward(grad, down, factor, gain(3))
    gain_mine[3:4] = gain_3
    kd = gather8(dd, d_down.astype(BF16))

    def share4(full):
        kb = slots(3)
        send(kb, full.at[y, core], full.at[y, core], chip_of(1 - y, 2))
        send(kb + 1, full.at[y, core], full.at[y, core], partner)
        return kb

    def meet4(kb, full):
        arrive(kb, full.at[1 - y, core])
        send(kb + 2, full.at[1 - y, core], full.at[1 - y, core], partner)
        arrive(kb + 1, full.at[y, 1 - core])
        arrive(kb + 2, full.at[1 - y, 1 - core])

    block_all[y, core] = result
    ko2 = slots(8)

    def backward(i, _):
        k = (me - i + 4) % 4
        meet8(kd, dd, i)
        low = dd[k].reshape(2 * S, D)
        d_active = mm(low, wf[2])

        @pl.when(i < 3)
        def _():
            pass8(kd, dd, i + 1)

        d_gate = (d_active * upg[k].astype(F32)).astype(BF16)
        d_up = (d_active * gel[k].astype(F32)).astype(BF16)
        upg[k] = d_gate
        gel[k] = d_up
        p8[k] = (
            (contract_last(d_gate, wf[0]) + contract_last(d_up, wf[1]))
            .astype(BF16)
            .reshape(2, S, D)
        )
        give8(ko2, i)

        @pl.when(i > 1)
        def _():
            push8(ko2, i - 1)

        return 0

    lax.fori_loop(0, 4, backward, 0)
    push8(ko2, 3)
    settle8(kd, dd)

    settle()
    gall = wf
    mine_x = pl.ds(pl.multiple_of(f * C * R, C * R), C * R)
    theirs_x = pl.ds(pl.multiple_of((1 - f) * C * R, C * R), C * R)
    ff_chunk = lambda w, low, high: (
        gall.at[w, :, low:high],
        gall_x.at[w, :, low:high],
        gall_z.at[:, w, :, low:high],
    )
    attn_chunk = lambda low, high: (
        ga.at[:, low:high],
        ga_x.at[:, low:high],
        ga_z.at[:, :, low:high],
    )
    chunks = (
        ff_chunk(2, 0, 128),
        ff_chunk(2, 128, 384),
        ff_chunk(2, 384, U),
        ff_chunk(0, 0, 512),
        ff_chunk(0, 512, U),
        attn_chunk(0, HD),
        ff_chunk(1, 0, 256),
        ff_chunk(1, 256, 640),
        attn_chunk(HD, 2 * HD + LANES),
        ff_chunk(1, 640, U),
    )
    kw = slots(len(chunks))
    kz = slots(len(chunks) * (C - 1))

    def weight_grad(w, left, right, early, lead=0):
        def tile(n, low, high):
            cols = pl.ds(pl.multiple_of(n * LANES, LANES), LANES)
            block = left[:, :, :, cols].reshape(8 * S, LANES)
            gall[w, cols, low:high] = contract_first(
                block, right[:, :, low:high].reshape(8 * S, high - low)
            ).astype(BF16)
            return 0

        first = D // LANES // 2
        if lead:
            lax.fori_loop(0, first + 1, lambda n, _: tile(n + first * (1 - f), 0, lead), 0)
            weight_send(early[0])
            early = early[1:]
        lax.fori_loop(0, first + 1, lambda n, _: tile(n + first * (1 - f), lead, U), 0)
        for q in early:
            weight_send(q)
        lax.fori_loop(0, first, lambda n, _: tile(n + (first + 1) * f, 0, U), 0)

    def weight_send(q):
        full, from_x, _ = chunks[q]
        send(kw + q, full.at[theirs_x], from_x, across)

    def weight_push(q):
        full, from_x, from_z = chunks[q]
        arrive(kw + q, from_x)

        def add(n, _):
            rows = pl.ds(pl.multiple_of(f * C * R + n * R, R), R)
            part = pl.ds(pl.multiple_of(n * R, R), R)
            full[rows] = (full[rows].astype(F32) + from_x[part].astype(F32)).astype(BF16)
            return 0

        lax.fori_loop(0, C, add, 0)
        for step in range(1, C):
            to = (c + step) % C
            send(
                kz + q * (C - 1) + step - 1,
                full.at[rows_of(f, to)],
                from_z.at[step - 1],
                {"context": to},
            )

    def weight_meet(*which):
        for q in which:
            for step in range(1, C):
                arrive(kz + q * (C - 1) + step - 1, chunks[q][2].at[step - 1])

    def weight_end(w):
        same = gall[w, rows_of(f, c)].astype(F32)
        other = jnp.zeros((R, U), F32)
        for step in range(1, C):
            if step % 2:
                other = other + gall_z[step - 1, w].astype(F32)
            else:
                same = same + gall_z[step - 1, w].astype(F32)
        ff_stage[:, 0:U] = jnp.where(m == 0, same, other)
        ff_stage[:, U:units] = jnp.where(m == 0, other, same)[:, 0 : units - U]
        into = out_down if w == 2 else out_gateup.at[:, w]
        saved = pltpu.make_async_copy(ff_stage, into, ls.at[5])
        saved.start()
        saved.wait()

    weight_grad(2, dd, active, (0, 1, 2), 128)
    weight_push(0)
    weight_grad(0, xg, upg, (3, 4))
    weight_push(1)
    d_normed = finish8(ko2)
    hidden = hid[...]
    d_hidden, gain_2 = rms_backward(d_normed, hidden, rms_factor(hidden), gain(2))
    d_hidden = cot[...].astype(F32) + d_hidden
    dhid[...] = d_hidden
    gain_mine[2:3] = gain_2
    branch = bran[...]
    d_branch, gain_1 = rms_backward(d_hidden, branch, rms_factor(branch), gain(1))
    gain_mine[1:2] = gain_1
    db[y, core] = d_branch.astype(BF16)
    kb = share4(db)
    weight_grad(1, xg, gel, ())
    weight_push(2)
    meet4(kb, db)

    def out_grad(n, _):
        cols = pl.ds(pl.multiple_of(n * LANES, LANES), LANES)
        ga[cols, 0:HD] = contract_first(
            db[:, :, :, cols].reshape(T, LANES), mix[...]
        ).astype(BF16)
        return 0

    lax.fori_loop(0, D // LANES, out_grad, 0)
    weight_send(5)
    weight_send(6)
    weight_send(7)

    def scores_back(i, gain_q):
        rows = pl.ds(pl.multiple_of(i * half, half), half)
        d_mixed = mm(db[i].reshape(half, D), wa[:, o_cols]).astype(BF16)
        dmix[rows] = d_mixed
        p = probs[rows]
        d_probs = contract_last(d_mixed, kv[:, HD:])
        inner = jnp.sum(p * d_probs, axis=1, keepdims=True)
        low = (p * (d_probs - inner)).astype(BF16)
        dscore[rows] = low
        d_q = mm(low, kv[:, 0:HD]) * scale
        raw = qraw[rows]
        factor = rms_factor(raw)
        d_raw, part = rms_backward(
            turn_back(d_q, cosine[rows], sine[rows]), raw, factor, head_gain(0)
        )
        dq[rows] = d_raw.astype(BF16)
        return gain_q + part

    gain_q = lax.fori_loop(0, 2, scores_back, jnp.zeros((1, HD), F32))
    kp = slots(3)

    def keys_back(n, _):
        cols = pl.ds(pl.multiple_of(n * half, half), half)
        d_k = contract_first(dscore[:, cols], qs[...]) * scale
        d_v = contract_first(probs[:, cols].astype(BF16), dmix[...])
        both = jnp.concatenate([d_k, d_v], axis=1).astype(BF16)
        kvp[n % 2, 0, n // 2] = both[0:S]
        kvp[n % 2, 1, n // 2] = both[S:]
        return 0

    lax.fori_loop(0, 4, keys_back, 0)
    for i in range(2):
        send(kp + i, kvp.at[i, 1 - core], kvp_core.at[i], partner)

    arrive(kp + (1 - y), kvp_core.at[1 - y])
    kvp_sum[...] = (kvp[1 - y, core].astype(F32) + kvp_core[1 - y].astype(F32)).astype(BF16)
    send(kp + 2, kvp_sum, kvp_chip, chip_of(1 - y, 2))
    kr = share4(block_all)
    weight_push(3)
    arrive(kp + y, kvp_core.at[y])
    arrive(kp + 2, kvp_chip)
    d_left = (
        kvp[y, core, 0].astype(F32) + kvp_core[y, 0].astype(F32) + kvp_chip[0].astype(F32)
    )
    kt = slots(1)
    ret_out[...] = d_left.astype(BF16)

    @pl.when(c > 0)
    def _():
        copy(kt, ret_out, ret_in, {"context": c - 1}).start()

    weight_push(4)
    weight_push(5)
    weight_push(6)

    @pl.when(c < C - 1)
    def _():
        arrive(kt, ret_in)

    @pl.when(c == C - 1)
    def _():
        ret_in[...] = jnp.zeros((S, 2 * HD), BF16)

    d_kv = (
        kvp[y, core, 1].astype(F32)
        + kvp_core[y, 1].astype(F32)
        + kvp_chip[1].astype(F32)
        + ret_in[...].astype(F32)
    )
    raw = jnp.concatenate([kv_raw[0, shard], kv_raw[1, shard]], axis=1).astype(F32)
    d_raw, gain_k = rms_backward(
        turn_back(d_kv[:, :HD], cosine[shard], sine[shard]), raw, rms_factor(raw), head_gain(1)
    )
    d_kv = jnp.concatenate([d_raw, d_kv[:, HD:]], axis=1).astype(BF16)
    for i in range(4):
        dkv_mine[i] = d_kv[:, i * LANES : (i + 1) * LANES]
    kq = slots(4)
    for i in range(1, 4):
        k = (t + i) % 4
        send(kq + i, dkv_mine.at[k], dkv_cols.at[t], {"tensor": k})
    dkv_cols[t] = dkv_mine[t]
    for i in range(1, 4):
        arrive(kq + i, dkv_cols.at[(t - i + 4) % 4])

    k4 = slots(2)

    def query_back(i, _):
        rows = pl.ds(pl.multiple_of(i * half, half), half)
        pair = pl.ds(i * 2, 2)
        part = contract_last(dq[rows], wa[:, q_cols])
        part = part + contract_last(dkv_cols[pair].reshape(half, LANES), wa[:, kv_part])
        part = part.astype(BF16)
        p4[i, 0] = part[0:S]
        p4[i, 1] = part[S:]
        copy(k4 + i, p4.at[i, 1 - core], p4_core.at[i], partner).start()
        return 0

    lax.fori_loop(0, 2, query_back, 0)

    def attn_grad(n, _):
        cols = pl.ds(pl.multiple_of(n * LANES, LANES), LANES)
        left = nrm[:, cols]
        ga[cols, HD : 2 * HD] = contract_first(left, dq[...]).astype(BF16)
        ga[cols, 2 * HD :] = contract_first(left, dkv_cols[...].reshape(T, LANES)).astype(BF16)
        return 0

    lax.fori_loop(0, D // LANES, attn_grad, 0)
    weight_send(8)
    weight_send(9)
    weight_push(7)
    kc = sum4(k4)
    meet4(kr, block_all)
    save_block = pltpu.make_async_copy(block_all, out_block, ls.at[3])
    save_block.start()
    d_normed = finish4(kc)
    copy(kc, p4_sum, p4_chip, chip_of(1 - y, 2)).wait_send()
    for i in range(2):
        copy(k4 + i, p4.at[i, 1 - core], p4_core.at[i], partner).wait_send()
    values = act[shard].astype(F32)
    d_input, gain_0 = rms_backward(d_normed, values, rms_factor(values), gain(0))
    input_all[y, core] = (dhid[...] + d_input).astype(BF16)
    gain_mine[0:1] = gain_0
    gain_mine[4:8] = jnp.zeros((4, D), F32)
    gain_mine[4:5, 0:HD] = gain_q
    gain_mine[5:6, 0:HD] = gain_k
    kn = slots(4 + 1 + C)
    for i in range(1, 4):
        send(kn + i, gain_mine, gain_tensor.at[i], {"tensor": (t + i) % 4})
    ki = share4(input_all)
    weight_push(8)
    total = gain_mine[...]
    for i in range(1, 4):
        arrive(kn + i, gain_tensor.at[i])
        total = total + gain_tensor[i]
    gain_tensor[0] = total
    send(kn, gain_tensor.at[0], gain_x.at[0], across)
    arrive(kn, gain_x.at[0])
    gain_x[1] = total + gain_x[0]
    for step in range(1, C):
        send(kn + 4 + step, gain_x.at[1], gain_z.at[step], along(step))
    weight_push(9)
    weight_meet(0, 1, 2)
    weight_end(2)
    meet4(ki, input_all)
    save_input = pltpu.make_async_copy(input_all, out_input, ls.at[4])
    save_input.start()
    weight_meet(3, 4)
    weight_end(0)
    weight_meet(5, 8)
    attn = ga[rows_of(f, c)].astype(F32)
    for step in range(1, C):
        attn = attn + ga_z[step - 1].astype(F32)
    kvg[t] = attn[:, 2 * HD :]
    kh = slots(4)
    for i in range(1, 4):
        send(kh + i, kvg.at[t], kvg.at[t], {"tensor": (t + i) % 4})
    st_out[...] = attn[:, 0:HD]
    st_query[...] = attn[:, HD : 2 * HD]
    staged = []

    def save(n, src, dst):
        staged.append(pltpu.make_async_copy(src, dst, ls.at[10 + n]))
        staged[-1].start()

    save(0, st_out, out_out)
    save(1, st_query, out_query)
    total = gain_x[1]
    for step in range(1, C):
        arrive(kn + 4 + step, gain_z.at[step])
        total = total + gain_z[step]
    owner = f * C + c
    moved = pltpu.roll(total, (D - owner * R) % D, 1)
    st_norm[...] = moved[0:4, 0:R]
    moved = pltpu.roll(total[:, 0:HD], (HD - owner * narrow) % HD, 1)
    st_head[...] = moved[4:6, 0:narrow]
    save(2, st_norm, out_norm)
    save(3, st_head, out_head)
    weight_meet(6, 7, 9)
    weight_end(1)
    for i in range(1, 4):
        arrive(kh + i, kvg.at[(t - i + 4) % 4])
    for k in range(4):
        st_kv[:, k * LANES : (k + 1) * LANES] = kvg[k]
    save(4, st_kv, out_kv)
    save_block.wait()
    save_input.wait()
    for moved in staged:
        moved.wait()
    settle()

    @pl.when(c < C - 1)
    def _():
        copy(ks, seg_row, seg_left, {"context": c + 1}).wait_send()
        copy(kk, kv.at[own_half], kv.at[my_half], {"context": c + 1}).wait_send()

    @pl.when(c > 0)
    def _():
        copy(kt, ret_out, ret_in, {"context": c - 1}).wait_send()
    assert counter[0] == SEMAPHORES, counter


def fused(
    mesh,
    activations,
    positions,
    seg_ids,
    norm_gains,
    head_gains,
    w_query,
    w_keyval,
    w_out,
    w_gateup,
    w_down,
    cotangent,
):
    C = mesh.shape["context"]
    T, D = activations.shape[1:]
    R, units = w_down.shape
    U = -(-units // (2 * LANES)) * LANES
    S = T // 4
    pack = -(-R // LANES) * LANES
    operands = (
        activations[0],
        positions,
        seg_ids,
        norm_gains,
        head_gains,
        w_gateup,
        w_down,
        cotangent[0],
        w_query,
        w_keyval,
        w_out,
    )
    scratch = [
        pltpu.VMEM((T, D), BF16),
        pltpu.VMEM(w_gateup.shape, BF16),
        pltpu.VMEM(w_down.shape, BF16),
        pltpu.VMEM((T, HD // 2), F32),
        pltpu.VMEM((T, HD // 2), F32),
        pltpu.VMEM((8, T), jnp.int32),
        pltpu.VMEM((T, 1), jnp.int32),
        pltpu.VMEM((8, pack), F32),
        pltpu.VMEM((2 * C, 8, pack), F32),
        pltpu.VMEM((2, 3, R, U), BF16),
        pltpu.VMEM((S, D), BF16),
        pltpu.VMEM((D, 2 * HD + LANES), BF16),
        pltpu.VMEM((3, D, U), BF16),
        pltpu.VMEM((8, T), jnp.int32),
        pltpu.VMEM((8, D), F32),
        pltpu.VMEM((8, HD), F32),
        pltpu.VMEM((T, D), BF16),
        pltpu.VMEM((T, HD), F32),
        pltpu.VMEM((4, T, LANES), BF16),
        pltpu.VMEM((T, HD), BF16),
        pltpu.VMEM((2 * T, 2 * HD), BF16),
        pltpu.VMEM((T, 2 * T), F32),
        pltpu.VMEM((T, HD), BF16),
        pltpu.VMEM((2, 2, S, D), BF16),
        pltpu.VMEM((2, S, D), BF16),
        pltpu.VMEM((S, D), BF16),
        pltpu.VMEM((S, D), BF16),
        pltpu.VMEM((S, D), F32),
        pltpu.VMEM((S, D), F32),
        pltpu.VMEM((4, 2, S, D), BF16),
        pltpu.VMEM((4, 2 * S, U), BF16),
        pltpu.VMEM((4, 2 * S, U), BF16),
        pltpu.VMEM((4, 2 * S, U), BF16),
        pltpu.VMEM((4, 2, S, D), BF16),
        pltpu.VMEM((4, S, D), BF16),
        pltpu.VMEM((3, S, D), BF16),
        pltpu.VMEM((3, S, D), BF16),
        pltpu.VMEM((4, 2, S, D), BF16),
        pltpu.VMEM((S, D), F32),
        pltpu.VMEM((2, 2, S, D), BF16),
        pltpu.VMEM((T, 2 * T), BF16),
        pltpu.VMEM((T, HD), BF16),
        pltpu.VMEM((T, HD), BF16),
        pltpu.VMEM((2, 2, 2, S, 2 * HD), BF16),
        pltpu.VMEM((2, 2, S, 2 * HD), BF16),
        pltpu.VMEM((2, S, 2 * HD), BF16),
        pltpu.VMEM((2, S, 2 * HD), BF16),
        pltpu.VMEM((S, 2 * HD), BF16),
        pltpu.VMEM((S, 2 * HD), BF16),
        pltpu.VMEM((4, S, LANES), BF16),
        pltpu.VMEM((4, S, LANES), BF16),
        pltpu.VMEM((3, C * R, U), BF16),
        pltpu.VMEM((C - 1, 3, R, U), BF16),
        pltpu.VMEM((D, 2 * HD + LANES), BF16),
        pltpu.VMEM((C * R, 2 * HD + LANES), BF16),
        pltpu.VMEM((C - 1, R, 2 * HD + LANES), BF16),
        pltpu.VMEM((4, R, LANES), F32),
        pltpu.VMEM((R, units), F32),
        pltpu.VMEM((8, D), F32),
        pltpu.VMEM((4, 8, D), F32),
        pltpu.VMEM((2, 8, D), F32),
        pltpu.VMEM((C, 8, D), F32),
        pltpu.VMEM((2, 2, S, D), BF16),
        pltpu.VMEM((2, 2, S, D), BF16),
        pltpu.VMEM((R, HD), F32),
        pltpu.VMEM((R, HD), F32),
        pltpu.VMEM(norm_gains.shape, F32),
        pltpu.VMEM(head_gains.shape, F32),
        pltpu.VMEM((R, 2 * HD), F32),
        pltpu.SemaphoreType.DMA((SEMAPHORES,)),
        pltpu.SemaphoreType.DMA((SEMAPHORES,)),
        pltpu.SemaphoreType.DMA((18,)),
    ]
    vmem = pl.BlockSpec(memory_space=pltpu.VMEM)
    anywhere = pl.BlockSpec(memory_space=pl.ANY)
    results = (
        jax.ShapeDtypeStruct((2, 2, S, D), BF16),
        jax.ShapeDtypeStruct((2, 2, S, D), BF16),
        jax.ShapeDtypeStruct(norm_gains.shape, F32),
        jax.ShapeDtypeStruct(head_gains.shape, F32),
        jax.ShapeDtypeStruct(w_query.shape, F32),
        jax.ShapeDtypeStruct(w_keyval.shape, F32),
        jax.ShapeDtypeStruct(w_out.shape, F32),
        jax.ShapeDtypeStruct(w_gateup.shape, F32),
        jax.ShapeDtypeStruct(w_down.shape, F32),
    )
    sizes = {"context": C, "tokens": T, "width": D, "rows": R, "units": U}
    parts = pl.pallas_call(
        functools.partial(fused_kernel, sizes),
        out_shape=results,
        in_specs=[anywhere] + [vmem] * 4 + [anywhere] * 6,
        out_specs=[anywhere] * len(results),
        scratch_shapes=scratch,
        compiler_params=pltpu.CompilerParams(
            collective_id=0, has_side_effects=True, vmem_limit_bytes=67043328
        ),
    )(*operands)
    count = len(parts)
    block_out, input_grad, *grads = pl.pallas_call(
        functools.partial(emit_kernel, count),
        out_shape=results,
        in_specs=[anywhere] * count,
        out_specs=[anywhere] * count,
        scratch_shapes=[pltpu.VMEM(part.shape, part.dtype) for part in parts]
        + [pltpu.SemaphoreType.DMA((count,))] * 2,
    )(*parts)
    return block_out.reshape(1, T, D), input_grad.reshape(1, T, D), *grads


def block(mesh, *arrays):
    tokens, rows = arrays[0].shape[1], arrays[9].shape[0]
    fits = (
        mesh.shape["fsdp"] == 2
        and mesh.shape["tensor"] == 4
        and mesh.shape["context"] == 4
        and tokens == WINDOW
        and rows % 16 == 0
        and arrays[5].shape[1] == HD
        and arrays[6].shape[1] == 4 * LANES
    )
    return fused(mesh, *arrays) if fits else shards(*arrays)


def shards(
    activations,
    positions,
    seg_ids,
    norm_gains,
    head_gains,
    w_query,
    w_keyval,
    w_out,
    w_gateup,
    w_down,
    cotangent,
):
    tokens = activations.shape[1]
    local_heads = w_query.shape[1] // HD
    inputs = activations[0].astype(jnp.float32)
    places = positions[0]
    documents = seg_ids[0]
    gains_all, heads_all, query_all, keyval_all, out_all = (
        lax.all_gather(norm_gains, ("fsdp", "context"), axis=1, tiled=True),
        lax.all_gather(head_gains, ("fsdp", "context"), axis=1, tiled=True),
        lax.all_gather(w_query, ("fsdp", "context"), axis=0, tiled=True),
        lax.all_gather(w_keyval, ("fsdp", "context"), axis=0, tiled=True),
        lax.all_gather(w_out, ("fsdp", "context"), axis=0, tiled=True),
    )
    gains_f = gains_all.astype(jnp.float32)
    heads_f = heads_all.astype(jnp.float32)
    normed_f, input_back = jax.vjp(rms_norm, inputs, gains_f[0])
    normed = normed_f.astype(jnp.bfloat16)
    query_raw = jnp.dot(normed, query_all, preferred_element_type=jnp.float32).reshape(
        tokens, local_heads, HD
    )
    keyval_raw = jnp.dot(normed, keyval_all, preferred_element_type=jnp.float32)

    def prepare(raw_heads, head_gain):
        return rotate(rms_norm(raw_heads, head_gain), places)

    query_rot, query_back = jax.vjp(prepare, query_raw, heads_f[0])
    key_rot, key_back = jax.vjp(prepare, keyval_raw[:, None, :HD], heads_f[1])
    queries = query_rot.astype(jnp.bfloat16)
    own_keyval = jnp.concatenate([key_rot[:, 0], keyval_raw[:, HD:]], axis=1).astype(jnp.bfloat16)
    labels = jnp.stack([places, documents])
    keep_from = tokens - tokens
    left_keyval, left_labels = from_behind((own_keyval, labels), "context", 1)
    keys_all = jnp.concatenate([left_keyval, own_keyval], axis=0)
    key_places = jnp.concatenate([left_labels[0], places])
    key_documents = jnp.concatenate([left_labels[1], documents])
    has_left = lax.axis_index("context") > 0
    key_live = jnp.concatenate([jnp.full((tokens,), has_left), jnp.ones((tokens,), dtype=bool)])
    scale_factor = HD ** (-0.5)
    block_rows = 512
    block_starts = jnp.arange(tokens // block_rows) * block_rows

    def block_scores():
        spacing = places[:, None] - key_places[None, :]
        visible = (
            key_live[None, :]
            & (documents[:, None] == key_documents[None, :])
            & (spacing >= 0)
            & (spacing < WINDOW)
        )
        raw_scores = (
            jnp.einsum("qhd,kd->hqk", queries, keys_all[:, :HD], preferred_element_type=jnp.float32)
            * scale_factor
        )
        return (jnp.where(visible[None], raw_scores, -1e30), keys_all, queries)

    def forward_block(start):
        scores, near_keyval, query_block = block_scores()
        row_top = jnp.max(scores, axis=-1, keepdims=True)
        raised = jnp.exp(scores - row_top)
        row_total = jnp.sum(raised, axis=-1, keepdims=True)
        probs = raised / row_total
        mixed_block = jnp.einsum(
            "hqk,kd->qhd",
            probs.astype(jnp.bfloat16),
            near_keyval[:, HD:],
            preferred_element_type=jnp.float32,
        )
        return (mixed_block.astype(jnp.bfloat16), row_top + jnp.log(row_total))

    mixed_blocks, log_blocks = lax.map(forward_block, block_starts)
    mixed_low = mixed_blocks.reshape(tokens, local_heads * HD)
    branch = lax.psum(contract_last(mixed_low, out_all).astype(jnp.bfloat16), "tensor").astype(jnp.float32)
    post_attn, post_attn_back = jax.vjp(rms_norm, branch, gains_f[1])
    hidden = inputs + post_attn
    normed_mlp_f, pre_mlp_back = jax.vjp(rms_norm, hidden, gains_f[2])
    normed_mlp = normed_mlp_f.astype(jnp.bfloat16)
    columns = normed_mlp
    gate_up = jnp.einsum(
        "bn,nkf->bkf",
        columns,
        lax.all_gather(w_gateup, ("fsdp", "context"), axis=0, tiled=True),
        preferred_element_type=jnp.float32,
    )
    active_f, glu_back = jax.vjp(glu, gate_up)
    active = active_f.astype(jnp.bfloat16)
    down = lax.psum(
        contract_last(
            active, lax.all_gather(w_down, ("fsdp", "context"), axis=0, tiled=True)
        ).astype(jnp.bfloat16),
        "tensor",
    ).astype(jnp.float32)
    post_mlp, post_mlp_back = jax.vjp(rms_norm, down, gains_f[3])
    result = hidden + post_mlp
    grad_out = cotangent[0].astype(jnp.float32)
    d_down, gain_post_mlp = post_mlp_back(grad_out)
    down_low = d_down.astype(jnp.bfloat16)
    columns = down_low
    d_active = jnp.dot(
        columns,
        lax.all_gather(w_down, ("fsdp", "context"), axis=0, tiled=True),
        preferred_element_type=jnp.float32,
    )
    d_gate_up = glu_back(d_active)[0].astype(jnp.bfloat16)
    d_normed_part = jnp.einsum(
        "bkf,nkf->bn",
        d_gate_up,
        lax.all_gather(w_gateup, ("fsdp", "context"), axis=0, tiled=True),
        preferred_element_type=jnp.float32,
    )
    d_normed_mlp = lax.psum(d_normed_part.astype(jnp.bfloat16), "tensor").astype(jnp.float32)
    d_hidden_norm, gain_pre_mlp = pre_mlp_back(d_normed_mlp)
    d_hidden = grad_out + d_hidden_norm
    features = normed_mlp
    grad_cols = down_low
    gate_up_term = jnp.einsum(
        "bn,bkf->nkf", features, d_gate_up, preferred_element_type=jnp.float32
    )
    down_term = contract_first(grad_cols, active)
    scatter = lambda part: lax.psum_scatter(
        part.astype(jnp.bfloat16), ("fsdp", "context"), scatter_dimension=0, tiled=True
    ).astype(jnp.float32)
    gate_grad = scatter(gate_up_term[:, 0])
    up_grad = scatter(gate_up_term[:, 1])
    down_grad = scatter(down_term)
    d_branch, gain_post_attn = post_attn_back(d_hidden)
    branch_low = d_branch.astype(jnp.bfloat16)
    d_mixed = jnp.dot(branch_low, out_all, preferred_element_type=jnp.float32)
    d_mixed_low = d_mixed.astype(jnp.bfloat16).reshape(tokens, local_heads, HD)

    def backward_block(carry, item):
        start, log_block = item
        scores, near_keyval, query_block = block_scores()
        probs_again = jnp.exp(scores - log_block)
        d_probs = jnp.einsum(
            "qhd,kd->hqk", d_mixed_low, near_keyval[:, HD:], preferred_element_type=jnp.float32
        )
        row_inner = jnp.sum(probs_again * d_probs, axis=-1, keepdims=True)
        d_scores = (probs_again * (d_probs - row_inner)).astype(jnp.bfloat16)
        d_query_block = (
            jnp.einsum(
                "hqk,kd->qhd", d_scores, near_keyval[:, :HD], preferred_element_type=jnp.float32
            )
            * scale_factor
        )
        d_keys = (
            jnp.einsum("hqk,qhd->kd", d_scores, query_block, preferred_element_type=jnp.float32)
            * scale_factor
        )
        d_values = jnp.einsum(
            "hqk,qhd->kd",
            probs_again.astype(jnp.bfloat16),
            d_mixed_low,
            preferred_element_type=jnp.float32,
        )
        updated = carry + jnp.concatenate([d_keys, d_values], axis=1)
        return (updated, d_query_block)

    d_keyval, d_query_blocks = lax.scan(
        backward_block,
        jnp.zeros((tokens + tokens, 2 * HD), jnp.float32),
        (block_starts, log_blocks),
    )
    d_queries = d_query_blocks.reshape(tokens, local_heads, HD)
    returned = from_behind(d_keyval[:tokens].astype(jnp.bfloat16), "context", -1).astype(
        jnp.float32
    )
    own_grad = d_keyval[tokens:].at[keep_from:].add(returned)
    d_query_raw, gain_query = query_back(d_queries)
    d_query_low = d_query_raw.reshape(tokens, local_heads * HD).astype(jnp.bfloat16)
    d_normed_query, keyval_grad, gain_query_all = (
        lax.psum(contract_last(d_query_low, query_all).astype(jnp.bfloat16), "tensor").astype(
            jnp.float32
        ),
        lax.psum(own_grad.astype(jnp.bfloat16), "tensor").astype(jnp.float32),
        lax.psum(gain_query.astype(jnp.bfloat16), "tensor").astype(jnp.float32),
    )
    d_key_raw, gain_key = key_back(keyval_grad[:, None, :HD])
    d_keyval_low = jnp.concatenate([d_key_raw[:, 0], keyval_grad[:, HD:]], axis=1).astype(
        jnp.bfloat16
    )
    d_normed = d_normed_query + contract_last(d_keyval_low, keyval_all)
    d_input_norm, gain_input = input_back(d_normed)
    input_total = d_hidden + d_input_norm
    features = normed
    grad_cols = branch_low
    attn_grads = lax.psum_scatter(
        jnp.stack(
            [contract_first(features, d_query_low), contract_first(grad_cols, mixed_low)], axis=1
        ).astype(jnp.bfloat16),
        ("fsdp", "context"),
        scatter_dimension=0,
        tiled=True,
    ).astype(jnp.float32)
    keyval_term = contract_first(normed, d_keyval_low)
    gain_terms = jnp.stack([gain_input, gain_post_attn, gain_pre_mlp, gain_post_mlp])
    head_terms = jnp.stack([gain_query_all, gain_key])
    gain_grad, head_grad, keyval_weight_grad = (
        lax.psum_scatter(
            gain_terms.astype(jnp.bfloat16), ("fsdp", "context"), scatter_dimension=1, tiled=True
        ).astype(jnp.float32),
        lax.psum_scatter(
            head_terms.astype(jnp.bfloat16), ("fsdp", "context"), scatter_dimension=1, tiled=True
        ).astype(jnp.float32),
        lax.psum_scatter(
            keyval_term.astype(jnp.bfloat16), ("fsdp", "context"), scatter_dimension=0, tiled=True
        ).astype(jnp.float32),
    )
    return (
        result[None].astype(jnp.bfloat16),
        input_total[None].astype(jnp.bfloat16),
        gain_grad,
        head_grad,
        attn_grads[:, 0],
        keyval_weight_grad,
        attn_grads[:, 1],
        jnp.stack([gate_grad, up_grad], axis=1),
        down_grad,
    )


def solution(mesh):
    return jax.shard_map(
        functools.partial(block, mesh),
        mesh=mesh,
        in_specs=(
            P("fsdp", "context", None),
            P("fsdp", "context"),
            P("fsdp", "context"),
            P(None, ("fsdp", "context")),
            P(None, ("fsdp", "context")),
            P(("fsdp", "context"), "tensor"),
            P(("fsdp", "context"), None),
            P(("fsdp", "context"), "tensor"),
            P(("fsdp", "context"), None, "tensor"),
            P(("fsdp", "context"), "tensor"),
            P("fsdp", "context", None),
        ),
        out_specs=(
            P("fsdp", "context", None),
            P("fsdp", "context", None),
            P(None, ("fsdp", "context")),
            P(None, ("fsdp", "context")),
            P(("fsdp", "context"), "tensor"),
            P(("fsdp", "context"), None),
            P(("fsdp", "context"), "tensor"),
            P(("fsdp", "context"), None, "tensor"),
            P(("fsdp", "context"), "tensor"),
        ),
        check_vma=False,
    )
```
